128 devices in a mesh: rows: 32 (over y, x, core), cols: 4 (over z).
Axes of the slice: x: 4, y: 4, z: 4, core: 2. Of those that a mesh axis runs over, the one named last changes fastest.
Arguments:
- token_ids: int32 [64, 2048], P('rows', 'cols'), may hold values from 0 to 524287, as said below
- lengths: int32 [64], P('rows'), may hold values from 1 to 2048
- table: bfloat16 [524288, 512], P('rows', 'cols'), may hold values from -6 to 6
- attn_gain: float32 [512], replicated, may hold values from 0.1 to 1.9
- w_qkv: bfloat16 [512, 1536], replicated, may hold values from -2 to 2
- w_out: bfloat16 [512, 512], replicated, may hold values from -0.25 to 0.25
- mlp_gain: float32 [512], replicated, may hold values from 0.1 to 1.9
- w_in: bfloat16 [512, 4096], replicated, may hold values from -0.25 to 0.25
- w_down: bfloat16 [2048, 512], replicated, may hold values from -0.125 to 0.125
Outputs:
- layer_out: bfloat16 [64, 2048, 512], P('rows', 'cols')
The draws below stay inside these ranges and needn't reach their ends.
Inputs may be any that keep to these rules, and one draw needn't show every extreme that they name: `token_ids`: ids lie in 0 to 524287. In each aligned block of 2 histories (4096 positions) at most 341 ids fall in any one block of 16384 consecutive table rows, and in every such block of histories some block of table rows receives exactly 341.
All inputs are finite; a program needn't handle non-finite values.
Results may differ from the reference program's by a relative error of at most 0.012.
Values may be sent and summed in bfloat16 or wider, within the bound.
A program may use at most 192 MiB of HBM per device.

```python
import jax
import jax.numpy as jnp
from jax import lax

D = 512
HEADS = 8
FF = 2048
VOC_DEV = 16384
BD = 2
L = 2048
B = 64
VOCAB = 524288
CAP = 341


def one_block(key):
    key_hot, key_order, key_shuffle, key_offset = jax.random.split(key, 4)
    block_count = B // BD
    token_count = BD * L
    hot_block = jax.random.randint(key_hot, (), 0, block_count)
    slot_ids = jnp.arange(block_count * CAP, dtype=jnp.int32)
    slot_block = slot_ids // CAP
    order_rank = jax.random.permutation(key_order, block_count * CAP).astype(jnp.int32)
    priority = jnp.where(slot_block == hot_block, 0, 1) * (block_count * CAP) + order_rank
    chosen_order = jnp.argsort(priority)
    chosen_block = slot_block[chosen_order[:token_count]]
    chosen_block = jax.random.permutation(key_shuffle, chosen_block)
    offsets = jax.random.randint(key_offset, (token_count,), 0, VOC_DEV)
    return (chosen_block * VOC_DEV + offsets).astype(jnp.int32).reshape(BD, L)


def draw_token_ids(key, part):
    keys = jax.random.split(jax.random.fold_in(key, 11), B // BD)
    return jax.vmap(one_block)(keys).reshape(B, L)


def draw_w_qkv(key, part):
    key_base = jax.random.fold_in(jax.random.fold_in(key, 23), 0)
    base = jnp.clip(jax.random.normal(key_base, (D, 3 * D), jnp.float32), -5.0, 5.0) / jnp.sqrt(1.0 * D)
    return jnp.clip(base, -2.0, 2.0).astype(jnp.bfloat16)


def touch_ends(drawn, stream_key, low, top_value):
    longest = drawn.shape.index(max(drawn.shape))
    spots = []
    for shift in (0, 1):
        where = [jax.random.randint(jax.random.fold_in(stream_key, axis), (), 0, length) for axis, length in enumerate(drawn.shape)]
        where[longest] = (where[longest] + shift) % drawn.shape[longest]
        spots.append(tuple(where))
    return drawn.at[spots[0]].set(low).at[spots[1]].set(top_value)


def block_scale(stream_key, extent, shards, low, largest):
    loudness = 1.0
    for axis_at, parts in shards:
        draws = jax.random.uniform(jax.random.fold_in(jax.random.fold_in(stream_key, 6), axis_at), (parts,), jnp.float32, low / len(shards), largest / len(shards))
        loudness = loudness * jnp.repeat(jnp.exp(draws), extent[axis_at] // parts).reshape((-1,) + (1,) * (len(extent) - 1 - axis_at))
    return loudness


def centred(key, shape, scale, most, cuts=(), kind=jnp.bfloat16):
    factor_of = block_scale(key, shape, cuts, -0.22, 0.18) if cuts else 1.0
    entries = jax.random.normal(key, shape, jnp.float32) * scale * factor_of
    return jnp.minimum(jnp.maximum(entries, -most), most).astype(kind)


def setup_inputs(seed: int = 0) -> dict:
    streams_of = jax.random.split(jax.random.key(seed), 10)
    return {
        "token_ids": draw_token_ids(jax.random.fold_in(streams_of[9], 71), 0),
        "lengths": touch_ends(jax.random.randint(streams_of[1], (B,), 1, L + 1), jax.random.fold_in(streams_of[1], 1), 1, L).astype(jnp.int32),
        "table": centred(streams_of[2], (VOCAB, D), 1.0, 6.0, ((0, 32), (1, 4))),
        "attn_gain": jnp.clip(1.0 + 0.18 * jax.random.normal(streams_of[3], (D,), jnp.float32), 0.1, 1.9),
        "w_qkv": draw_w_qkv(jax.random.fold_in(streams_of[9], 71), 0),
        "w_out": centred(streams_of[5], (D, D), D ** -0.5, 0.25),
        "mlp_gain": jnp.clip(1.0 + 0.18 * jax.random.normal(streams_of[6], (D,), jnp.float32), 0.1, 1.9),
        "w_in": centred(streams_of[7], (D, 2 * FF), D ** -0.5, 0.25),
        "w_down": centred(streams_of[8], (FF, D), FF ** -0.5, 0.125),
    }


def rms_norm(values_f32, gain):
    mean_sq = lax.optimization_barrier(jnp.mean(values_f32 * values_f32, axis=-1, keepdims=True))
    return values_f32 * lax.rsqrt(mean_sq + 1e-06) * gain

def layer(sequence, length, attn_gain, w_qkv, w_out, mlp_gain, w_in, w_down):
    residual = sequence.astype(jnp.float32)
    normed = rms_norm(residual, attn_gain).astype(jnp.bfloat16)
    projected = jnp.dot(normed, w_qkv, preferred_element_type=jnp.float32).astype(jnp.bfloat16)
    head_dim = D // HEADS
    queries = projected[:, :D].reshape(L, HEADS, head_dim).astype(jnp.float32)
    keys = projected[:, D:2 * D].reshape(L, HEADS, head_dim).astype(jnp.float32)
    values = projected[:, 2 * D:].reshape(L, HEADS, head_dim).astype(jnp.float32)
    scores = jnp.einsum('qhd,khd->hqk', queries, keys) * 0.125
    position = jnp.arange(L, dtype=jnp.int32)
    valid = (position[None, :] <= position[:, None]) & (position[None, :] < length)
    valid = valid[None, :, :]
    scores = jnp.where(valid, scores, -1e+30)
    row_max = lax.optimization_barrier(jnp.max(scores, axis=-1, keepdims=True))
    probs = jnp.where(valid, jnp.exp(scores - row_max), 0.0)
    total = lax.optimization_barrier(jnp.sum(probs, axis=-1))
    weights = probs.astype(jnp.bfloat16).astype(jnp.float32)
    summed = jnp.einsum('hqk,khd->hqd', weights, values) / total[..., None]
    attended = jnp.transpose(summed, (1, 0, 2)).reshape(L, D).astype(jnp.bfloat16)
    hidden = (residual + jnp.dot(attended, w_out, preferred_element_type=jnp.float32)).astype(jnp.bfloat16)
    hidden_f32 = hidden.astype(jnp.float32)
    normed_two = rms_norm(hidden_f32, mlp_gain).astype(jnp.bfloat16)
    gate_up = jnp.dot(normed_two, w_in, preferred_element_type=jnp.float32)
    act = (jax.nn.silu(gate_up[:, :FF]) * gate_up[:, FF:]).astype(jnp.bfloat16)
    return (hidden_f32 + jnp.dot(act, w_down, preferred_element_type=jnp.float32)).astype(jnp.bfloat16)

def reference(token_ids, lengths, table, attn_gain, w_qkv, w_out, mlp_gain, w_in, w_down):
    embedded = jnp.take(table, token_ids, axis=0)

    def one_history(pair):
        sequence, length = pair
        return layer(sequence, length, attn_gain, w_qkv, w_out, mlp_gain, w_in, w_down)
    return lax.map(one_history, (embedded, lengths))
```

```python
import functools

import jax
import jax.numpy as jnp
from jax import lax
from jax.experimental import pallas as pl
from jax.experimental.pallas import tpu as pltpu
from jax.sharding import PartitionSpec as P

D = 512
FF = 2048
CAP = 344
BF = jnp.bfloat16
F32 = jnp.float32
MESH = pl.DeviceIdType.MESH
ANY = pl.BlockSpec(memory_space=pl.ANY)
VM = pl.BlockSpec(memory_space=pltpu.VMEM)
SM = pl.BlockSpec(memory_space=pltpu.SMEM)
LOG2E = 1.4426950408889634
NEG = -1e30


def dot(a, b):
    return jnp.dot(a, b, preferred_element_type=F32)


def dot_t(a, b):
    return lax.dot_general(a, b, (((1,), (1,)), ((), ())), preferred_element_type=F32)


def place():
    r, z = lax.axis_index("rows"), lax.axis_index("cols")
    return r, z, r // 8, (r // 2) % 4, r % 2


def greet(devices):
    barrier = pltpu.get_barrier_semaphore()
    for device in devices:
        pl.semaphore_signal(barrier, inc=1, device_id=device, device_id_type=MESH)
    pl.semaphore_wait(barrier, len(devices))


def remote(src, dst, send_sem, recv_sem, device):
    return pltpu.make_async_remote_copy(
        src_ref=src, dst_ref=dst, send_sem=send_sem, recv_sem=recv_sem,
        device_id=device, device_id_type=MESH)


def params(collective_id=None, vmem=60):
    kw = {}
    if collective_id is not None:
        kw = dict(collective_id=collective_id, has_side_effects=True)
    return pltpu.CompilerParams(vmem_limit_bytes=vmem * 2**20, **kw)


def ids_kernel(ids_ref, out_ref, send_sem, recv_sem):
    r, z, _, _, _ = place()
    peers = [(r, (z + s) % 4) for s in (1, 2, 3)]
    greet(peers)
    copies = []
    for s, device in enumerate(peers):
        copy = remote(ids_ref, out_ref.at[z], send_sem.at[s], recv_sem.at[s], device)
        copy.start()
        copies.append(copy)
    out_ref[z] = ids_ref[...]
    for copy in copies:
        copy.wait()


def request_kernel(len_ref, ids_ref, msg_ref, slot_ref):
    ids = ids_ref[...]
    owner = ids >> 14
    low, high = (ids & 127).astype(F32), ((ids >> 7) & 127).astype(F32)
    before = (lax.broadcasted_iota(jnp.int32, (128, 128), 0)
              < lax.broadcasted_iota(jnp.int32, (128, 128), 1)).astype(F32).astype(BF)
    above = (lax.broadcasted_iota(jnp.int32, (32, 32), 1)
             < lax.broadcasted_iota(jnp.int32, (32, 32), 0)).astype(F32).astype(BF)
    ones = jnp.ones((128, 128), BF)
    rank = jnp.zeros((32, 128), F32)
    for o in range(32):
        hit = owner == o
        one = jnp.where(hit, 1.0, 0.0).astype(BF)
        prior = dot(one, before) + dot(dot(above, one).astype(BF), ones)
        rank = rank + jnp.where(hit, prior, 0.0)
    rank_i = rank.astype(jnp.int32)
    slot_ref[...] = owner * CAP + rank_i
    owners = lax.broadcasted_iota(jnp.int32, (32, 128), 0)
    ks = lax.broadcasted_iota(jnp.int32, (384, 128), 0)
    acc = jnp.zeros((64, 384), F32)
    count = jnp.zeros((32, 128), F32)
    for a in range(32):
        hit = owners == owner[a : a + 1, :]
        count = count + jnp.where(hit, 1.0, 0.0)
        left = jnp.concatenate(
            [jnp.where(hit, low[a : a + 1, :], 0.0), jnp.where(hit, high[a : a + 1, :], 0.0)], axis=0)
        right = jnp.where(ks == rank_i[a : a + 1, :], 1.0, 0.0)
        acc = acc + dot_t(left.astype(BF), right.astype(BF))
    req = (acc[32:] * 128.0 + acc[:32]).astype(jnp.int32)
    for j in range(3):
        msg_ref[:, j, :] = req[:, 128 * j : 128 * j + 128]
    total = jnp.sum(count, axis=1, keepdims=True).astype(jnp.int32)
    lane = lax.broadcasted_iota(jnp.int32, (32, 128), 1)
    tail = jnp.where(lane == 0, total, 0)
    tail = jnp.where(lane == 1, len_ref[0], jnp.where(lane == 2, len_ref[1], tail))
    msg_ref[:, 3, :] = tail


def ask_kernel(msg_ref, out_ref, send_sem, recv_sem):
    r, z, _, _, _ = place()
    peers = [((r + s) % 32, z) for s in range(1, 32)]
    greet(peers)
    copies = []
    for s, device in enumerate(peers):
        copy = remote(msg_ref.at[device[0]], out_ref.at[r], send_sem.at[s], recv_sem.at[s], device)
        copy.start()
        copies.append(copy)
    out_ref[r] = msg_ref[r]
    for copy in copies:
        copy.wait()


def lookup_kernel(asked_ref, table_ref, out_ref, wide, stage):
    def widen(i, _):
        rows = pl.ds(pl.multiple_of(i * 256, 256), 256)
        wide[rows, :] = table_ref[rows, :].astype(F32)
        return 0

    lax.fori_loop(0, 64, widen, 0)
    stage[...] = jnp.zeros_like(stage)

    def block(p, _):
        def some(j, _):
            base = j * 16
            row, col = base // 128, lax.rem(base, 128)
            for i in range(16):
                stage[pl.ds(base + i, 1), :] = wide[pl.ds(asked_ref[p, row, col + i], 1), :]
            return 0

        lax.fori_loop(0, (asked_ref[p, 3, 0] + 15) // 16, some, 0)
        out_ref[p] = stage[0:CAP, :].astype(BF)
        return 0

    lax.fori_loop(0, 32, block, 0)


def routes():
    out = []
    for dy in range(4):
        for dx in range(4):
            for dk in range(2):
                if dx == dy == dk == 0:
                    continue
                side = 1 if dk == 0 else 3
                hop = None
                if dx == 2 or dy == 2:
                    hop = (side if dy == 2 else 0, side if dx == 2 else 0)
                out.append((dy, dx, dk, hop))
    key = lambda f: (f[3] is None, (f[0] * 5 + f[1] * 3 + f[2] * 7) % 11)
    return sorted(out, key=key)


def back_kernel(src_ref, out_ref, relay, own, send_sem, recv_sem, hop_send, hop_recv, own_sem):
    r, z, y, x, k = place()

    def row(dy, dx, dk):
        return (((y + dy) % 4) * 4 + (x + dx) % 4) * 2 + (k + dk) % 2

    flows = routes()
    hops = [f for f in flows if f[3] is not None]
    direct = [f for f in flows if f[3] is None]
    greet([((r + s) % 32, z) for s in range(1, 32)])
    first, final = [], []
    for i, (dy, dx, dk, (hy, hx)) in enumerate(hops):
        copy = remote(src_ref.at[row(dy, dx, dk)], relay.at[i], hop_send.at[i], hop_recv.at[i], (row(hy, hx, 0), z))
        copy.start()
        first.append(copy)
    for i, (dy, dx, dk, _) in enumerate(direct):
        copy = remote(src_ref.at[row(dy, dx, dk)], out_ref.at[r], send_sem.at[i], recv_sem.at[i], (row(dy, dx, dk), z))
        copy.start()
        final.append(copy)
    take = pltpu.make_async_copy(src_ref.at[r], own, own_sem)
    take.start()
    take.wait()
    put = pltpu.make_async_copy(own, out_ref.at[r], own_sem)
    put.start()
    for i, (dy, dx, dk, (hy, hx)) in enumerate(hops):
        first[i].wait_recv()
        n = len(direct) + i
        copy = remote(relay.at[i], out_ref.at[row(-hy, -hx, 0)], send_sem.at[n], recv_sem.at[n],
                      (row(dy - hy, dx - hx, dk), z))
        copy.start()
        final.append(copy)
    put.wait()
    for copy in first:
        copy.wait_send()
    for copy in final:
        copy.wait()


def compact_kernel(slot_ref, src_ref, out_ref, wide, stage):
    def widen(i, _):
        wide[pl.ds(pl.multiple_of(i * CAP, 8), CAP), :] = src_ref[i].astype(F32)
        return 0

    lax.fori_loop(0, 32, widen, 0)

    def some(j, _):
        a, col = j // 8, lax.rem(j, 8) * 16
        h, zz, jj = lax.rem(a, 8) // 4, a // 8, lax.rem(a, 4)
        base = h * 2048 + zz * 512 + jj * 128 + col
        for i in range(16):
            stage[pl.ds(base + i, 1), :] = wide[pl.ds(slot_ref[a, col + i], 1), :]
        return 0

    lax.fori_loop(0, 256, some, 0)

    def narrow(i, _):
        rows = pl.ds(pl.multiple_of(i * 256, 256), 256)
        out_ref[rows, :] = stage[rows, :].astype(BF)
        return 0

    lax.fori_loop(0, 16, narrow, 0)


def spread_kernel(src_ref, out_ref, relay, send_sem, relay_send, relay_recv, recv_sem, pass_send, pass_recv,
                  own_send, own_recv, own_sem, bounce):
    r, z, y, x, k = place()
    base = r - k
    other = (base + 1 - k, z)
    up, down = (z + 1) % 4, (z + 3) % 4
    holder = z // 2

    def part(i):
        return pl.ds(1024 * i, 1024)

    mine = part(0) if False else pl.ds(pl.multiple_of(1024 * k, 1024), 1024)
    theirs = pl.ds(pl.multiple_of(1024 * (1 - k), 1024), 1024)
    peers = [(base + 1 - k, z)]
    for kk in range(2):
        for s in (1, 3):
            peers.append((base + kk, (z + s) % 4))
    greet(peers)

    def far(h, half):
        step = 1 if half == 0 else 3
        return remote(src_ref.at[h, part(half)], relay, relay_send, relay_recv, (base + half, (z + step) % 4))

    def near(h, half, step):
        return remote(src_ref.at[h, part(half)], out_ref.at[z, part(half)],
                      send_sem.at[step // 2, half], recv_sem.at[step // 2], (base + half, (z + step) % 4))

    def own(h):
        return remote(src_ref.at[h], out_ref.at[z], own_send, own_recv, other)

    def inner(h):
        return (pltpu.make_async_copy(src_ref.at[h], bounce, own_sem),
                pltpu.make_async_copy(bounce, out_ref.at[z], own_sem))

    dist = [(2 * k + h - z) % 4 for h in range(2)]
    for h in range(2):
        @pl.when(dist[h] == 2)
        def _():
            for half in range(2):
                remote(src_ref.at[h, part(half)], relay, relay_send.at[half], relay_recv,
                       (base + half, up if half == 0 else down)).start()

    for h in range(2):
        for step in (1, 3):
            @pl.when(dist[h] == step)
            def _():
                for half in range(2):
                    near(h, half, step).start()

        @pl.when(dist[h] == 0)
        def _():
            own(h).start()
            take, put = inner(h)
            take.start()
            take.wait()
            put.start()

    back = jnp.where(k == 0, down, up)
    ahead = jnp.where(k == 0, up, down)
    relayed = remote(relay, out_ref.at[back, mine], pass_send.at[3], recv_sem.at[2], (r, ahead))
    remote(src_ref.at[0, part(0)], relay, relay_send.at[0], relay_recv, (r, ahead)).wait_recv()
    relayed.start()
    passed = []
    for i, source in enumerate((down, up, (z + 2) % 4)):
        got = out_ref.at[source, mine]
        remote(got, got, send_sem.at[0, 0], recv_sem.at[i], other).wait_recv()
        copy = remote(got, got, pass_send.at[i], pass_recv.at[i], other)
        copy.start()
        passed.append(copy)

    for i, copy in enumerate(passed):
        copy.wait_send()
        source = (down, up, (z + 2) % 4)[i]
        remote(out_ref.at[source, theirs], out_ref.at[source, theirs], pass_send.at[i], pass_recv.at[i],
               other).wait_recv()
    relayed.wait_send()

    for h in range(2):
        @pl.when(dist[h] == 2)
        def _():
            for half in range(2):
                remote(src_ref.at[h, part(half)], relay, relay_send.at[half], relay_recv,
                       (base + half, up if half == 0 else down)).wait_send()
        for step in (1, 3):
            @pl.when(dist[h] == step)
            def _():
                for half in range(2):
                    near(h, half, step).wait_send()

        @pl.when(dist[h] == 0)
        def _():
            own(h).wait_send()
            inner(h)[1].wait()

    @pl.when(k != holder)
    def _():
        own(0).wait_recv()


def layer_kernel(len_ref, x_ref, gain_ref, wqkv_ref, wout_ref, gain2_ref, win_hbm, wdown_hbm, out_ref,
                 nrm, qs, ke, ko, ve, vo, sc, att, win_ref, wdown_ref, sems):
    k = lax.axis_index("rows") % 2
    get_in = pltpu.make_async_copy(win_hbm, win_ref, sems.at[0])
    get_down = pltpu.make_async_copy(wdown_hbm, wdown_ref, sems.at[1])
    get_in.start()
    get_down.start()
    length = len_ref[0]
    quarters = (k, 3 - k)

    def norm(i, _):
        rows = pl.ds(pl.multiple_of(i * 256, 256), 256)
        parts = [x_ref[c, rows, :].astype(F32) for c in range(4)]
        square = parts[0] * parts[0]
        for part in parts[1:]:
            square = square + part * part
        scale = lax.rsqrt(jnp.sum(square, axis=1, keepdims=True) * (1.0 / D) + 1e-6)
        for c in range(4):
            nrm[rows, 128 * c : 128 * c + 128] = (parts[c] * scale * gain_ref[:, 128 * c : 128 * c + 128]).astype(BF)
        return 0

    lax.fori_loop(0, 8, norm, 0)

    def project(i, _):
        rows = pl.ds(pl.multiple_of(i * 256, 256), 256)
        here = nrm[rows, :]
        keys = dot(here, wqkv_ref[:, D : 2 * D])
        vals = dot(here, wqkv_ref[:, 2 * D :])
        lane = lax.broadcasted_iota(jnp.int32, (256, 128), 1)
        pos = lax.broadcasted_iota(jnp.int32, (256, 128), 0) + i * 256
        bias = jnp.where(pos < length, 0.0, NEG)
        for c in range(4):
            cols = slice(128 * c, 128 * c + 128)
            ke[rows, cols] = jnp.where(lane == 64, bias, keys[:, cols]).astype(BF)
            ko[rows, cols] = jnp.where(lane == 0, bias, keys[:, cols]).astype(BF)
            ve[rows, cols] = jnp.where(lane == 64, 1.0, vals[:, cols]).astype(BF)
            vo[rows, cols] = jnp.where(lane == 0, 1.0, vals[:, cols]).astype(BF)
        return 0

    lax.fori_loop(0, 8, project, 0)
    for a in range(2):
        rows = pl.ds(pl.multiple_of(quarters[a] * 512, 512), 512)
        qs[512 * a : 512 * a + 512, :] = (dot(nrm[rows, :], wqkv_ref[:, :D]) * (0.125 * LOG2E)).astype(BF)

    def attend(kk):
        def heads(hp, _):
            cols = pl.ds(pl.multiple_of(hp * 128, 128), 128)
            lane = lax.broadcasted_iota(jnp.int32, (256, 128), 1)
            tri = (lax.broadcasted_iota(jnp.int32, (256, 256), 1)
                   <= lax.broadcasted_iota(jnp.int32, (256, 256), 0))
            for a, quarter in enumerate((kk, 3 - kk)):
                for j in range(2):
                    n = 2 * quarter + j + 1
                    at = 512 * a + 256 * j
                    q = qs[at : at + 256, cols].astype(F32)
                    accs = []
                    for odd in range(2):
                        kref, vref = (ko, vo) if odd else (ke, ve)
                        if odd:
                            qa = jnp.where(lane >= 64, q, jnp.where(lane == 0, 1.0, 0.0)).astype(BF)
                        else:
                            qa = jnp.where(lane < 64, q, jnp.where(lane == 64, 1.0, 0.0)).astype(BF)
                        top = None
                        for c in range(n):
                            s = dot_t(qa, kref[256 * c : 256 * c + 256, cols])
                            if c == n - 1:
                                s = jnp.where(tri, s, NEG)
                            sc[odd, c] = s
                            m = jnp.maximum(s[:, :128], s[:, 128:])
                            top = m if top is None else jnp.maximum(top, m)
                        top = jnp.max(top, axis=1, keepdims=True)
                        acc = jnp.zeros((256, 128), F32)
                        for c in range(n):
                            p = jnp.exp2(sc[odd, c] - top).astype(BF)
                            acc = acc + dot(p, vref[256 * c : 256 * c + 256, cols])
                        accs.append(acc)
                    even = accs[0] / accs[0][:, 64:65]
                    odd_ = accs[1] / accs[1][:, 0:1]
                    att[at : at + 256, cols] = jnp.where(lane < 64, even, odd_).astype(BF)
            return 0

        lax.fori_loop(0, 4, heads, 0)

    for kk in range(2):
        @pl.when(k == kk)
        def _():
            attend(kk)

    get_in.wait()
    get_down.wait()

    def mlp(i, _):
        rows = pl.ds(pl.multiple_of(i * 256, 256), 256)
        quarter = jnp.where(i < 2, quarters[0], quarters[1])
        src = pl.ds(pl.multiple_of(quarter * 512 + lax.rem(i, 2) * 256, 256), 256)
        resid = jnp.concatenate([x_ref[c, src, :].astype(F32) for c in range(4)], axis=1)
        hidden = (resid + dot(att[rows, :], wout_ref[...])).astype(BF).astype(F32)
        scale = lax.rsqrt(jnp.mean(hidden * hidden, axis=1, keepdims=True) + 1e-6)
        normed = (hidden * scale * gain2_ref[...]).astype(BF)
        out = hidden
        for f in range(4):
            cols = slice(512 * f, 512 * f + 512)
            up_cols = slice(FF + 512 * f, FF + 512 * f + 512)
            gate = dot(normed, win_ref[:, cols])
            up = dot(normed, win_ref[:, up_cols])
            act = (gate / (1.0 + jnp.exp(-gate)) * up).astype(BF)
            out = out + dot(act, wdown_ref[cols, :])
        out_ref[rows, :] = out.astype(BF)
        return 0

    lax.fori_loop(0, 4, mlp, 0)


def give_kernel(src_ref, out_ref, relay, bounce, send_sem, far_send, relay_recv, recv_sem, pass_send, own_sem):
    r, z, y, x, k = place()
    base = r - k
    up, down = (z + 1) % 4, (z + 3) % 4
    across = (z + 2) % 4
    holder, slot = z // 2, z % 2
    peers = [(base + 1 - k, z)]
    for kk in range(2):
        for s in (1, 3):
            peers.append((base + kk, (z + s) % 4))
    greet(peers)

    def worker(q):
        return jnp.where((q == 0) | (q == 3), 0, 1)

    def piece(q, rows=pl.ds(0, 512)):
        at = jnp.where(q < 2, 0, 1)
        return src_ref.at[at, rows]

    halves = (pl.ds(0, 256), pl.ds(256, 256))
    via = (up, down)

    def far(half):
        return remote(piece(across, halves[half]), relay, far_send.at[half], relay_recv, (r, via[half]))

    def near(i):
        return remote(piece(via[i]), out_ref.at[slot], send_sem.at[i], recv_sem.at[slot, 0], (base + holder, via[i]))

    def own():
        return remote(piece(z), out_ref.at[slot], send_sem.at[2], recv_sem.at[slot, 0], (base + 1 - k, z))

    @pl.when(worker(across) == k)
    def _():
        far(0).start()
        far(1).start()

    for i in range(2):
        @pl.when(worker(via[i]) == k)
        def _():
            near(i).start()

    @pl.when((worker(z) == k) & (holder != k))
    def _():
        own().start()

    @pl.when((worker(z) == k) & (holder == k))
    def _():
        take = pltpu.make_async_copy(piece(z), bounce, own_sem)
        take.start()
        take.wait()
        put = pltpu.make_async_copy(bounce, out_ref.at[slot], own_sem)
        put.start()
        put.wait()

    def passing(half):
        source, target = (down, up) if half == 0 else (up, down)
        return remote(relay, out_ref.at[source % 2, halves[half]], pass_send, recv_sem.at[source % 2, half],
                      (base + source // 2, target))

    for half in range(2):
        @pl.when(worker(via[half]) == k)
        def _():
            far(half).wait_recv()
            passing(half).start()
            passing(half).wait_send()

    for h in range(2):
        source = 2 * k + h
        dist = (source - z) % 4
        @pl.when((dist == 1) | (dist == 3) | ((dist == 0) & (worker(z) != k)))
        def _():
            remote(src_ref.at[0], out_ref.at[h], send_sem.at[0], recv_sem.at[h, 0], (base + 1 - k, z)).wait_recv()
        @pl.when(dist == 2)
        def _():
            for half in range(2):
                remote(src_ref.at[0, halves[half]], out_ref.at[h, halves[half]], send_sem.at[0],
                       recv_sem.at[h, half], (base + 1 - k, z)).wait_recv()

    @pl.when(worker(across) == k)
    def _():
        far(0).wait_send()
        far(1).wait_send()

    for i in range(2):
        @pl.when(worker(via[i]) == k)
        def _():
            near(i).wait_send()

    @pl.when((worker(z) == k) & (holder != k))
    def _():
        own().wait_send()


def local(token_ids, lengths, table, attn_gain, w_qkv, w_out, mlp_gain, w_in, w_down):
    dma = pltpu.SemaphoreType.DMA
    ids = pl.pallas_call(
        ids_kernel,
        out_shape=jax.ShapeDtypeStruct((4, 8, 128), jnp.int32),
        in_specs=[VM], out_specs=VM,
        scratch_shapes=[dma((3,)), dma((3,))],
        compiler_params=params(1),
    )(token_ids.reshape(8, 128))
    msg, slot = pl.pallas_call(
        request_kernel,
        out_shape=[jax.ShapeDtypeStruct((32, 4, 128), jnp.int32), jax.ShapeDtypeStruct((32, 128), jnp.int32)],
        in_specs=[SM, VM], out_specs=[VM, VM],
        compiler_params=params(),
    )(lengths, ids.reshape(32, 128))
    asked = pl.pallas_call(
        ask_kernel,
        out_shape=jax.ShapeDtypeStruct((32, 4, 128), jnp.int32),
        in_specs=[VM], out_specs=VM,
        scratch_shapes=[dma((31,)), dma((31,))],
        compiler_params=params(2),
    )(msg)
    looked = pl.pallas_call(
        lookup_kernel,
        out_shape=jax.ShapeDtypeStruct((32, CAP, 128), BF),
        in_specs=[SM, VM], out_specs=VM,
        scratch_shapes=[pltpu.VMEM((16384, 128), F32), pltpu.VMEM((352, 128), F32)],
        compiler_params=params(),
    )(asked, table)
    returned = pl.pallas_call(
        back_kernel,
        out_shape=jax.ShapeDtypeStruct((32, CAP, 128), BF),
        in_specs=[ANY], out_specs=ANY,
        scratch_shapes=[pltpu.VMEM((14, CAP, 128), BF), pltpu.VMEM((CAP, 128), BF), dma((31,)), dma((31,)),
                        dma((14,)), dma((14,)), dma],
        compiler_params=params(3),
    )(looked)
    embedded = pl.pallas_call(
        compact_kernel,
        out_shape=jax.ShapeDtypeStruct((4096, 128), BF),
        in_specs=[SM, VM], out_specs=VM,
        scratch_shapes=[pltpu.VMEM((32 * CAP, 128), F32), pltpu.VMEM((4096, 128), F32)],
        compiler_params=params(),
    )(slot, returned)
    full = pl.pallas_call(
        spread_kernel,
        out_shape=jax.ShapeDtypeStruct((4, 2048, 128), BF),
        in_specs=[ANY], out_specs=ANY,
        scratch_shapes=[pltpu.VMEM((1024, 128), BF), dma((2, 2)), dma((2,)), dma, dma((3,)), dma((4,)), dma((3,)),
                        dma, dma, dma, pltpu.VMEM((2048, 128), BF)],
        compiler_params=params(4),
    )(embedded.reshape(2, 2048, 128))
    r, z = lax.axis_index("rows"), lax.axis_index("cols")
    length = lax.dynamic_slice(asked, (r - r % 2 + z // 2, 3, 1 + z % 2), (1, 1, 1)).reshape(1)
    done = pl.pallas_call(
        layer_kernel,
        out_shape=jax.ShapeDtypeStruct((1024, D), BF),
        in_specs=[SM, VM, VM, VM, VM, VM, ANY, ANY], out_specs=VM,
        scratch_shapes=[pltpu.VMEM((2048, D), BF), pltpu.VMEM((1024, D), BF)]
        + [pltpu.VMEM((2048, D), BF)] * 4
        + [pltpu.VMEM((2, 8, 256, 256), F32), pltpu.VMEM((1024, D), BF),
           pltpu.VMEM((D, 2 * FF), BF), pltpu.VMEM((FF, D), BF), dma((2,))],
        compiler_params=params(),
    )(length, full, attn_gain.reshape(1, D), w_qkv, w_out, mlp_gain.reshape(1, D), w_in, w_down)
    return pl.pallas_call(
        give_kernel,
        out_shape=jax.ShapeDtypeStruct((2, 512, D), BF),
        in_specs=[ANY], out_specs=ANY,
        scratch_shapes=[pltpu.VMEM((256, D), BF), pltpu.VMEM((512, D), BF), dma((3,)), dma((2,)), dma, dma((2, 2)),
                        dma, dma],
        compiler_params=params(5),
    )(done.reshape(2, 512, D))


def solution(mesh):
    in_specs = (P("rows", "cols"), P("rows"), P("rows", "cols"), P(), P(), P(), P(), P(), P())
    return jax.shard_map(local, mesh=mesh, in_specs=in_specs, out_specs=P("rows", "cols", None), check_vma=False)
```

```python
import functools

import jax
import jax.numpy as jnp
from jax import lax
from jax.experimental import pallas as pl
from jax.experimental.pallas import tpu as pltpu
from jax.sharding import PartitionSpec as P

D = 512
FF = 2048
CAP = 344
BF = jnp.bfloat16
F32 = jnp.float32
MESH = pl.DeviceIdType.MESH
ANY = pl.BlockSpec(memory_space=pl.ANY)
VM = pl.BlockSpec(memory_space=pltpu.VMEM)
SM = pl.BlockSpec(memory_space=pltpu.SMEM)
LOG2E = 1.4426950408889634
NEG = -1e30


def dot(a, b):
    return jnp.dot(a, b, preferred_element_type=F32)


def dot_t(a, b):
    return lax.dot_general(a, b, (((1,), (1,)), ((), ())), preferred_element_type=F32)


def place():
    r, z = lax.axis_index("rows"), lax.axis_index("cols")
    return r, z, r // 8, (r // 2) % 4, r % 2


def greet(devices):
    barrier = pltpu.get_barrier_semaphore()
    for device in devices:
        pl.semaphore_signal(barrier, inc=1, device_id=device, device_id_type=MESH)
    pl.semaphore_wait(barrier, len(devices))


def remote(src, dst, send_sem, recv_sem, device):
    return pltpu.make_async_remote_copy(
        src_ref=src, dst_ref=dst, send_sem=send_sem, recv_sem=recv_sem,
        device_id=device, device_id_type=MESH)


def params(collective_id=None, vmem=60):
    kw = {}
    if collective_id is not None:
        kw = dict(collective_id=collective_id, has_side_effects=True)
    return pltpu.CompilerParams(vmem_limit_bytes=vmem * 2**20, **kw)


def ask_kernel(len_ref, mine_ref, out_ref, slot_ref, ids_ref, msg_ref, ids_send, ids_recv, send_sem, recv_sem):
    r, z, _, _, _ = place()
    near = [(r, (z + s) % 4) for s in (1, 2, 3)]
    peers = [((r + s) % 32, z) for s in range(1, 32)]
    greet(near + peers)
    copies = []
    for s, device in enumerate(near):
        copy = remote(mine_ref, ids_ref.at[z], ids_send.at[s], ids_recv.at[s], device)
        copy.start()
        copies.append(copy)
    ids_ref[z] = mine_ref[...]
    before = (lax.broadcasted_iota(jnp.int32, (128, 128), 0)
              < lax.broadcasted_iota(jnp.int32, (128, 128), 1)).astype(F32)
    above = (lax.broadcasted_iota(jnp.int32, (32, 32), 1)
             < lax.broadcasted_iota(jnp.int32, (32, 32), 0)).astype(F32).astype(BF)
    both = jnp.concatenate([before, jnp.ones((128, 128), F32)], axis=0).astype(BF)
    owners = lax.broadcasted_iota(jnp.int32, (32, 128), 0)
    ks = lax.broadcasted_iota(jnp.int32, (384, 128), 0)
    lane = lax.broadcasted_iota(jnp.int32, (32, 128), 1)
    for copy in copies:
        copy.wait()
    ids = ids_ref[...].reshape(32, 128)
    owner = ids >> 14
    low, high = (ids & 127).astype(F32), ((ids >> 7) & 127).astype(F32)
    ones = [jnp.where(owner == o, 1.0, 0.0).astype(BF) for o in range(32)]
    rows_above = dot(above, jnp.concatenate(ones, axis=1)).astype(BF)
    prior = dot(
        jnp.concatenate(
            [jnp.concatenate(ones, axis=0),
             jnp.concatenate([rows_above[:, 128 * o : 128 * o + 128] for o in range(32)], axis=0)], axis=1),
        both)
    rank = jnp.zeros((32, 128), F32)
    for o in range(32):
        rank = rank + jnp.where(owner == o, prior[32 * o : 32 * o + 32], 0.0)
    rank_i = rank.astype(jnp.int32)
    acc = jnp.zeros((64, 384), F32)
    count = jnp.zeros((32, 128), F32)
    for a in range(0, 32, 2):
        lefts, rights = [], []
        for b in (a, a + 1):
            hit = owners == owner[b : b + 1, :]
            count = count + jnp.where(hit, 1.0, 0.0)
            lefts.append(jnp.concatenate(
                [jnp.where(hit, low[b : b + 1, :], 0.0), jnp.where(hit, high[b : b + 1, :], 0.0)], axis=0).astype(BF))
            rights.append(jnp.where(ks == rank_i[b : b + 1, :], 1.0, 0.0).astype(BF))
        acc = acc + dot_t(jnp.concatenate(lefts, axis=1), jnp.concatenate(rights, axis=1))
    req = (acc[32:] * 128.0 + acc[:32]).astype(jnp.int32)
    for j in range(3):
        msg_ref[:, j, :] = req[:, 128 * j : 128 * j + 128]
    tail = jnp.where(lane == 1, len_ref[0], jnp.where(lane == 2, len_ref[1], 0))
    msg_ref[:, 3, :] = tail
    slot_ref[...] = owner * CAP + rank_i
    copies = []
    for s, device in enumerate(peers):
        copy = remote(msg_ref.at[device[0]], out_ref.at[r], send_sem.at[s], recv_sem.at[s], device)
        copy.start()
        copies.append(copy)
    out_ref[r] = msg_ref[r]
    for copy in copies:
        copy.wait()


def routes():
    out = []
    for dy in range(4):
        for dx in range(4):
            for dk in range(2):
                if dx == dy == dk == 0:
                    continue
                side = 1 if dk == 0 else 3
                hop = None
                if dx == 2 or dy == 2:
                    hop = (side if dy == 2 else 0, side if dx == 2 else 0)
                out.append((dy, dx, dk, hop))
    key = lambda f: (f[3] is None, (f[0] * 5 + f[1] * 3 + f[2] * 7) % 11)
    return sorted(out, key=key)


def lookup_kernel(asked_ref, table_ref, out_ref, wide, stage, block, relay, send_sem, recv_sem, hop_send, hop_recv):
    r, z, y, x, k = place()

    def row(dy, dx, dk):
        return (((y + dy) % 4) * 4 + (x + dx) % 4) * 2 + (k + dk) % 2

    flows = routes()
    hops = [f for f in flows if f[3] is not None]
    direct = [f for f in flows if f[3] is None]
    barrier = pltpu.get_barrier_semaphore()
    for s in range(1, 32):
        pl.semaphore_signal(barrier, inc=1, device_id=((r + s) % 32, z), device_id_type=MESH)

    def widen(i, _):
        rows = pl.ds(pl.multiple_of(i * 256, 256), 256)
        wide[rows, :] = table_ref[rows, :].astype(F32)
        return 0

    lax.fori_loop(0, 64, widen, 0)
    pl.semaphore_wait(barrier, 31)

    def fill(p, dst):
        def some(j, _):
            base = j * 43
            for i in range(43):
                at = base + i
                stage[pl.ds(at, 1), :] = wide[pl.ds(asked_ref[p, at // 128, lax.rem(at, 128)], 1), :]
            return 0

        lax.fori_loop(0, 8, some, 0)
        dst[...] = stage[...].astype(BF)

    first, final, waiting = [], [], None
    for n, (dy, dx, dk, hop) in enumerate(hops + direct):
        p = row(dy, dx, dk)
        fill(p, block.at[n])
        if hop is not None:
            copy = remote(block.at[n], relay.at[n], hop_send.at[n], hop_recv.at[n], (row(*hop, 0), z))
            first.append(copy)
        else:
            i = n - len(hops)
            copy = remote(block.at[n], out_ref.at[r], send_sem.at[i], recv_sem.at[i], (p, z))
            final.append(copy)
        if waiting is not None:
            waiting.start()
        waiting = copy
    fill(r, out_ref.at[r])
    waiting.start()
    for i, (dy, dx, dk, (hy, hx)) in enumerate(hops):
        first[i].wait_recv()
        n = len(direct) + i
        copy = remote(relay.at[i], out_ref.at[row(-hy, -hx, 0)], send_sem.at[n], recv_sem.at[n],
                      (row(dy - hy, dx - hx, dk), z))
        copy.start()
        final.append(copy)
    for copy in first:
        copy.wait_send()
    for copy in final:
        copy.wait()


def spread_kernel(slot_ref, back_ref, out_ref, wide, stage, emb, relay, send_sem, relay_send, relay_recv, recv_sem,
                  pass_send, pass_recv, own_send, own_recv):
    r, z, y, x, k = place()
    base = r - k
    other = (base + 1 - k, z)
    up, down = (z + 1) % 4, (z + 3) % 4
    holder = z // 2
    mine = pl.ds(pl.multiple_of(1024 * k, 1024), 1024)
    theirs = pl.ds(pl.multiple_of(1024 * (1 - k), 1024), 1024)
    peers = [(base + 1 - k, z)]
    for kk in range(2):
        for s in (1, 3):
            peers.append((base + kk, (z + s) % 4))
    barrier = pltpu.get_barrier_semaphore()
    for device in peers:
        pl.semaphore_signal(barrier, inc=1, device_id=device, device_id_type=MESH)

    def widen(i, _):
        wide[pl.ds(pl.multiple_of(i * CAP, 8), CAP), :] = back_ref[i].astype(F32)
        return 0

    lax.fori_loop(0, 32, widen, 0)
    pl.semaphore_wait(barrier, len(peers))

    def part(i):
        return pl.ds(1024 * i, 1024)

    def far(h, half):
        return remote(emb.at[h, part(half)], relay, relay_send.at[half], relay_recv,
                      (base + half, up if half == 0 else down))

    def near(h, half, step):
        return remote(emb.at[h, part(half)], out_ref.at[z, part(half)],
                      send_sem.at[step // 2, half], recv_sem.at[step // 2], (base + half, (z + step) % 4))

    def own(h, half):
        return remote(emb.at[h, part(half)], out_ref.at[z, part(half)], own_send.at[half], own_recv.at[half], other)

    def send(h, half, act):
        dist = (2 * k + h - z) % 4

        @pl.when(dist == 2)
        def _():
            act(far(h, half))

        for step in (1, 3):
            @pl.when(dist == step)
            def _():
                act(near(h, half, step))

        @pl.when(dist == 0)
        def _():
            act(own(h, half))

    lead = jnp.where((2 * k - z) % 4 < 2, 1, 0)
    pieces = [(h, half) for h in (lead, 1 - lead) for half in range(2)]
    waiting = None
    for h, half in pieces:
        def gather(j, _):
            a = (half * 2 + j // 4) * 8 + h * 4 + lax.rem(j, 4)
            for i in range(128):
                stage[pl.ds(j * 128 + i, 1), :] = wide[pl.ds(slot_ref[a, i], 1), :]
            return 0

        lax.fori_loop(0, 8, gather, 0)
        emb[h, part(half), :] = stage[...].astype(BF)

        @pl.when((2 * k + h - z) % 4 == 0)
        def _():
            out_ref[z, part(half), :] = stage[...].astype(BF)

        if waiting is not None:
            send(*waiting, lambda copy: copy.start())
        waiting = (h, half)
    send(*waiting, lambda copy: copy.start())

    behind = jnp.where(k == 0, down, up)
    ahead = jnp.where(k == 0, up, down)
    relayed = remote(relay, out_ref.at[behind, mine], pass_send.at[3], recv_sem.at[2], (r, ahead))
    far(0, 0).wait_recv()
    relayed.start()
    passed = []
    for i, source in enumerate((down, up, (z + 2) % 4)):
        got = out_ref.at[source, mine]
        remote(got, got, pass_send.at[i], recv_sem.at[i], other).wait_recv()
        copy = remote(got, got, pass_send.at[i], pass_recv.at[i], other)
        copy.start()
        passed.append(copy)

    for i, source in enumerate((down, up, (z + 2) % 4)):
        passed[i].wait_send()
        got = out_ref.at[source, theirs]
        remote(got, got, pass_send.at[i], pass_recv.at[i], other).wait_recv()
    relayed.wait_send()
    for h, half in pieces:
        send(h, half, lambda copy: copy.wait_send())

    @pl.when(k != holder)
    def _():
        for half in range(2):
            own(0, half).wait_recv()


def layer_kernel(len_ref, x_ref, gain_ref, wqkv_ref, wout_ref, gain2_ref, win_hbm, wdown_hbm, out_ref,
                 nrm, qs, ke, ko, ve, vo, sc, att, win_ref, wdown_ref, sems):
    k = lax.axis_index("rows") % 2
    get_in = pltpu.make_async_copy(win_hbm, win_ref, sems.at[0])
    get_down = pltpu.make_async_copy(wdown_hbm, wdown_ref, sems.at[1])
    get_in.start()
    get_down.start()
    length = len_ref[0]
    quarters = (k, 3 - k)

    def norm(i, _):
        rows = pl.ds(pl.multiple_of(i * 256, 256), 256)
        parts = [x_ref[c, rows, :].astype(F32) for c in range(4)]
        square = parts[0] * parts[0]
        for part in parts[1:]:
            square = square + part * part
        scale = lax.rsqrt(jnp.sum(square, axis=1, keepdims=True) * (1.0 / D) + 1e-6)
        for c in range(4):
            nrm[rows, 128 * c : 128 * c + 128] = (parts[c] * scale * gain_ref[:, 128 * c : 128 * c + 128]).astype(BF)
        return 0

    lax.fori_loop(0, 8, norm, 0)

    def project(i, _):
        rows = pl.ds(pl.multiple_of(i * 256, 256), 256)
        here = nrm[rows, :]
        keys = dot(here, wqkv_ref[:, D : 2 * D])
        vals = dot(here, wqkv_ref[:, 2 * D :])
        lane = lax.broadcasted_iota(jnp.int32, (256, 128), 1)
        pos = lax.broadcasted_iota(jnp.int32, (256, 128), 0) + i * 256
        bias = jnp.where(pos < length, 0.0, NEG)
        for c in range(4):
            cols = slice(128 * c, 128 * c + 128)
            ke[rows, cols] = jnp.where(lane == 64, bias, keys[:, cols]).astype(BF)
            ko[rows, cols] = jnp.where(lane == 0, bias, keys[:, cols]).astype(BF)
            ve[rows, cols] = jnp.where(lane == 64, 1.0, vals[:, cols]).astype(BF)
            vo[rows, cols] = jnp.where(lane == 0, 1.0, vals[:, cols]).astype(BF)
        return 0

    lax.fori_loop(0, 8, project, 0)
    for a in range(2):
        rows = pl.ds(pl.multiple_of(quarters[a] * 512, 512), 512)
        qs[512 * a : 512 * a + 512, :] = (dot(nrm[rows, :], wqkv_ref[:, :D]) * (0.125 * LOG2E)).astype(BF)

    def attend(kk):
        def heads(hp, _):
            cols = pl.ds(pl.multiple_of(hp * 128, 128), 128)
            lane = lax.broadcasted_iota(jnp.int32, (256, 128), 1)
            tri = (lax.broadcasted_iota(jnp.int32, (256, 256), 1)
                   <= lax.broadcasted_iota(jnp.int32, (256, 256), 0))
            for a, quarter in enumerate((kk, 3 - kk)):
                for j in range(2):
                    n = 2 * quarter + j + 1
                    at = 512 * a + 256 * j
                    q = qs[at : at + 256, cols].astype(F32)
                    accs = []
                    for odd in range(2):
                        kref, vref = (ko, vo) if odd else (ke, ve)
                        if odd:
                            qa = jnp.where(lane >= 64, q, jnp.where(lane == 0, 1.0, 0.0)).astype(BF)
                        else:
                            qa = jnp.where(lane < 64, q, jnp.where(lane == 64, 1.0, 0.0)).astype(BF)
                        top = None
                        for c in range(n):
                            s = dot_t(qa, kref[256 * c : 256 * c + 256, cols])
                            if c == n - 1:
                                s = jnp.where(tri, s, NEG)
                            sc[odd, c] = s
                            m = jnp.maximum(s[:, :128], s[:, 128:])
                            top = m if top is None else jnp.maximum(top, m)
                        top = jnp.max(top, axis=1, keepdims=True)
                        acc = jnp.zeros((256, 128), F32)
                        for c in range(n):
                            p = jnp.exp2(sc[odd, c] - top).astype(BF)
                            acc = acc + dot(p, vref[256 * c : 256 * c + 256, cols])
                        accs.append(acc)
                    even = accs[0] / accs[0][:, 64:65]
                    odd_ = accs[1] / accs[1][:, 0:1]
                    att[at : at + 256, cols] = jnp.where(lane < 64, even, odd_).astype(BF)
            return 0

        lax.fori_loop(0, 4, heads, 0)

    for kk in range(2):
        @pl.when(k == kk)
        def _():
            attend(kk)

    get_in.wait()
    get_down.wait()

    def mlp(i, _):
        rows = pl.ds(pl.multiple_of(i * 256, 256), 256)
        quarter = jnp.where(i < 2, quarters[0], quarters[1])
        src = pl.ds(pl.multiple_of(quarter * 512 + lax.rem(i, 2) * 256, 256), 256)
        resid = jnp.concatenate([x_ref[c, src, :].astype(F32) for c in range(4)], axis=1)
        hidden = (resid + dot(att[rows, :], wout_ref[...])).astype(BF).astype(F32)
        scale = lax.rsqrt(jnp.mean(hidden * hidden, axis=1, keepdims=True) + 1e-6)
        normed = (hidden * scale * gain2_ref[...]).astype(BF)
        out = hidden
        for f in range(4):
            cols = slice(512 * f, 512 * f + 512)
            up_cols = slice(FF + 512 * f, FF + 512 * f + 512)
            gate = dot(normed, win_ref[:, cols])
            up = dot(normed, win_ref[:, up_cols])
            act = (gate / (1.0 + jnp.exp(-gate)) * up).astype(BF)
            out = out + dot(act, wdown_ref[cols, :])
        out_ref[rows, :] = out.astype(BF)
        return 0

    lax.fori_loop(0, 4, mlp, 0)


def give_kernel(src_ref, out_ref, relay, bounce, send_sem, far_send, relay_recv, recv_sem, pass_send, own_sem):
    r, z, y, x, k = place()
    base = r - k
    up, down = (z + 1) % 4, (z + 3) % 4
    across = (z + 2) % 4
    holder, slot = z // 2, z % 2
    peers = [(base + 1 - k, z)]
    for kk in range(2):
        for s in (1, 3):
            peers.append((base + kk, (z + s) % 4))
    greet(peers)

    def worker(q):
        return jnp.where((q == 0) | (q == 3), 0, 1)

    def piece(q, rows=pl.ds(0, 512)):
        at = jnp.where(q < 2, 0, 1)
        return src_ref.at[at, rows]

    halves = (pl.ds(0, 256), pl.ds(256, 256))
    via = (up, down)

    def far(half):
        return remote(piece(across, halves[half]), relay, far_send.at[half], relay_recv, (r, via[half]))

    def near(i):
        return remote(piece(via[i]), out_ref.at[slot], send_sem.at[i], recv_sem.at[slot, 0], (base + holder, via[i]))

    def own():
        return remote(piece(z), out_ref.at[slot], send_sem.at[2], recv_sem.at[slot, 0], (base + 1 - k, z))

    @pl.when(worker(across) == k)
    def _():
        far(0).start()
        far(1).start()

    for i in range(2):
        @pl.when(worker(via[i]) == k)
        def _():
            near(i).start()

    @pl.when((worker(z) == k) & (holder != k))
    def _():
        own().start()

    @pl.when((worker(z) == k) & (holder == k))
    def _():
        take = pltpu.make_async_copy(piece(z), bounce, own_sem)
        take.start()
        take.wait()
        put = pltpu.make_async_copy(bounce, out_ref.at[slot], own_sem)
        put.start()
        put.wait()

    def passing(half):
        source, target = (down, up) if half == 0 else (up, down)
        return remote(relay, out_ref.at[source % 2, halves[half]], pass_send, recv_sem.at[source % 2, half],
                      (base + source // 2, target))

    for half in range(2):
        @pl.when(worker(via[half]) == k)
        def _():
            far(half).wait_recv()
            passing(half).start()
            passing(half).wait_send()

    for h in range(2):
        source = 2 * k + h
        dist = (source - z) % 4
        @pl.when((dist == 1) | (dist == 3) | ((dist == 0) & (worker(z) != k)))
        def _():
            remote(src_ref.at[0], out_ref.at[h], send_sem.at[0], recv_sem.at[h, 0], (base + 1 - k, z)).wait_recv()
        @pl.when(dist == 2)
        def _():
            for half in range(2):
                remote(src_ref.at[0, halves[half]], out_ref.at[h, halves[half]], send_sem.at[0],
                       recv_sem.at[h, half], (base + 1 - k, z)).wait_recv()

    @pl.when(worker(across) == k)
    def _():
        far(0).wait_send()
        far(1).wait_send()

    for i in range(2):
        @pl.when(worker(via[i]) == k)
        def _():
            near(i).wait_send()

    @pl.when((worker(z) == k) & (holder != k))
    def _():
        own().wait_send()


def local(token_ids, lengths, table, attn_gain, w_qkv, w_out, mlp_gain, w_in, w_down):
    dma = pltpu.SemaphoreType.DMA
    asked, slot = pl.pallas_call(
        ask_kernel,
        out_shape=[jax.ShapeDtypeStruct((32, 4, 128), jnp.int32), jax.ShapeDtypeStruct((32, 128), jnp.int32)],
        in_specs=[SM, VM], out_specs=[VM, VM],
        scratch_shapes=[pltpu.VMEM((4, 8, 128), jnp.int32), pltpu.VMEM((32, 4, 128), jnp.int32),
                        dma((3,)), dma((3,)), dma((31,)), dma((31,))],
        compiler_params=params(1),
    )(lengths, token_ids.reshape(8, 128))
    returned = pl.pallas_call(
        lookup_kernel,
        out_shape=jax.ShapeDtypeStruct((32, CAP, 128), BF),
        in_specs=[SM, VM], out_specs=VM,
        scratch_shapes=[pltpu.VMEM((16384, 128), F32), pltpu.VMEM((CAP, 128), F32), pltpu.VMEM((31, CAP, 128), BF),
                        pltpu.VMEM((14, CAP, 128), BF), dma((31,)), dma((31,)), dma((14,)), dma((14,))],
        compiler_params=params(2),
    )(asked, table)
    full = pl.pallas_call(
        spread_kernel,
        out_shape=jax.ShapeDtypeStruct((4, 2048, 128), BF),
        in_specs=[SM, VM], out_specs=VM,
        scratch_shapes=[pltpu.VMEM((32 * CAP, 128), F32), pltpu.VMEM((1024, 128), F32), pltpu.VMEM((2, 2048, 128), BF),
                        pltpu.VMEM((1024, 128), BF), dma((2, 2)), dma((2,)), dma, dma((3,)), dma((4,)), dma((3,)),
                        dma((2,)), dma((2,))],
        compiler_params=params(3),
    )(slot, returned)
    r, z = lax.axis_index("rows"), lax.axis_index("cols")
    length = lax.dynamic_slice(asked, (r - r % 2 + z // 2, 3, 1 + z % 2), (1, 1, 1)).reshape(1)
    done = pl.pallas_call(
        layer_kernel,
        out_shape=jax.ShapeDtypeStruct((1024, D), BF),
        in_specs=[SM, VM, VM, VM, VM, VM, ANY, ANY], out_specs=VM,
        scratch_shapes=[pltpu.VMEM((2048, D), BF), pltpu.VMEM((1024, D), BF)]
        + [pltpu.VMEM((2048, D), BF)] * 4
        + [pltpu.VMEM((2, 8, 256, 256), F32), pltpu.VMEM((1024, D), BF),
           pltpu.VMEM((D, 2 * FF), BF), pltpu.VMEM((FF, D), BF), dma((2,))],
        compiler_params=params(),
    )(length, full, attn_gain.reshape(1, D), w_qkv, w_out, mlp_gain.reshape(1, D), w_in, w_down)
    return pl.pallas_call(
        give_kernel,
        out_shape=jax.ShapeDtypeStruct((2, 512, D), BF),
        in_specs=[ANY], out_specs=ANY,
        scratch_shapes=[pltpu.VMEM((256, D), BF), pltpu.VMEM((512, D), BF), dma((3,)), dma((2,)), dma, dma((2, 2)),
                        dma, dma],
        compiler_params=params(4),
    )(done.reshape(2, 512, D))


def solution(mesh):
    in_specs = (P("rows", "cols"), P("rows"), P("rows", "cols"), P(), P(), P(), P(), P(), P())
    return jax.shard_map(local, mesh=mesh, in_specs=in_specs, out_specs=P("rows", "cols", None), check_vma=False)
```

```python
import functools

import jax
import jax.numpy as jnp
from jax import lax
from jax.experimental import pallas as pl
from jax.experimental.pallas import tpu as pltpu
from jax.sharding import PartitionSpec as P

D = 512
FF = 2048
CAP = 344
BF = jnp.bfloat16
F32 = jnp.float32
MESH = pl.DeviceIdType.MESH
ANY = pl.BlockSpec(memory_space=pl.ANY)
VM = pl.BlockSpec(memory_space=pltpu.VMEM)
SM = pl.BlockSpec(memory_space=pltpu.SMEM)
LOG2E = 1.4426950408889634
NEG = -1e30


def dot(a, b):
    return jnp.dot(a, b, preferred_element_type=F32)


def dot_t(a, b):
    return lax.dot_general(a, b, (((1,), (1,)), ((), ())), preferred_element_type=F32)


def place():
    r, z = lax.axis_index("rows"), lax.axis_index("cols")
    return r, z, r // 8, (r // 2) % 4, r % 2


def greet(devices):
    barrier = pltpu.get_barrier_semaphore()
    for device in devices:
        pl.semaphore_signal(barrier, inc=1, device_id=device, device_id_type=MESH)
    pl.semaphore_wait(barrier, len(devices))


def remote(src, dst, send_sem, recv_sem, device):
    return pltpu.make_async_remote_copy(
        src_ref=src, dst_ref=dst, send_sem=send_sem, recv_sem=recv_sem,
        device_id=device, device_id_type=MESH)


def params(collective_id=None, vmem=60):
    kw = {}
    if collective_id is not None:
        kw = dict(collective_id=collective_id, has_side_effects=True)
    return pltpu.CompilerParams(vmem_limit_bytes=vmem * 2**20, **kw)


def ask_kernel(len_ref, mine_ref, out_ref, slot_ref, ids_ref, msg_ref, ids_send, ids_recv, send_sem, recv_sem):
    r, z, _, _, _ = place()
    near = [(r, (z + s) % 4) for s in (1, 2, 3)]
    peers = [((r + s) % 32, z) for s in range(1, 32)]
    greet(near + peers)
    copies = []
    for s, device in enumerate(near):
        copy = remote(mine_ref, ids_ref.at[z], ids_send.at[s], ids_recv.at[s], device)
        copy.start()
        copies.append(copy)
    ids_ref[z] = mine_ref[...]
    before = (lax.broadcasted_iota(jnp.int32, (128, 128), 0)
              < lax.broadcasted_iota(jnp.int32, (128, 128), 1)).astype(F32)
    above = (lax.broadcasted_iota(jnp.int32, (32, 32), 1)
             < lax.broadcasted_iota(jnp.int32, (32, 32), 0)).astype(F32).astype(BF)
    both = jnp.concatenate([before, jnp.ones((128, 128), F32)], axis=0).astype(BF)
    owners = lax.broadcasted_iota(jnp.int32, (32, 128), 0)
    ks = lax.broadcasted_iota(jnp.int32, (384, 128), 0)
    lane = lax.broadcasted_iota(jnp.int32, (32, 128), 1)
    for copy in copies:
        copy.wait()
    ids = ids_ref[...].reshape(32, 128)
    owner = ids >> 14
    low, high = (ids & 127).astype(F32), ((ids >> 7) & 127).astype(F32)
    ones = [jnp.where(owner == o, 1.0, 0.0).astype(BF) for o in range(32)]
    rows_above = dot(above, jnp.concatenate(ones, axis=1)).astype(BF)
    prior = dot(
        jnp.concatenate(
            [jnp.concatenate(ones, axis=0),
             jnp.concatenate([rows_above[:, 128 * o : 128 * o + 128] for o in range(32)], axis=0)], axis=1),
        both)
    rank = jnp.zeros((32, 128), F32)
    for o in range(32):
        rank = rank + jnp.where(owner == o, prior[32 * o : 32 * o + 32], 0.0)
    rank_i = rank.astype(jnp.int32)
    acc = jnp.zeros((64, 384), F32)
    count = jnp.zeros((32, 128), F32)
    for a in range(0, 32, 2):
        lefts, rights = [], []
        for b in (a, a + 1):
            hit = owners == owner[b : b + 1, :]
            count = count + jnp.where(hit, 1.0, 0.0)
            lefts.append(jnp.concatenate(
                [jnp.where(hit, low[b : b + 1, :], 0.0), jnp.where(hit, high[b : b + 1, :], 0.0)], axis=0).astype(BF))
            rights.append(jnp.where(ks == rank_i[b : b + 1, :], 1.0, 0.0).astype(BF))
        acc = acc + dot_t(jnp.concatenate(lefts, axis=1), jnp.concatenate(rights, axis=1))
    req = (acc[32:] * 128.0 + acc[:32]).astype(jnp.int32)
    for j in range(3):
        msg_ref[:, j, :] = req[:, 128 * j : 128 * j + 128]
    tail = jnp.where(lane == 1, len_ref[0], jnp.where(lane == 2, len_ref[1], 0))
    msg_ref[:, 3, :] = tail
    slot_ref[...] = owner * CAP + rank_i
    copies = []
    for s, device in enumerate(peers):
        copy = remote(msg_ref.at[device[0]], out_ref.at[r], send_sem.at[s], recv_sem.at[s], device)
        copy.start()
        copies.append(copy)
    out_ref[r] = msg_ref[r]
    for copy in copies:
        copy.wait()


def routes():
    out = []
    for dy in range(4):
        for dx in range(4):
            for dk in range(2):
                if dx == dy == dk == 0:
                    continue
                side = 1 if dk == 0 else 3
                hop = None
                if dx == 2 or dy == 2:
                    hop = (side if dy == 2 else 0, side if dx == 2 else 0)
                out.append((dy, dx, dk, hop))
    key = lambda f: (f[3] is None, (f[0] * 5 + f[1] * 3 + f[2] * 7) % 11)
    return sorted(out, key=key)


def lookup_kernel(asked_ref, table_ref, out_ref, wide, stage, block, relay, send_sem, recv_sem, hop_send, hop_recv):
    r, z, y, x, k = place()

    def row(dy, dx, dk):
        return (((y + dy) % 4) * 4 + (x + dx) % 4) * 2 + (k + dk) % 2

    flows = routes()
    hops = [f for f in flows if f[3] is not None]
    direct = [f for f in flows if f[3] is None]
    barrier = pltpu.get_barrier_semaphore()
    for s in range(1, 32):
        pl.semaphore_signal(barrier, inc=1, device_id=((r + s) % 32, z), device_id_type=MESH)

    def widen(i, _):
        rows = pl.ds(pl.multiple_of(i * 256, 256), 256)
        wide[rows, :] = table_ref[rows, :].astype(F32)
        return 0

    lax.fori_loop(0, 64, widen, 0)
    pl.semaphore_wait(barrier, 31)

    def fill(p, dst):
        def some(j, _):
            base = j * 43
            for i in range(43):
                stage[pl.ds(base + i, 1), :] = wide[pl.ds(asked_ref[p * 512 + base + i], 1), :]
            return 0

        lax.fori_loop(0, 8, some, 0)
        dst[...] = stage[...].astype(BF)

    first, final, waiting = [], [], None
    for n, (dy, dx, dk, hop) in enumerate(hops + direct):
        p = row(dy, dx, dk)
        fill(p, block.at[n])
        if hop is not None:
            copy = remote(block.at[n], relay.at[n], hop_send.at[n], hop_recv.at[n], (row(*hop, 0), z))
            first.append(copy)
        else:
            i = n - len(hops)
            copy = remote(block.at[n], out_ref.at[r], send_sem.at[i], recv_sem.at[i], (p, z))
            final.append(copy)
        if waiting is not None:
            waiting.start()
        waiting = copy
    fill(r, out_ref.at[r])
    waiting.start()
    for i, (dy, dx, dk, (hy, hx)) in enumerate(hops):
        first[i].wait_recv()
        n = len(direct) + i
        copy = remote(relay.at[i], out_ref.at[row(-hy, -hx, 0)], send_sem.at[n], recv_sem.at[n],
                      (row(dy - hy, dx - hx, dk), z))
        copy.start()
        final.append(copy)
    for copy in first:
        copy.wait_send()
    for copy in final:
        copy.wait()


def spread_kernel(slot_ref, back_ref, out_ref, wide, stage, emb, relay, send_sem, relay_send, relay_recv, recv_sem,
                  pass_send, pass_recv, own_send, own_recv):
    r, z, y, x, k = place()
    base = r - k
    other = (base + 1 - k, z)
    up, down = (z + 1) % 4, (z + 3) % 4
    holder = z // 2
    mine = pl.ds(pl.multiple_of(1024 * k, 1024), 1024)
    theirs = pl.ds(pl.multiple_of(1024 * (1 - k), 1024), 1024)
    peers = [(base + 1 - k, z)]
    for kk in range(2):
        for s in (1, 3):
            peers.append((base + kk, (z + s) % 4))
    barrier = pltpu.get_barrier_semaphore()
    for device in peers:
        pl.semaphore_signal(barrier, inc=1, device_id=device, device_id_type=MESH)

    def widen(i, _):
        wide[pl.ds(pl.multiple_of(i * CAP, 8), CAP), :] = back_ref[i].astype(F32)
        return 0

    lax.fori_loop(0, 32, widen, 0)
    pl.semaphore_wait(barrier, len(peers))

    def part(i):
        return pl.ds(1024 * i, 1024)

    def far(h, half):
        return remote(emb.at[h, part(half)], relay, relay_send.at[half], relay_recv,
                      (base + half, up if half == 0 else down))

    def near(h, half, step):
        return remote(emb.at[h, part(half)], out_ref.at[z, part(half)],
                      send_sem.at[step // 2, half], recv_sem.at[step // 2], (base + half, (z + step) % 4))

    def own(h, half):
        return remote(emb.at[h, part(half)], out_ref.at[z, part(half)], own_send.at[half], own_recv.at[half], other)

    def send(h, half, act):
        dist = (2 * k + h - z) % 4

        @pl.when(dist == 2)
        def _():
            act(far(h, half))

        for step in (1, 3):
            @pl.when(dist == step)
            def _():
                act(near(h, half, step))

        @pl.when(dist == 0)
        def _():
            act(own(h, half))

    lead = jnp.where((2 * k - z) % 4 < 2, 1, 0)
    pieces = [(h, half) for h in (lead, 1 - lead) for half in range(2)]
    waiting = None
    for h, half in pieces:
        def gather(j, _):
            a = (half * 2 + j // 4) * 8 + h * 4 + lax.rem(j, 4)
            for i in range(128):
                stage[pl.ds(j * 128 + i, 1), :] = wide[pl.ds(slot_ref[a, i], 1), :]
            return 0

        lax.fori_loop(0, 8, gather, 0)
        emb[h, part(half), :] = stage[...].astype(BF)

        @pl.when((2 * k + h - z) % 4 == 0)
        def _():
            out_ref[z, part(half), :] = stage[...].astype(BF)

        if waiting is not None:
            send(*waiting, lambda copy: copy.start())
        waiting = (h, half)
    send(*waiting, lambda copy: copy.start())

    behind = jnp.where(k == 0, down, up)
    ahead = jnp.where(k == 0, up, down)
    relayed = remote(relay, out_ref.at[behind, mine], pass_send.at[3], recv_sem.at[2], (r, ahead))
    far(0, 0).wait_recv()
    relayed.start()
    passed = []
    for i, source in enumerate((down, up, (z + 2) % 4)):
        got = out_ref.at[source, mine]
        remote(got, got, pass_send.at[i], recv_sem.at[i], other).wait_recv()
        copy = remote(got, got, pass_send.at[i], pass_recv.at[i], other)
        copy.start()
        passed.append(copy)

    for i, source in enumerate((down, up, (z + 2) % 4)):
        passed[i].wait_send()
        got = out_ref.at[source, theirs]
        remote(got, got, pass_send.at[i], pass_recv.at[i], other).wait_recv()
    relayed.wait_send()
    for h, half in pieces:
        send(h, half, lambda copy: copy.wait_send())

    @pl.when(k != holder)
    def _():
        for half in range(2):
            own(0, half).wait_recv()


def layer_kernel(len_ref, x_ref, gain_ref, wqkv_ref, wout_ref, gain2_ref, win_hbm, wdown_hbm, out_ref,
                 nrm, qs, ke, ko, ve, vo, sc, att, win_ref, wdown_ref, sems):
    k = lax.axis_index("rows") % 2
    get_in = pltpu.make_async_copy(win_hbm, win_ref, sems.at[0])
    get_down = pltpu.make_async_copy(wdown_hbm, wdown_ref, sems.at[1])
    get_in.start()
    get_down.start()
    length = len_ref[0]
    quarters = (k, 3 - k)

    def norm(i, _):
        rows = pl.ds(pl.multiple_of(i * 256, 256), 256)
        parts = [x_ref[c, rows, :].astype(F32) for c in range(4)]
        square = parts[0] * parts[0]
        for part in parts[1:]:
            square = square + part * part
        scale = lax.rsqrt(jnp.sum(square, axis=1, keepdims=True) * (1.0 / D) + 1e-6)
        for c in range(4):
            nrm[rows, 128 * c : 128 * c + 128] = (parts[c] * scale * gain_ref[:, 128 * c : 128 * c + 128]).astype(BF)
        return 0

    lax.fori_loop(0, 8, norm, 0)

    def project(i, _):
        rows = pl.ds(pl.multiple_of(i * 256, 256), 256)
        here = nrm[rows, :]
        keys = dot(here, wqkv_ref[:, D : 2 * D])
        vals = dot(here, wqkv_ref[:, 2 * D :])
        lane = lax.broadcasted_iota(jnp.int32, (256, 128), 1)
        pos = lax.broadcasted_iota(jnp.int32, (256, 128), 0) + i * 256
        bias = jnp.where(pos < length, 0.0, NEG)
        for c in range(4):
            cols = slice(128 * c, 128 * c + 128)
            ke[rows, cols] = jnp.where(lane == 64, bias, keys[:, cols]).astype(BF)
            ko[rows, cols] = jnp.where(lane == 0, bias, keys[:, cols]).astype(BF)
            ve[rows, cols] = jnp.where(lane == 64, 1.0, vals[:, cols]).astype(BF)
            vo[rows, cols] = jnp.where(lane == 0, 1.0, vals[:, cols]).astype(BF)
        return 0

    lax.fori_loop(0, 8, project, 0)
    for a in range(2):
        rows = pl.ds(pl.multiple_of(quarters[a] * 512, 512), 512)
        qs[512 * a : 512 * a + 512, :] = (dot(nrm[rows, :], wqkv_ref[:, :D]) * (0.125 * LOG2E)).astype(BF)

    def attend(kk):
        def heads(hp, _):
            cols = pl.ds(pl.multiple_of(hp * 128, 128), 128)
            lane = lax.broadcasted_iota(jnp.int32, (256, 128), 1)
            tri = (lax.broadcasted_iota(jnp.int32, (256, 256), 1)
                   <= lax.broadcasted_iota(jnp.int32, (256, 256), 0))
            for a, quarter in enumerate((kk, 3 - kk)):
                for j in range(2):
                    n = 2 * quarter + j + 1
                    at = 512 * a + 256 * j
                    q = qs[at : at + 256, cols].astype(F32)
                    accs = []
                    for odd in range(2):
                        kref, vref = (ko, vo) if odd else (ke, ve)
                        if odd:
                            qa = jnp.where(lane >= 64, q, jnp.where(lane == 0, 1.0, 0.0)).astype(BF)
                        else:
                            qa = jnp.where(lane < 64, q, jnp.where(lane == 64, 1.0, 0.0)).astype(BF)
                        top = None
                        for c in range(n):
                            s = dot_t(qa, kref[256 * c : 256 * c + 256, cols])
                            if c == n - 1:
                                s = jnp.where(tri, s, NEG)
                            sc[odd, c] = s
                            m = jnp.maximum(s[:, :128], s[:, 128:])
                            top = m if top is None else jnp.maximum(top, m)
                        top = jnp.max(top, axis=1, keepdims=True)
                        acc = jnp.zeros((256, 128), F32)
                        for c in range(n):
                            p = jnp.exp2(sc[odd, c] - top).astype(BF)
                            acc = acc + dot(p, vref[256 * c : 256 * c + 256, cols])
                        accs.append(acc)
                    even = accs[0] / accs[0][:, 64:65]
                    odd_ = accs[1] / accs[1][:, 0:1]
                    att[at : at + 256, cols] = jnp.where(lane < 64, even, odd_).astype(BF)
            return 0

        lax.fori_loop(0, 4, heads, 0)

    for kk in range(2):
        @pl.when(k == kk)
        def _():
            attend(kk)

    get_in.wait()
    get_down.wait()

    def mlp(i, _):
        rows = pl.ds(pl.multiple_of(i * 256, 256), 256)
        quarter = jnp.where(i < 2, quarters[0], quarters[1])
        src = pl.ds(pl.multiple_of(quarter * 512 + lax.rem(i, 2) * 256, 256), 256)
        resid = jnp.concatenate([x_ref[c, src, :].astype(F32) for c in range(4)], axis=1)
        hidden = (resid + dot(att[rows, :], wout_ref[...])).astype(BF).astype(F32)
        scale = lax.rsqrt(jnp.mean(hidden * hidden, axis=1, keepdims=True) + 1e-6)
        normed = (hidden * scale * gain2_ref[...]).astype(BF)
        out = hidden
        for f in range(4):
            cols = slice(512 * f, 512 * f + 512)
            up_cols = slice(FF + 512 * f, FF + 512 * f + 512)
            gate = dot(normed, win_ref[:, cols])
            up = dot(normed, win_ref[:, up_cols])
            act = (gate / (1.0 + jnp.exp(-gate)) * up).astype(BF)
            out = out + dot(act, wdown_ref[cols, :])
        out_ref[rows, :] = out.astype(BF)
        return 0

    lax.fori_loop(0, 4, mlp, 0)


def give_kernel(src_ref, out_ref, relay, bounce, send_sem, far_send, relay_recv, recv_sem, pass_send, own_sem):
    r, z, y, x, k = place()
    base = r - k
    up, down = (z + 1) % 4, (z + 3) % 4
    across = (z + 2) % 4
    holder, slot = z // 2, z % 2
    peers = [(base + 1 - k, z)]
    for kk in range(2):
        for s in (1, 3):
            peers.append((base + kk, (z + s) % 4))
    greet(peers)

    def worker(q):
        return jnp.where((q == 0) | (q == 3), 0, 1)

    def piece(q, rows=pl.ds(0, 512)):
        at = jnp.where(q < 2, 0, 1)
        return src_ref.at[at, rows]

    halves = (pl.ds(0, 256), pl.ds(256, 256))
    via = (up, down)

    def far(half):
        return remote(piece(across, halves[half]), relay, far_send.at[half], relay_recv, (r, via[half]))

    def near(i):
        return remote(piece(via[i]), out_ref.at[slot], send_sem.at[i], recv_sem.at[slot, 0], (base + holder, via[i]))

    def own():
        return remote(piece(z), out_ref.at[slot], send_sem.at[2], recv_sem.at[slot, 0], (base + 1 - k, z))

    @pl.when(worker(across) == k)
    def _():
        far(0).start()
        far(1).start()

    for i in range(2):
        @pl.when(worker(via[i]) == k)
        def _():
            near(i).start()

    @pl.when((worker(z) == k) & (holder != k))
    def _():
        own().start()

    @pl.when((worker(z) == k) & (holder == k))
    def _():
        take = pltpu.make_async_copy(piece(z), bounce, own_sem)
        take.start()
        take.wait()
        put = pltpu.make_async_copy(bounce, out_ref.at[slot], own_sem)
        put.start()
        put.wait()

    def passing(half):
        source, target = (down, up) if half == 0 else (up, down)
        return remote(relay, out_ref.at[source % 2, halves[half]], pass_send, recv_sem.at[source % 2, half],
                      (base + source // 2, target))

    for half in range(2):
        @pl.when(worker(via[half]) == k)
        def _():
            far(half).wait_recv()
            passing(half).start()
            passing(half).wait_send()

    for h in range(2):
        source = 2 * k + h
        dist = (source - z) % 4
        @pl.when((dist == 1) | (dist == 3) | ((dist == 0) & (worker(z) != k)))
        def _():
            remote(src_ref.at[0], out_ref.at[h], send_sem.at[0], recv_sem.at[h, 0], (base + 1 - k, z)).wait_recv()
        @pl.when(dist == 2)
        def _():
            for half in range(2):
                remote(src_ref.at[0, halves[half]], out_ref.at[h, halves[half]], send_sem.at[0],
                       recv_sem.at[h, half], (base + 1 - k, z)).wait_recv()

    @pl.when(worker(across) == k)
    def _():
        far(0).wait_send()
        far(1).wait_send()

    for i in range(2):
        @pl.when(worker(via[i]) == k)
        def _():
            near(i).wait_send()

    @pl.when((worker(z) == k) & (holder != k))
    def _():
        own().wait_send()


def local(token_ids, lengths, table, attn_gain, w_qkv, w_out, mlp_gain, w_in, w_down):
    dma = pltpu.SemaphoreType.DMA
    asked, slot = pl.pallas_call(
        ask_kernel,
        out_shape=[jax.ShapeDtypeStruct((32, 4, 128), jnp.int32), jax.ShapeDtypeStruct((32, 128), jnp.int32)],
        in_specs=[SM, VM], out_specs=[VM, VM],
        scratch_shapes=[pltpu.VMEM((4, 8, 128), jnp.int32), pltpu.VMEM((32, 4, 128), jnp.int32),
                        dma((3,)), dma((3,)), dma((31,)), dma((31,))],
        compiler_params=params(1),
    )(lengths, token_ids.reshape(8, 128))
    returned = pl.pallas_call(
        lookup_kernel,
        out_shape=jax.ShapeDtypeStruct((32, CAP, 128), BF),
        in_specs=[SM, VM], out_specs=VM,
        scratch_shapes=[pltpu.VMEM((16384, 128), F32), pltpu.VMEM((CAP, 128), F32), pltpu.VMEM((31, CAP, 128), BF),
                        pltpu.VMEM((14, CAP, 128), BF), dma((31,)), dma((31,)), dma((14,)), dma((14,))],
        compiler_params=params(2),
    )(asked.reshape(32 * 512), table)
    full = pl.pallas_call(
        spread_kernel,
        out_shape=jax.ShapeDtypeStruct((4, 2048, 128), BF),
        in_specs=[SM, VM], out_specs=VM,
        scratch_shapes=[pltpu.VMEM((32 * CAP, 128), F32), pltpu.VMEM((1024, 128), F32), pltpu.VMEM((2, 2048, 128), BF),
                        pltpu.VMEM((1024, 128), BF), dma((2, 2)), dma((2,)), dma, dma((3,)), dma((4,)), dma((3,)),
                        dma((2,)), dma((2,))],
        compiler_params=params(3),
    )(slot, returned)
    r, z = lax.axis_index("rows"), lax.axis_index("cols")
    length = lax.dynamic_slice(asked, (r - r % 2 + z // 2, 3, 1 + z % 2), (1, 1, 1)).reshape(1)
    done = pl.pallas_call(
        layer_kernel,
        out_shape=jax.ShapeDtypeStruct((1024, D), BF),
        in_specs=[SM, VM, VM, VM, VM, VM, ANY, ANY], out_specs=VM,
        scratch_shapes=[pltpu.VMEM((2048, D), BF), pltpu.VMEM((1024, D), BF)]
        + [pltpu.VMEM((2048, D), BF)] * 4
        + [pltpu.VMEM((2, 8, 256, 256), F32), pltpu.VMEM((1024, D), BF),
           pltpu.VMEM((D, 2 * FF), BF), pltpu.VMEM((FF, D), BF), dma((2,))],
        compiler_params=params(),
    )(length, full, attn_gain.reshape(1, D), w_qkv, w_out, mlp_gain.reshape(1, D), w_in, w_down)
    return pl.pallas_call(
        give_kernel,
        out_shape=jax.ShapeDtypeStruct((2, 512, D), BF),
        in_specs=[ANY], out_specs=ANY,
        scratch_shapes=[pltpu.VMEM((256, D), BF), pltpu.VMEM((512, D), BF), dma((3,)), dma((2,)), dma, dma((2, 2)),
                        dma, dma],
        compiler_params=params(4),
    )(done.reshape(2, 512, D))


def solution(mesh):
    in_specs = (P("rows", "cols"), P("rows"), P("rows", "cols"), P(), P(), P(), P(), P(), P())
    return jax.shard_map(local, mesh=mesh, in_specs=in_specs, out_specs=P("rows", "cols", None), check_vma=False)
```

```python
import functools

import jax
import jax.numpy as jnp
from jax import lax
from jax.experimental import pallas as pl
from jax.experimental.pallas import tpu as pltpu
from jax.sharding import PartitionSpec as P

D = 512
FF = 2048
CAP = 344
BF = jnp.bfloat16
F32 = jnp.float32
MESH = pl.DeviceIdType.MESH
ANY = pl.BlockSpec(memory_space=pl.ANY)
VM = pl.BlockSpec(memory_space=pltpu.VMEM)
SM = pl.BlockSpec(memory_space=pltpu.SMEM)
LOG2E = 1.4426950408889634
NEG = -1e30


def dot(a, b):
    return jnp.dot(a, b, preferred_element_type=F32)


def dot_t(a, b):
    return lax.dot_general(a, b, (((1,), (1,)), ((), ())), preferred_element_type=F32)


def place():
    r, z = lax.axis_index("rows"), lax.axis_index("cols")
    return r, z, r // 8, (r // 2) % 4, r % 2


def greet(devices):
    barrier = pltpu.get_barrier_semaphore()
    for device in devices:
        pl.semaphore_signal(barrier, inc=1, device_id=device, device_id_type=MESH)
    pl.semaphore_wait(barrier, len(devices))


def remote(src, dst, send_sem, recv_sem, device):
    return pltpu.make_async_remote_copy(
        src_ref=src, dst_ref=dst, send_sem=send_sem, recv_sem=recv_sem,
        device_id=device, device_id_type=MESH)


def params(collective_id=None, vmem=60):
    kw = {}
    if collective_id is not None:
        kw = dict(collective_id=collective_id, has_side_effects=True)
    return pltpu.CompilerParams(vmem_limit_bytes=vmem * 2**20, **kw)


def ask_kernel(len_ref, mine_ref, out_ref, slot_ref, ids_ref, msg_ref, ids_send, ids_recv, send_sem, recv_sem):
    r, z, _, _, _ = place()
    near = [(r, (z + s) % 4) for s in (1, 2, 3)]
    peers = [((r + s) % 32, z) for s in range(1, 32)]
    greet(near + peers)
    copies = []
    for s, device in enumerate(near):
        copy = remote(mine_ref, ids_ref.at[z], ids_send.at[s], ids_recv.at[s], device)
        copy.start()
        copies.append(copy)
    ids_ref[z] = mine_ref[...]
    before = (lax.broadcasted_iota(jnp.int32, (128, 128), 0)
              < lax.broadcasted_iota(jnp.int32, (128, 128), 1)).astype(F32)
    above = (lax.broadcasted_iota(jnp.int32, (32, 32), 1)
             < lax.broadcasted_iota(jnp.int32, (32, 32), 0)).astype(F32).astype(BF)
    both = jnp.concatenate([before, jnp.ones((128, 128), F32)], axis=0).astype(BF)
    owners = lax.broadcasted_iota(jnp.int32, (32, 128), 0)
    ks = lax.broadcasted_iota(jnp.int32, (384, 128), 0)
    lane = lax.broadcasted_iota(jnp.int32, (32, 128), 1)
    for copy in copies:
        copy.wait()
    ids = ids_ref[...].reshape(32, 128)
    owner = ids >> 14
    low, high = (ids & 127).astype(F32), ((ids >> 7) & 127).astype(F32)
    ones = [jnp.where(owner == o, 1.0, 0.0).astype(BF) for o in range(32)]
    rows_above = dot(above, jnp.concatenate(ones, axis=1)).astype(BF)
    prior = dot(
        jnp.concatenate(
            [jnp.concatenate(ones, axis=0),
             jnp.concatenate([rows_above[:, 128 * o : 128 * o + 128] for o in range(32)], axis=0)], axis=1),
        both)
    rank = jnp.zeros((32, 128), F32)
    for o in range(32):
        rank = rank + jnp.where(owner == o, prior[32 * o : 32 * o + 32], 0.0)
    rank_i = rank.astype(jnp.int32)
    acc = jnp.zeros((64, 384), F32)
    count = jnp.zeros((32, 128), F32)
    for a in range(0, 32, 2):
        lefts, rights = [], []
        for b in (a, a + 1):
            hit = owners == owner[b : b + 1, :]
            count = count + jnp.where(hit, 1.0, 0.0)
            lefts.append(jnp.concatenate(
                [jnp.where(hit, low[b : b + 1, :], 0.0), jnp.where(hit, high[b : b + 1, :], 0.0)], axis=0).astype(BF))
            rights.append(jnp.where(ks == rank_i[b : b + 1, :], 1.0, 0.0).astype(BF))
        acc = acc + dot_t(jnp.concatenate(lefts, axis=1), jnp.concatenate(rights, axis=1))
    req = (acc[32:] * 128.0 + acc[:32]).astype(jnp.int32)
    for j in range(3):
        msg_ref[:, j, :] = req[:, 128 * j : 128 * j + 128]
    tail = jnp.where(lane == 1, len_ref[0], jnp.where(lane == 2, len_ref[1], 0))
    msg_ref[:, 3, :] = tail
    slot_ref[...] = owner * CAP + rank_i
    copies = []
    for s, device in enumerate(peers):
        copy = remote(msg_ref.at[device[0]], out_ref.at[r], send_sem.at[s], recv_sem.at[s], device)
        copy.start()
        copies.append(copy)
    out_ref[r] = msg_ref[r]
    for copy in copies:
        copy.wait()


def routes():
    out = []
    for dy in range(4):
        for dx in range(4):
            for dk in range(2):
                if dx == dy == dk == 0:
                    continue
                side = 1 if dk == 0 else 3
                hop = None
                if dx == 2 or dy == 2:
                    hop = (side if dy == 2 else 0, side if dx == 2 else 0)
                out.append((dy, dx, dk, hop))
    key = lambda f: (f[3] is None, (f[0] * 5 + f[1] * 3 + f[2] * 7) % 11)
    return sorted(out, key=key)


def lookup_kernel(asked_ref, table_ref, out_ref, wide, stage, block, relay, send_sem, recv_sem, hop_send, hop_recv):
    r, z, y, x, k = place()

    def row(dy, dx, dk):
        return (((y + dy) % 4) * 4 + (x + dx) % 4) * 2 + (k + dk) % 2

    flows = routes()
    hops = [f for f in flows if f[3] is not None]
    direct = [f for f in flows if f[3] is None]
    barrier = pltpu.get_barrier_semaphore()
    for s in range(1, 32):
        pl.semaphore_signal(barrier, inc=1, device_id=((r + s) % 32, z), device_id_type=MESH)

    def widen(i, _):
        rows = pl.ds(pl.multiple_of(i * 256, 256), 256)
        wide[rows, :] = table_ref[rows, :].astype(F32)
        return 0

    lax.fori_loop(0, 64, widen, 0)
    pl.semaphore_wait(barrier, 31)

    def fill(p, dst):
        def some(j, _):
            base = j * 43
            for i in range(43):
                stage[pl.ds(base + i, 1), :] = wide[pl.ds(asked_ref[p * 512 + base + i], 1), :]
            return 0

        lax.fori_loop(0, 8, some, 0)
        dst[...] = stage[...].astype(BF)

    first, final, waiting = [], [], None
    for n, (dy, dx, dk, hop) in enumerate(hops + direct):
        p = row(dy, dx, dk)
        fill(p, block.at[n])
        if hop is not None:
            copy = remote(block.at[n], relay.at[n], hop_send.at[n], hop_recv.at[n], (row(*hop, 0), z))
            first.append(copy)
        else:
            i = n - len(hops)
            copy = remote(block.at[n], out_ref.at[r], send_sem.at[i], recv_sem.at[i], (p, z))
            final.append(copy)
        if waiting is not None:
            waiting.start()
        waiting = copy
    fill(r, out_ref.at[r])
    waiting.start()
    for i, (dy, dx, dk, (hy, hx)) in enumerate(hops):
        first[i].wait_recv()
        n = len(direct) + i
        copy = remote(relay.at[i], out_ref.at[row(-hy, -hx, 0)], send_sem.at[n], recv_sem.at[n],
                      (row(dy - hy, dx - hx, dk), z))
        copy.start()
        final.append(copy)
    for copy in first:
        copy.wait_send()
    for copy in final:
        copy.wait()


def spread_kernel(slot_ref, back_ref, out_ref, wide, stage, emb, relay, send_sem, relay_send, relay_recv, recv_sem,
                  pass_send, pass_recv, own_send, own_recv):
    r, z, y, x, k = place()
    base = r - k
    other = (base + 1 - k, z)
    up, down = (z + 1) % 4, (z + 3) % 4
    holder = z // 2
    mine = pl.ds(pl.multiple_of(1024 * k, 1024), 1024)
    theirs = pl.ds(pl.multiple_of(1024 * (1 - k), 1024), 1024)
    peers = [(base + 1 - k, z)]
    for kk in range(2):
        for s in (1, 3):
            peers.append((base + kk, (z + s) % 4))
    barrier = pltpu.get_barrier_semaphore()
    for device in peers:
        pl.semaphore_signal(barrier, inc=1, device_id=device, device_id_type=MESH)

    def widen(i, _):
        wide[pl.ds(pl.multiple_of(i * CAP, 8), CAP), :] = back_ref[i].astype(F32)
        return 0

    lax.fori_loop(0, 32, widen, 0)
    pl.semaphore_wait(barrier, len(peers))

    def part(i):
        return pl.ds(1024 * i, 1024)

    def far(h, half):
        return remote(emb.at[h, part(half)], relay, relay_send.at[half], relay_recv,
                      (base + half, up if half == 0 else down))

    def near(h, half, step):
        return remote(emb.at[h, part(half)], out_ref.at[z, part(half)],
                      send_sem.at[step // 2, half], recv_sem.at[step // 2], (base + half, (z + step) % 4))

    def own(h, half):
        return remote(emb.at[h, part(half)], out_ref.at[z, part(half)], own_send.at[half], own_recv.at[half], other)

    def send(h, half, act):
        dist = (2 * k + h - z) % 4

        @pl.when(dist == 2)
        def _():
            act(far(h, half))

        for step in (1, 3):
            @pl.when(dist == step)
            def _():
                act(near(h, half, step))

        @pl.when(dist == 0)
        def _():
            act(own(h, half))

    lead = jnp.where((2 * k - z) % 4 < 2, 1, 0)
    pieces = [(h, half) for h in (lead, 1 - lead) for half in range(2)]
    waiting = None
    for h, half in pieces:
        def gather(j, _):
            a = (half * 2 + j // 4) * 8 + h * 4 + lax.rem(j, 4)
            for i in range(128):
                stage[pl.ds(j * 128 + i, 1), :] = wide[pl.ds(slot_ref[a, i], 1), :]
            return 0

        lax.fori_loop(0, 8, gather, 0)
        emb[h, part(half), :] = stage[...].astype(BF)

        @pl.when((2 * k + h - z) % 4 == 0)
        def _():
            out_ref[z, part(half), :] = stage[...].astype(BF)

        if waiting is not None:
            send(*waiting, lambda copy: copy.start())
        waiting = (h, half)
    send(*waiting, lambda copy: copy.start())

    behind = jnp.where(k == 0, down, up)
    ahead = jnp.where(k == 0, up, down)
    relayed = remote(relay, out_ref.at[behind, mine], pass_send.at[3], recv_sem.at[2], (r, ahead))
    far(0, 0).wait_recv()
    relayed.start()
    passed = []
    for i, source in enumerate((down, up, (z + 2) % 4)):
        got = out_ref.at[source, mine]
        remote(got, got, pass_send.at[i], recv_sem.at[i], other).wait_recv()
        copy = remote(got, got, pass_send.at[i], pass_recv.at[i], other)
        copy.start()
        passed.append(copy)

    for i, source in enumerate((down, up, (z + 2) % 4)):
        passed[i].wait_send()
        got = out_ref.at[source, theirs]
        remote(got, got, pass_send.at[i], pass_recv.at[i], other).wait_recv()
    relayed.wait_send()
    for h, half in pieces:
        send(h, half, lambda copy: copy.wait_send())

    @pl.when(k != holder)
    def _():
        for half in range(2):
            own(0, half).wait_recv()


def layer_kernel(len_ref, x_ref, gain_ref, wqkv_ref, wout_ref, gain2_ref, win_hbm, wdown_hbm, out_ref,
                 nrm, qs, ke, ko, vt, wvt, sc, att, obuf, relay, win_ref, wdown_ref, sems,
                 send_sem, far_recv, recv_sem, pass_send):
    r, z, _, _, k = place()
    base = r - k
    up, down = (z + 1) % 4, (z + 3) % 4
    holder, slot = z // 2, z % 2
    peers = [(base + 1 - k, z)]
    for kk in range(2):
        for s in (1, 3):
            peers.append((base + kk, (z + s) % 4))
    barrier = pltpu.get_barrier_semaphore()
    for device in peers:
        pl.semaphore_signal(barrier, inc=1, device_id=device, device_id_type=MESH)
    get_in = pltpu.make_async_copy(win_hbm, win_ref, sems.at[0])
    get_down = pltpu.make_async_copy(wdown_hbm, wdown_ref, sems.at[1])
    get_in.start()
    get_down.start()
    length = len_ref[0]

    def worker(q):
        return jnp.where((q == 0) | (q == 3), 0, 1)

    def quarter_of(step):
        early = jnp.where(z < 2, 1, 0)
        return jnp.where(step == early, k, 3 - k)

    def block(b):
        return pl.ds(256 * b, 256)

    def near(step, b, q):
        return remote(obuf.at[step, block(b)], out_ref.at[slot, block(b)], send_sem.at[step, b],
                      recv_sem.at[slot, b], (base + holder, q))

    def own(step, b):
        return remote(obuf.at[step, block(b)], out_ref.at[slot, block(b)], send_sem.at[step, b],
                      recv_sem.at[slot, b], (base + 1 - k, z))

    def far(b):
        return remote(obuf.at[0, block(b)], relay, send_sem.at[0, b], far_recv, (r, (up, down)[b]))

    def passing(b):
        source, target = ((down, up), (up, down))[b]
        return remote(relay, out_ref.at[source % 2, block(b)], pass_send, recv_sem.at[source % 2, b],
                      (base + source // 2, target))

    def send(step, b, act):
        q = quarter_of(step)
        dist = (q - z) % 4

        @pl.when((dist == 1) | (dist == 3))
        def _():
            act(near(step, b, q))

        @pl.when((dist == 0) & (holder != k))
        def _():
            act(own(step, b))

        if step == 0:
            @pl.when(dist == 2)
            def _():
                act(far(b))

    for c in range(4):
        wvt[128 * c : 128 * c + 128, :] = wqkv_ref[:, 2 * D + 128 * c : 2 * D + 128 * c + 128].astype(F32).T.astype(BF)

    def project(i, _):
        rows = pl.ds(pl.multiple_of(i * 256, 256), 256)
        parts = [x_ref[c, rows, :].astype(F32) for c in range(4)]
        square = parts[0] * parts[0]
        for part in parts[1:]:
            square = square + part * part
        scale = lax.rsqrt(jnp.sum(square, axis=1, keepdims=True) * (1.0 / D) + 1e-6)
        here = jnp.concatenate(
            [(parts[c] * scale * gain_ref[:, 128 * c : 128 * c + 128]).astype(BF) for c in range(4)], axis=1)
        nrm[rows, :] = here
        keys = dot(here, wqkv_ref[:, D : 2 * D])
        vals = dot_t(wvt[...], here)
        lane = lax.broadcasted_iota(jnp.int32, (256, 128), 1)
        pos = lax.broadcasted_iota(jnp.int32, (256, 128), 0) + i * 256
        bias = jnp.where(pos < length, 0.0, NEG)
        tail = jnp.where(lax.broadcasted_iota(jnp.int32, (16, 256), 0) == 0, 1.0, 0.0).astype(BF)
        for c in range(4):
            cols = slice(128 * c, 128 * c + 128)
            ke[rows, cols] = jnp.where(lane == 64, bias, keys[:, cols]).astype(BF)
            ko[rows, cols] = jnp.where(lane == 0, bias, keys[:, cols]).astype(BF)
        for h in range(8):
            vt[h, 0:64, rows] = vals[64 * h : 64 * h + 64, :].astype(BF)
            vt[h, 64:80, rows] = tail
        return 0

    lax.fori_loop(0, 8, project, 0)

    def attend(quarter):
        def heads(hp, _):
            cols = pl.ds(pl.multiple_of(hp * 128, 128), 128)
            lane = lax.broadcasted_iota(jnp.int32, (256, 128), 1)
            tri = (lax.broadcasted_iota(jnp.int32, (256, 256), 0)
                   <= lax.broadcasted_iota(jnp.int32, (256, 256), 1))
            for j in range(2):
                n = 2 * quarter + j + 1
                at = 256 * j
                q = qs[at : at + 256, cols].astype(F32)
                outs = []
                for odd in range(2):
                    kref = ko if odd else ke
                    if odd:
                        qa = jnp.where(lane >= 64, q, jnp.where(lane == 0, 1.0, 0.0)).astype(BF)
                    else:
                        qa = jnp.where(lane < 64, q, jnp.where(lane == 64, 1.0, 0.0)).astype(BF)
                    top = None
                    for c in range(n):
                        s = dot_t(kref[256 * c : 256 * c + 256, cols], qa)
                        if c == n - 1:
                            s = jnp.where(tri, s, NEG)
                        sc[odd, c] = s
                        m = jnp.max(s.reshape(4, 8, 8, 256), axis=1)
                        top = m if top is None else jnp.maximum(top, m)
                    top = jnp.max(jnp.max(top, axis=0), axis=0, keepdims=True)
                    acc = None
                    for c in range(n):
                        p = jnp.exp2(sc[odd, c] - top).astype(BF)
                        o = dot(vt[2 * hp + odd, :, 256 * c : 256 * c + 256], p)
                        acc = o if acc is None else acc + o
                    outs.append(acc[0:64, :] / acc[64:65, :])
                att[at : at + 256, cols] = jnp.concatenate(outs, axis=0).T.astype(BF)
            return 0

        lax.fori_loop(0, 4, heads, 0)

    def compute_attention(quarter):
        rows = pl.ds(pl.multiple_of(quarter * 512, 512), 512)
        qs[...] = (dot(nrm[rows, :], wqkv_ref[:, :D]) * (0.125 * LOG2E)).astype(BF)
        for q in range(4):
            @pl.when(quarter == q)
            def _():
                attend(q)

    def mlp(step, b, quarter):
        rows = pl.ds(pl.multiple_of(256 * b, 256), 256)
        src = pl.ds(pl.multiple_of(quarter * 512 + b * 256, 256), 256)
        resid = jnp.concatenate([x_ref[c, src, :].astype(F32) for c in range(4)], axis=1)
        hidden = (resid + dot(att[rows, :], wout_ref[...])).astype(BF).astype(F32)
        scale = lax.rsqrt(jnp.mean(hidden * hidden, axis=1, keepdims=True) + 1e-6)
        normed = (hidden * scale * gain2_ref[...]).astype(BF)
        out = hidden
        for f in range(4):
            cols = slice(512 * f, 512 * f + 512)
            up_cols = slice(FF + 512 * f, FF + 512 * f + 512)
            gate = dot(normed, win_ref[:, cols])
            high = dot(normed, win_ref[:, up_cols])
            act = (gate / (1.0 + jnp.exp(-gate)) * high).astype(BF)
            out = out + dot(act, wdown_ref[cols, :])
        obuf[step, rows, :] = out.astype(BF)

        @pl.when((quarter == z) & (holder == k))
        def _():
            out_ref[slot, rows, :] = out.astype(BF)

    def run(step, _):
        quarter = quarter_of(step)
        compute_attention(quarter)

        @pl.when(step == 0)
        def _():
            get_in.wait()
            get_down.wait()
            pl.semaphore_wait(barrier, len(peers))

        @pl.when(step == 1)
        def _():
            for b in range(2):
                @pl.when(worker((up, down)[b]) == k)
                def _():
                    far(b).wait_recv()
                    passing(b).start()

        def each(b, _):
            mlp(step, b, quarter)
            for ss in range(2):
                for bb in range(2):
                    @pl.when((step == ss) & (b == bb))
                    def _():
                        send(ss, bb, lambda copy: copy.start())
            return 0

        lax.fori_loop(0, 2, each, 0)
        return 0

    lax.fori_loop(0, 2, run, 0)

    for h in range(2):
        @pl.when((2 * k + h != z) | (worker(z) != k))
        def _():
            for b in range(2):
                remote(obuf.at[0, block(b)], out_ref.at[h, block(b)], send_sem.at[0, b], recv_sem.at[h, b],
                       (base + 1 - k, z)).wait_recv()
    for ss in range(2):
        for b in range(2):
            send(ss, b, lambda copy: copy.wait_send())
    for b in range(2):
        @pl.when(worker((up, down)[b]) == k)
        def _():
            passing(b).wait_send()


def local(token_ids, lengths, table, attn_gain, w_qkv, w_out, mlp_gain, w_in, w_down):
    dma = pltpu.SemaphoreType.DMA
    asked, slot = pl.pallas_call(
        ask_kernel,
        out_shape=[jax.ShapeDtypeStruct((32, 4, 128), jnp.int32), jax.ShapeDtypeStruct((32, 128), jnp.int32)],
        in_specs=[SM, VM], out_specs=[VM, VM],
        scratch_shapes=[pltpu.VMEM((4, 8, 128), jnp.int32), pltpu.VMEM((32, 4, 128), jnp.int32),
                        dma((3,)), dma((3,)), dma((31,)), dma((31,))],
        compiler_params=params(1),
    )(lengths, token_ids.reshape(8, 128))
    returned = pl.pallas_call(
        lookup_kernel,
        out_shape=jax.ShapeDtypeStruct((32, CAP, 128), BF),
        in_specs=[SM, VM], out_specs=VM,
        scratch_shapes=[pltpu.VMEM((16384, 128), F32), pltpu.VMEM((CAP, 128), F32), pltpu.VMEM((31, CAP, 128), BF),
                        pltpu.VMEM((14, CAP, 128), BF), dma((31,)), dma((31,)), dma((14,)), dma((14,))],
        compiler_params=params(2),
    )(asked.reshape(32 * 512), table)
    full = pl.pallas_call(
        spread_kernel,
        out_shape=jax.ShapeDtypeStruct((4, 2048, 128), BF),
        in_specs=[SM, VM], out_specs=VM,
        scratch_shapes=[pltpu.VMEM((32 * CAP, 128), F32), pltpu.VMEM((1024, 128), F32), pltpu.VMEM((2, 2048, 128), BF),
                        pltpu.VMEM((1024, 128), BF), dma((2, 2)), dma((2,)), dma, dma((3,)), dma((4,)), dma((3,)),
                        dma((2,)), dma((2,))],
        compiler_params=params(3),
    )(slot, returned)
    r, z = lax.axis_index("rows"), lax.axis_index("cols")
    length = lax.dynamic_slice(asked, (r - r % 2 + z // 2, 3, 1 + z % 2), (1, 1, 1)).reshape(1)
    return pl.pallas_call(
        layer_kernel,
        out_shape=jax.ShapeDtypeStruct((2, 512, D), BF),
        in_specs=[SM, VM, VM, VM, VM, VM, ANY, ANY], out_specs=VM,
        scratch_shapes=[pltpu.VMEM((2048, D), BF), pltpu.VMEM((512, D), BF), pltpu.VMEM((2048, D), BF),
                        pltpu.VMEM((2048, D), BF), pltpu.VMEM((8, 80, 2048), BF), pltpu.VMEM((D, D), BF),
                        pltpu.VMEM((2, 8, 256, 256), F32), pltpu.VMEM((512, D), BF), pltpu.VMEM((2, 512, D), BF),
                        pltpu.VMEM((256, D), BF), pltpu.VMEM((D, 2 * FF), BF), pltpu.VMEM((FF, D), BF), dma((2,)),
                        dma((2, 2)), dma, dma((2, 2)), dma],
        compiler_params=params(4),
    )(length, full, attn_gain.reshape(1, D), w_qkv, w_out, mlp_gain.reshape(1, D), w_in, w_down)


def solution(mesh):
    in_specs = (P("rows", "cols"), P("rows"), P("rows", "cols"), P(), P(), P(), P(), P(), P())
    return jax.shard_map(local, mesh=mesh, in_specs=in_specs, out_specs=P("rows", "cols", None), check_vma=False)
```

```python
import functools

import jax
import jax.numpy as jnp
from jax import lax
from jax.experimental import pallas as pl
from jax.experimental.pallas import tpu as pltpu
from jax.sharding import PartitionSpec as P

D = 512
FF = 2048
CAP = 344
BF = jnp.bfloat16
F32 = jnp.float32
MESH = pl.DeviceIdType.MESH
ANY = pl.BlockSpec(memory_space=pl.ANY)
VM = pl.BlockSpec(memory_space=pltpu.VMEM)
SM = pl.BlockSpec(memory_space=pltpu.SMEM)
LOG2E = 1.4426950408889634
NEG = -1e30


def dot(a, b):
    return jnp.dot(a, b, preferred_element_type=F32)


def dot_t(a, b):
    return lax.dot_general(a, b, (((1,), (1,)), ((), ())), preferred_element_type=F32)


def place():
    r, z = lax.axis_index("rows"), lax.axis_index("cols")
    return r, z, r // 8, (r // 2) % 4, r % 2


def greet(devices):
    barrier = pltpu.get_barrier_semaphore()
    for device in devices:
        pl.semaphore_signal(barrier, inc=1, device_id=device, device_id_type=MESH)
    pl.semaphore_wait(barrier, len(devices))


def remote(src, dst, send_sem, recv_sem, device):
    return pltpu.make_async_remote_copy(
        src_ref=src, dst_ref=dst, send_sem=send_sem, recv_sem=recv_sem,
        device_id=device, device_id_type=MESH)


def params(collective_id=None, vmem=60):
    kw = {}
    if collective_id is not None:
        kw = dict(collective_id=collective_id, has_side_effects=True)
    return pltpu.CompilerParams(vmem_limit_bytes=vmem * 2**20, **kw)


def ask_kernel(len_ref, mine_ref, out_ref, slot_ref, ids_ref, msg_ref, ids_send, ids_recv, send_sem, recv_sem):
    r, z, _, _, _ = place()
    near = [(r, (z + s) % 4) for s in (1, 2, 3)]
    peers = [((r + s) % 32, z) for s in range(1, 32)]
    greet(near + peers)
    copies = []
    for s, device in enumerate(near):
        copy = remote(mine_ref, ids_ref.at[z], ids_send.at[s], ids_recv.at[s], device)
        copy.start()
        copies.append(copy)
    ids_ref[z] = mine_ref[...]
    before = (lax.broadcasted_iota(jnp.int32, (128, 128), 0)
              < lax.broadcasted_iota(jnp.int32, (128, 128), 1)).astype(F32)
    above = (lax.broadcasted_iota(jnp.int32, (32, 32), 1)
             < lax.broadcasted_iota(jnp.int32, (32, 32), 0)).astype(F32).astype(BF)
    both = jnp.concatenate([before, jnp.ones((128, 128), F32)], axis=0).astype(BF)
    owners = lax.broadcasted_iota(jnp.int32, (32, 128), 0)
    ks = lax.broadcasted_iota(jnp.int32, (384, 128), 0)
    lane = lax.broadcasted_iota(jnp.int32, (32, 128), 1)
    for copy in copies:
        copy.wait()
    ids = ids_ref[...].reshape(32, 128)
    owner = ids >> 14
    low, high = (ids & 127).astype(F32), ((ids >> 7) & 127).astype(F32)
    ones = [jnp.where(owner == o, 1.0, 0.0).astype(BF) for o in range(32)]
    rows_above = dot(above, jnp.concatenate(ones, axis=1)).astype(BF)
    prior = dot(
        jnp.concatenate(
            [jnp.concatenate(ones, axis=0),
             jnp.concatenate([rows_above[:, 128 * o : 128 * o + 128] for o in range(32)], axis=0)], axis=1),
        both)
    rank = jnp.zeros((32, 128), F32)
    for o in range(32):
        rank = rank + jnp.where(owner == o, prior[32 * o : 32 * o + 32], 0.0)
    rank_i = rank.astype(jnp.int32)
    acc = jnp.zeros((64, 384), F32)
    count = jnp.zeros((32, 128), F32)
    for a in range(0, 32, 2):
        lefts, rights = [], []
        for b in (a, a + 1):
            hit = owners == owner[b : b + 1, :]
            count = count + jnp.where(hit, 1.0, 0.0)
            lefts.append(jnp.concatenate(
                [jnp.where(hit, low[b : b + 1, :], 0.0), jnp.where(hit, high[b : b + 1, :], 0.0)], axis=0).astype(BF))
            rights.append(jnp.where(ks == rank_i[b : b + 1, :], 1.0, 0.0).astype(BF))
        acc = acc + dot_t(jnp.concatenate(lefts, axis=1), jnp.concatenate(rights, axis=1))
    req = (acc[32:] * 128.0 + acc[:32]).astype(jnp.int32)
    for j in range(3):
        msg_ref[:, j, :] = req[:, 128 * j : 128 * j + 128]
    tail = jnp.where(lane == 1, len_ref[0], jnp.where(lane == 2, len_ref[1], 0))
    msg_ref[:, 3, :] = tail
    slot_ref[...] = owner * CAP + rank_i
    copies = []
    for s, device in enumerate(peers):
        copy = remote(msg_ref.at[device[0]], out_ref.at[r], send_sem.at[s], recv_sem.at[s], device)
        copy.start()
        copies.append(copy)
    out_ref[r] = msg_ref[r]
    for copy in copies:
        copy.wait()


def routes():
    out = []
    for dy in range(4):
        for dx in range(4):
            for dk in range(2):
                if dx == dy == dk == 0:
                    continue
                side = 1 if dk == 0 else 3
                hop = None
                if dx == 2 or dy == 2:
                    hop = (side if dy == 2 else 0, side if dx == 2 else 0)
                out.append((dy, dx, dk, hop))
    key = lambda f: (f[3] is None, (f[0] * 5 + f[1] * 3 + f[2] * 7) % 11)
    return sorted(out, key=key)


def lookup_kernel(asked_ref, table_ref, out_ref, wide, stage, block, relay, send_sem, recv_sem, hop_send, hop_recv):
    r, z, y, x, k = place()

    def row(dy, dx, dk):
        return (((y + dy) % 4) * 4 + (x + dx) % 4) * 2 + (k + dk) % 2

    flows = routes()
    hops = [f for f in flows if f[3] is not None]
    direct = [f for f in flows if f[3] is None]
    barrier = pltpu.get_barrier_semaphore()
    for s in range(1, 32):
        pl.semaphore_signal(barrier, inc=1, device_id=((r + s) % 32, z), device_id_type=MESH)

    def widen(i, _):
        rows = pl.ds(pl.multiple_of(i * 256, 256), 256)
        wide[rows, :] = table_ref[rows, :].astype(F32)
        return 0

    lax.fori_loop(0, 64, widen, 0)
    pl.semaphore_wait(barrier, 31)

    def fill(p, dst):
        def some(j, _):
            base = j * 43
            for i in range(43):
                stage[pl.ds(base + i, 1), :] = wide[pl.ds(asked_ref[p * 512 + base + i], 1), :]
            return 0

        lax.fori_loop(0, 8, some, 0)
        dst[...] = stage[...].astype(BF)

    first, final, waiting = [], [], None
    for n, (dy, dx, dk, hop) in enumerate(hops + direct):
        p = row(dy, dx, dk)
        fill(p, block.at[n])
        if hop is not None:
            copy = remote(block.at[n], relay.at[n], hop_send.at[n], hop_recv.at[n], (row(*hop, 0), z))
            first.append(copy)
        else:
            i = n - len(hops)
            copy = remote(block.at[n], out_ref.at[r], send_sem.at[i], recv_sem.at[i], (p, z))
            final.append(copy)
        if waiting is not None:
            waiting.start()
        waiting = copy
    fill(r, out_ref.at[r])
    waiting.start()
    for i, (dy, dx, dk, (hy, hx)) in enumerate(hops):
        first[i].wait_recv()
        n = len(direct) + i
        copy = remote(relay.at[i], out_ref.at[row(-hy, -hx, 0)], send_sem.at[n], recv_sem.at[n],
                      (row(dy - hy, dx - hx, dk), z))
        copy.start()
        final.append(copy)
    for copy in first:
        copy.wait_send()
    for copy in final:
        copy.wait()


def spread_kernel(slot_ref, back_ref, out_ref, wide, stage, emb, relay, send_sem, relay_send, relay_recv, recv_sem,
                  pass_send, pass_recv, own_send, own_recv):
    r, z, y, x, k = place()
    base = r - k
    other = (base + 1 - k, z)
    up, down = (z + 1) % 4, (z + 3) % 4
    holder = z // 2
    mine = pl.ds(pl.multiple_of(1024 * k, 1024), 1024)
    theirs = pl.ds(pl.multiple_of(1024 * (1 - k), 1024), 1024)
    peers = [(base + 1 - k, z)]
    for kk in range(2):
        for s in (1, 3):
            peers.append((base + kk, (z + s) % 4))
    barrier = pltpu.get_barrier_semaphore()
    for device in peers:
        pl.semaphore_signal(barrier, inc=1, device_id=device, device_id_type=MESH)

    def widen(i, _):
        wide[pl.ds(pl.multiple_of(i * CAP, 8), CAP), :] = back_ref[i].astype(F32)
        return 0

    lax.fori_loop(0, 32, widen, 0)
    pl.semaphore_wait(barrier, len(peers))

    def part(i):
        return pl.ds(1024 * i, 1024)

    def far(h, half):
        return remote(emb.at[h, part(half)], relay, relay_send.at[half], relay_recv,
                      (base + half, up if half == 0 else down))

    def near(h, half, step):
        return remote(emb.at[h, part(half)], out_ref.at[z, part(half)],
                      send_sem.at[step // 2, half], recv_sem.at[step // 2], (base + half, (z + step) % 4))

    def own(h, half):
        return remote(emb.at[h, part(half)], out_ref.at[z, part(half)], own_send.at[half], own_recv.at[half], other)

    def send(h, half, act):
        dist = (2 * k + h - z) % 4

        @pl.when(dist == 2)
        def _():
            act(far(h, half))

        for step in (1, 3):
            @pl.when(dist == step)
            def _():
                act(near(h, half, step))

        @pl.when(dist == 0)
        def _():
            act(own(h, half))

    lead = jnp.where((2 * k - z) % 4 < 2, 1, 0)
    pieces = [(h, half) for h in (lead, 1 - lead) for half in range(2)]
    waiting = None
    for h, half in pieces:
        def gather(j, _):
            a = (half * 2 + j // 4) * 8 + h * 4 + lax.rem(j, 4)
            for i in range(128):
                stage[pl.ds(j * 128 + i, 1), :] = wide[pl.ds(slot_ref[a, i], 1), :]
            return 0

        lax.fori_loop(0, 8, gather, 0)
        emb[h, part(half), :] = stage[...].astype(BF)

        @pl.when((2 * k + h - z) % 4 == 0)
        def _():
            out_ref[z, part(half), :] = stage[...].astype(BF)

        if waiting is not None:
            send(*waiting, lambda copy: copy.start())
        waiting = (h, half)
    send(*waiting, lambda copy: copy.start())

    behind = jnp.where(k == 0, down, up)
    ahead = jnp.where(k == 0, up, down)
    relayed = remote(relay, out_ref.at[behind, mine], pass_send.at[3], recv_sem.at[2], (r, ahead))
    far(0, 0).wait_recv()
    relayed.start()
    passed = []
    for i, source in enumerate((down, up, (z + 2) % 4)):
        got = out_ref.at[source, mine]
        remote(got, got, pass_send.at[i], recv_sem.at[i], other).wait_recv()
        copy = remote(got, got, pass_send.at[i], pass_recv.at[i], other)
        copy.start()
        passed.append(copy)

    for i, source in enumerate((down, up, (z + 2) % 4)):
        passed[i].wait_send()
        got = out_ref.at[source, theirs]
        remote(got, got, pass_send.at[i], pass_recv.at[i], other).wait_recv()
    relayed.wait_send()
    for h, half in pieces:
        send(h, half, lambda copy: copy.wait_send())

    @pl.when(k != holder)
    def _():
        for half in range(2):
            own(0, half).wait_recv()


def layer_kernel(len_ref, x_ref, gain_ref, wqkv_ref, wout_ref, gain2_ref, win_hbm, wdown_hbm, out_ref,
                 nrm, qs, ke, ko, vt, wvt, sc, att, hid, act, obuf, relay, win_ref, wdown_ref, sems,
                 send_sem, far_recv, recv_sem, pass_send):
    r, z, _, _, k = place()
    base = r - k
    up, down = (z + 1) % 4, (z + 3) % 4
    holder, slot = z // 2, z % 2
    peers = [(base + 1 - k, z)]
    for kk in range(2):
        for s in (1, 3):
            peers.append((base + kk, (z + s) % 4))
    barrier = pltpu.get_barrier_semaphore()
    for device in peers:
        pl.semaphore_signal(barrier, inc=1, device_id=device, device_id_type=MESH)
    get_in = pltpu.make_async_copy(win_hbm, win_ref, sems.at[0])
    get_down = pltpu.make_async_copy(wdown_hbm, wdown_ref, sems.at[1])
    get_in.start()
    get_down.start()
    length = len_ref[0]

    def worker(q):
        return jnp.where((q == 0) | (q == 3), 0, 1)

    def quarter_of(step):
        early = jnp.where(z < 2, 1, 0)
        return jnp.where(step == early, k, 3 - k)

    def block(b):
        return pl.ds(256 * b, 256)

    def near(step, b, q):
        return remote(obuf.at[step, block(b)], out_ref.at[slot, block(b)], send_sem.at[step, b],
                      recv_sem.at[slot, b], (base + holder, q))

    def own(step, b):
        return remote(obuf.at[step, block(b)], out_ref.at[slot, block(b)], send_sem.at[step, b],
                      recv_sem.at[slot, b], (base + 1 - k, z))

    def far(b):
        return remote(obuf.at[0, block(b)], relay, send_sem.at[0, b], far_recv, (r, (up, down)[b]))

    def passing(b):
        source, target = ((down, up), (up, down))[b]
        return remote(relay, out_ref.at[source % 2, block(b)], pass_send, recv_sem.at[source % 2, b],
                      (base + source // 2, target))

    def send(step, b, act):
        q = quarter_of(step)
        dist = (q - z) % 4

        @pl.when((dist == 1) | (dist == 3))
        def _():
            act(near(step, b, q))

        @pl.when((dist == 0) & (holder != k))
        def _():
            act(own(step, b))

        if step == 0:
            @pl.when(dist == 2)
            def _():
                act(far(b))

    for c in range(4):
        wvt[128 * c : 128 * c + 128, :] = wqkv_ref[:, 2 * D + 128 * c : 2 * D + 128 * c + 128].astype(F32).T.astype(BF)

    def project(i, _):
        rows = pl.ds(pl.multiple_of(i * 512, 512), 512)
        parts = [x_ref[c, rows, :].astype(F32) for c in range(4)]
        square = parts[0] * parts[0]
        for part in parts[1:]:
            square = square + part * part
        scale = lax.rsqrt(jnp.sum(square, axis=1, keepdims=True) * (1.0 / D) + 1e-6)
        here = jnp.concatenate(
            [(parts[c] * scale * gain_ref[:, 128 * c : 128 * c + 128]).astype(BF) for c in range(4)], axis=1)
        nrm[rows, :] = here
        keys = dot(here, wqkv_ref[:, D : 2 * D])
        vals = dot_t(wvt[...], here)
        lane = lax.broadcasted_iota(jnp.int32, (512, 128), 1)
        pos = lax.broadcasted_iota(jnp.int32, (512, 128), 0) + i * 512
        bias = jnp.where(pos < length, 0.0, NEG)
        tail = jnp.where(lax.broadcasted_iota(jnp.int32, (16, 512), 0) == 0, 1.0, 0.0).astype(BF)
        for c in range(4):
            cols = slice(128 * c, 128 * c + 128)
            ke[rows, cols] = jnp.where(lane == 64, bias, keys[:, cols]).astype(BF)
            ko[rows, cols] = jnp.where(lane == 0, bias, keys[:, cols]).astype(BF)
        for h in range(8):
            vt[h, 0:64, rows] = vals[64 * h : 64 * h + 64, :].astype(BF)
            vt[h, 64:80, rows] = tail
        return 0

    lax.fori_loop(0, 4, project, 0)

    def attend(quarter):
        lane = lax.broadcasted_iota(jnp.int32, (256, 128), 1)
        tri = (lax.broadcasted_iota(jnp.int32, (256, 256), 0)
               <= lax.broadcasted_iota(jnp.int32, (256, 256), 1))
        order = [(0, 0), (0, 1), (1, 0), (1, 1)]

        def tiles(j):
            return 2 * quarter + j + 1

        def columns(hp):
            return pl.ds(pl.multiple_of(hp * 128, 128), 128)

        def query(hp, g):
            j, odd = order[g]
            q = qs[256 * j : 256 * j + 256, columns(hp)].astype(F32)
            if odd:
                return jnp.where(lane >= 64, q, jnp.where(lane == 0, 1.0, 0.0)).astype(BF)
            return jnp.where(lane < 64, q, jnp.where(lane == 64, 1.0, 0.0)).astype(BF)

        def score(hp, g, qa, c, top):
            j, odd = order[g]
            s = dot_t((ko if odd else ke)[256 * c : 256 * c + 256, columns(hp)], qa)
            if c == tiles(j) - 1:
                s = jnp.where(tri, s, NEG)
            sc[g % 2, c] = s
            m = jnp.max(s.reshape(4, 8, 8, 256), axis=1)
            return m if top is None else jnp.maximum(top, m)

        def finish(top):
            return jnp.max(jnp.max(top, axis=0), axis=0, keepdims=True)

        def first_scores(hp):
            qa, top = query(hp, 0), None
            for c in range(tiles(0)):
                top = score(hp, 0, qa, c, top)
            return finish(top)

        def heads(hp, top):
            outs = []
            after = jnp.minimum(hp + 1, 3)
            for g, (j, odd) in enumerate(order):
                ahead, hp_ahead = (g + 1) % 4, hp if g < 3 else after
                qa, top_ahead, acc = query(hp_ahead, ahead), None, None
                n, n_ahead = tiles(j), tiles(order[ahead][0])
                for c in range(max(n, n_ahead)):
                    if c < n_ahead:
                        top_ahead = score(hp_ahead, ahead, qa, c, top_ahead)
                    if c < n:
                        p = jnp.exp2(sc[g % 2, c] - top).astype(BF)
                        o = dot(vt[2 * hp + odd, :, 256 * c : 256 * c + 256], p)
                        acc = o if acc is None else acc + o
                outs.append(acc[0:64, :] / acc[64:65, :])
                if odd:
                    att[256 * j : 256 * j + 256, columns(hp)] = jnp.concatenate(outs, axis=0).T.astype(BF)
                    outs = []
                top = finish(top_ahead)
            return top

        lax.fori_loop(0, 4, heads, first_scores(0))

    def compute_attention(quarter):
        rows = pl.ds(pl.multiple_of(quarter * 512, 512), 512)
        qs[...] = (dot(nrm[rows, :], wqkv_ref[:, :D]) * (0.125 * LOG2E)).astype(BF)
        for q in range(4):
            @pl.when(quarter == q)
            def _():
                attend(q)

    def mlp(quarter):
        src = pl.ds(pl.multiple_of(quarter * 512, 512), 512)
        resid = jnp.concatenate([x_ref[c, src, :].astype(F32) for c in range(4)], axis=1)
        hidden = (resid + dot(att[...], wout_ref[...])).astype(BF)
        hid[...] = hidden
        hidden = hidden.astype(F32)
        scale = lax.rsqrt(jnp.mean(hidden * hidden, axis=1, keepdims=True) + 1e-6)
        att[...] = (hidden * scale * gain2_ref[...]).astype(BF)

        for f in range(0, FF, 256):
            gate = dot(att[...], win_ref[:, f : f + 256])
            high = dot(att[...], win_ref[:, FF + f : FF + f + 256])
            act[:, f : f + 256] = (gate / (1.0 + jnp.exp(-gate)) * high).astype(BF)

    def lower(step, b, quarter):
        rows = pl.ds(pl.multiple_of(256 * b, 256), 256)
        out = (hid[rows, :].astype(F32) + dot(act[rows, :], wdown_ref[...])).astype(BF)
        obuf[step, rows, :] = out

        @pl.when((quarter == z) & (holder == k))
        def _():
            out_ref[slot, rows, :] = out

    def run(step, _):
        quarter = quarter_of(step)
        compute_attention(quarter)

        @pl.when(step == 0)
        def _():
            get_in.wait()
            get_down.wait()
            pl.semaphore_wait(barrier, len(peers))

        @pl.when(step == 1)
        def _():
            for b in range(2):
                @pl.when(worker((up, down)[b]) == k)
                def _():
                    far(b).wait_recv()
                    passing(b).start()

        mlp(quarter)

        def each(b, _):
            lower(step, b, quarter)
            for ss in range(2):
                for bb in range(2):
                    @pl.when((step == ss) & (b == bb))
                    def _():
                        send(ss, bb, lambda copy: copy.start())
            return 0

        lax.fori_loop(0, 2, each, 0)
        return 0

    lax.fori_loop(0, 2, run, 0)

    for h in range(2):
        @pl.when((2 * k + h != z) | (worker(z) != k))
        def _():
            for b in range(2):
                remote(obuf.at[0, block(b)], out_ref.at[h, block(b)], send_sem.at[0, b], recv_sem.at[h, b],
                       (base + 1 - k, z)).wait_recv()
    for ss in range(2):
        for b in range(2):
            send(ss, b, lambda copy: copy.wait_send())
    for b in range(2):
        @pl.when(worker((up, down)[b]) == k)
        def _():
            passing(b).wait_send()


def local(token_ids, lengths, table, attn_gain, w_qkv, w_out, mlp_gain, w_in, w_down):
    dma = pltpu.SemaphoreType.DMA
    asked, slot = pl.pallas_call(
        ask_kernel,
        out_shape=[jax.ShapeDtypeStruct((32, 4, 128), jnp.int32), jax.ShapeDtypeStruct((32, 128), jnp.int32)],
        in_specs=[SM, VM], out_specs=[VM, VM],
        scratch_shapes=[pltpu.VMEM((4, 8, 128), jnp.int32), pltpu.VMEM((32, 4, 128), jnp.int32),
                        dma((3,)), dma((3,)), dma((31,)), dma((31,))],
        compiler_params=params(1),
    )(lengths, token_ids.reshape(8, 128))
    returned = pl.pallas_call(
        lookup_kernel,
        out_shape=jax.ShapeDtypeStruct((32, CAP, 128), BF),
        in_specs=[SM, VM], out_specs=VM,
        scratch_shapes=[pltpu.VMEM((16384, 128), F32), pltpu.VMEM((CAP, 128), F32), pltpu.VMEM((31, CAP, 128), BF),
                        pltpu.VMEM((14, CAP, 128), BF), dma((31,)), dma((31,)), dma((14,)), dma((14,))],
        compiler_params=params(2),
    )(asked.reshape(32 * 512), table)
    full = pl.pallas_call(
        spread_kernel,
        out_shape=jax.ShapeDtypeStruct((4, 2048, 128), BF),
        in_specs=[SM, VM], out_specs=VM,
        scratch_shapes=[pltpu.VMEM((32 * CAP, 128), F32), pltpu.VMEM((1024, 128), F32), pltpu.VMEM((2, 2048, 128), BF),
                        pltpu.VMEM((1024, 128), BF), dma((2, 2)), dma((2,)), dma, dma((3,)), dma((4,)), dma((3,)),
                        dma((2,)), dma((2,))],
        compiler_params=params(3),
    )(slot, returned)
    r, z = lax.axis_index("rows"), lax.axis_index("cols")
    length = lax.dynamic_slice(asked, (r - r % 2 + z // 2, 3, 1 + z % 2), (1, 1, 1)).reshape(1)
    return pl.pallas_call(
        layer_kernel,
        out_shape=jax.ShapeDtypeStruct((2, 512, D), BF),
        in_specs=[SM, VM, VM, VM, VM, VM, ANY, ANY], out_specs=VM,
        scratch_shapes=[pltpu.VMEM((2048, D), BF), pltpu.VMEM((512, D), BF), pltpu.VMEM((2048, D), BF),
                        pltpu.VMEM((2048, D), BF), pltpu.VMEM((8, 80, 2048), BF), pltpu.VMEM((D, D), BF),
                        pltpu.VMEM((2, 8, 256, 256), F32), pltpu.VMEM((512, D), BF), pltpu.VMEM((512, D), BF),
                        pltpu.VMEM((512, FF), BF), pltpu.VMEM((2, 512, D), BF),
                        pltpu.VMEM((256, D), BF), pltpu.VMEM((D, 2 * FF), BF), pltpu.VMEM((FF, D), BF), dma((2,)),
                        dma((2, 2)), dma, dma((2, 2)), dma],
        compiler_params=params(4),
    )(length, full, attn_gain.reshape(1, D), w_qkv, w_out, mlp_gain.reshape(1, D), w_in, w_down)


def solution(mesh):
    in_specs = (P("rows", "cols"), P("rows"), P("rows", "cols"), P(), P(), P(), P(), P(), P())
    return jax.shard_map(local, mesh=mesh, in_specs=in_specs, out_specs=P("rows", "cols", None), check_vma=False)
```

```python
import functools

import jax
import jax.numpy as jnp
from jax import lax
from jax.experimental import pallas as pl
from jax.experimental.pallas import tpu as pltpu
from jax.sharding import PartitionSpec as P

D = 512
FF = 2048
CAP = 344
BF = jnp.bfloat16
F32 = jnp.float32
MESH = pl.DeviceIdType.MESH
ANY = pl.BlockSpec(memory_space=pl.ANY)
VM = pl.BlockSpec(memory_space=pltpu.VMEM)
SM = pl.BlockSpec(memory_space=pltpu.SMEM)
LOG2E = 1.4426950408889634
NEG = -1e30


def dot(a, b):
    return jnp.dot(a, b, preferred_element_type=F32)


def dot_t(a, b):
    return lax.dot_general(a, b, (((1,), (1,)), ((), ())), preferred_element_type=F32)


def place():
    r, z = lax.axis_index("rows"), lax.axis_index("cols")
    return r, z, r // 8, (r // 2) % 4, r % 2


def greet(devices):
    barrier = pltpu.get_barrier_semaphore()
    for device in devices:
        pl.semaphore_signal(barrier, inc=1, device_id=device, device_id_type=MESH)
    pl.semaphore_wait(barrier, len(devices))


def remote(src, dst, send_sem, recv_sem, device):
    return pltpu.make_async_remote_copy(
        src_ref=src, dst_ref=dst, send_sem=send_sem, recv_sem=recv_sem,
        device_id=device, device_id_type=MESH)


def params(collective_id=None, vmem=60):
    kw = {}
    if collective_id is not None:
        kw = dict(collective_id=collective_id, has_side_effects=True)
    return pltpu.CompilerParams(vmem_limit_bytes=vmem * 2**20, **kw)


def routes():
    out = []
    for dy in range(4):
        for dx in range(4):
            for dk in range(2):
                if dx == dy == dk == 0:
                    continue
                side = 1 if dk == 0 else 3
                hop = None
                if dx == 2 or dy == 2:
                    hop = (side if dy == 2 else 0, side if dx == 2 else 0)
                out.append((dy, dx, dk, hop))
    key = lambda f: (f[3] is None, (f[0] * 5 + f[1] * 3 + f[2] * 7) % 11)
    return sorted(out, key=key)


def requests(ids, lens, msg_ref, slot_ref):
    before = (lax.broadcasted_iota(jnp.int32, (128, 128), 0)
              < lax.broadcasted_iota(jnp.int32, (128, 128), 1)).astype(F32)
    above = (lax.broadcasted_iota(jnp.int32, (32, 32), 1)
             < lax.broadcasted_iota(jnp.int32, (32, 32), 0)).astype(F32).astype(BF)
    both = jnp.concatenate([before, jnp.ones((128, 128), F32)], axis=0).astype(BF)
    owners = lax.broadcasted_iota(jnp.int32, (32, 128), 0)
    column = lax.broadcasted_iota(jnp.int32, (4 * 128, 128), 0)
    ks = jnp.where((column & 127) < CAP // 4, (column >> 7) * (CAP // 4) + (column & 127), -1)
    lane = lax.broadcasted_iota(jnp.int32, (32, 128), 1)
    owner = ids >> 14
    low, high = (ids & 127).astype(F32), ((ids >> 7) & 127).astype(F32)
    ones = [jnp.where(owner == o, 1.0, 0.0).astype(BF) for o in range(32)]
    rows_above = dot(above, jnp.concatenate(ones, axis=1)).astype(BF)
    prior = dot(
        jnp.concatenate(
            [jnp.concatenate(ones, axis=0),
             jnp.concatenate([rows_above[:, 128 * o : 128 * o + 128] for o in range(32)], axis=0)], axis=1),
        both)
    rank = jnp.zeros((32, 128), F32)
    for o in range(32):
        rank = rank + jnp.where(owner == o, prior[32 * o : 32 * o + 32], 0.0)
    rank_i = rank.astype(jnp.int32)
    slot_ref[...] = jnp.clip(owner * CAP + rank_i, 0, 32 * CAP - 1)
    acc = jnp.zeros((64, 4 * 128), F32)
    for a in range(0, 32, 2):
        lefts, rights = [], []
        for b in (a, a + 1):
            hit = owners == owner[b : b + 1, :]
            lefts.append(jnp.concatenate(
                [jnp.where(hit, low[b : b + 1, :], 0.0), jnp.where(hit, high[b : b + 1, :], 0.0)], axis=0).astype(BF))
            rights.append(jnp.where(ks == rank_i[b : b + 1, :], 1.0, 0.0).astype(BF))
        acc = acc + dot_t(jnp.concatenate(lefts, axis=1), jnp.concatenate(rights, axis=1))
    req = (acc[32:] * 128.0 + acc[:32]).astype(jnp.int32)
    req0 = jnp.where(lane == 126, lens[0], jnp.where(lane == 127, lens[1], req[:, :128]))
    msg_ref[:, 0, :] = req0
    for j in range(1, 4):
        msg_ref[:, j, :] = req[:, 128 * j : 128 * j + 128]


def front_kernel(len_ref, tok_ref, table_hbm, out_ref, lens_ref,
                 ids_ref, msg_ref, asked_v, asked_s, slot_v, slot_s, table_ref, wide, stage, block, relay, back, emb,
                 relay_z, ids_send, ids_recv, ask_send, ask_recv, copy_sem, send_sem, recv_sem, hop_send, hop_recv,
                 z_send, z_relay_send, z_relay_recv, z_recv, pass_send, pass_recv, own_send, own_recv):
    r, z, y, x, k = place()
    base = r - k
    other = (base + 1 - k, z)
    up, down = (z + 1) % 4, (z + 3) % 4
    holder = z // 2
    column = [(r, (z + s) % 4) for s in (1, 2, 3)]
    plane = [((r + s) % 32, z) for s in range(1, 32)]
    load = pltpu.make_async_copy(table_hbm, table_ref, copy_sem.at[0])
    load.start()
    greet(column + plane + [(base + 1 - k, up), (base + 1 - k, down)])

    copies = []
    for s, device in enumerate(column):
        copy = remote(tok_ref, ids_ref.at[z], ids_send.at[s], ids_recv.at[s], device)
        copy.start()
        copies.append(copy)
    ids_ref[z] = tok_ref[...]
    for copy in copies:
        copy.wait()
    ids = jnp.concatenate(
        [ids_ref[c, h : h + 1, 128 * j : 128 * j + 128] for c in range(4) for h in range(2) for j in range(4)], axis=0)
    requests(ids, (len_ref[0], len_ref[1]), msg_ref, slot_v)

    copies = []
    for s, device in enumerate(plane):
        copy = remote(msg_ref.at[device[0]], asked_v.at[r], ask_send.at[s], ask_recv.at[s], device)
        copy.start()
        copies.append(copy)
    asked_v[r] = msg_ref[r]
    to_slots = pltpu.make_async_copy(slot_v, slot_s, copy_sem.at[1])
    to_slots.start()
    load.wait()

    def widen(i, _):
        rows = pl.ds(pl.multiple_of(i * 256, 256), 256)
        wide[rows, :] = table_ref[rows, :].astype(F32)
        return 0

    lax.fori_loop(0, 64, widen, 0)
    for copy in copies:
        copy.wait()
    asked_v[...] = jnp.clip(asked_v[...], 0, 16383)
    to_asked = pltpu.make_async_copy(asked_v, asked_s, copy_sem.at[2])
    to_asked.start()
    to_asked.wait()
    to_slots.wait()
    lens_ref[...] = asked_v[base + holder, 0:1, :]

    def row(dy, dx, dk):
        return (((y + dy) % 4) * 4 + (x + dx) % 4) * 2 + (k + dk) % 2

    def fill(p, dst):
        def some(j, _):
            for i in range(CAP // 4):
                stage[pl.ds(j * (CAP // 4) + i, 1), :] = wide[pl.ds(asked_s[p, j, i], 1), :]
            return 0

        lax.fori_loop(0, 4, some, 0)
        dst[...] = stage[0:CAP, :].astype(BF)

    flows = routes()
    hops = [f for f in flows if f[3] is not None]
    direct = [f for f in flows if f[3] is None]
    first, final, waiting = [], [], None
    for n, (dy, dx, dk, hop) in enumerate(hops + direct):
        p = row(dy, dx, dk)
        fill(p, block.at[n])
        if hop is not None:
            copy = remote(block.at[n], relay.at[n], hop_send.at[n], hop_recv.at[n], (row(*hop, 0), z))
            first.append(copy)
        else:
            i = n - len(hops)
            copy = remote(block.at[n], back.at[r], send_sem.at[i], recv_sem.at[i], (p, z))
            final.append((copy, row(-dy, -dx, dk)))
        if waiting is not None:
            waiting.start()
        waiting = copy
    fill(r, back.at[r])
    waiting.start()
    for i, (dy, dx, dk, (hy, hx)) in enumerate(hops):
        first[i].wait_recv()
        n = len(direct) + i
        copy = remote(relay.at[i], back.at[row(-hy, -hx, 0)], send_sem.at[n], recv_sem.at[n],
                      (row(dy - hy, dx - hx, dk), z))
        copy.start()
        final.append((copy, row(-dy, -dx, dk)))

    def spread(source):
        wide[pl.ds(pl.multiple_of(source * CAP, 8), CAP), :] = back[source].astype(F32)

    spread(r)
    for copy, source in final:
        copy.wait_recv()
        spread(source)

    mine = pl.ds(pl.multiple_of(1024 * k, 1024), 1024)
    theirs = pl.ds(pl.multiple_of(1024 * (1 - k), 1024), 1024)

    def part(i):
        return pl.ds(1024 * i, 1024)

    def far(h, half):
        return remote(emb.at[h, part(half)], relay_z, z_relay_send.at[half], z_relay_recv,
                      (base + half, up if half == 0 else down))

    def near(h, half, step):
        return remote(emb.at[h, part(half)], out_ref.at[z, part(half)],
                      z_send.at[step // 2, half], z_recv.at[step // 2], (base + half, (z + step) % 4))

    def own(h, half):
        return remote(emb.at[h, part(half)], out_ref.at[z, part(half)], own_send.at[half], own_recv.at[half], other)

    def send(h, half, act):
        dist = (2 * k + h - z) % 4

        @pl.when(dist == 2)
        def _():
            act(far(h, half))

        for step in (1, 3):
            @pl.when(dist == step)
            def _():
                act(near(h, half, step))

        @pl.when(dist == 0)
        def _():
            act(own(h, half))

    lead = jnp.where((2 * k - z) % 4 < 2, 1, 0)
    pieces = [(h, half) for h in (lead, 1 - lead) for half in range(2)]
    waiting = None
    for h, half in pieces:
        def gather(j, _):
            a = (half * 2 + j // 4) * 8 + h * 4 + lax.rem(j, 4)
            for i in range(128):
                stage[pl.ds(j * 128 + i, 1), :] = wide[pl.ds(slot_s[a, i], 1), :]
            return 0

        lax.fori_loop(0, 8, gather, 0)
        emb[h, part(half), :] = stage[...].astype(BF)

        @pl.when((2 * k + h - z) % 4 == 0)
        def _():
            out_ref[z, part(half), :] = stage[...].astype(BF)

        if waiting is not None:
            send(*waiting, lambda copy: copy.start())
        waiting = (h, half)
    send(*waiting, lambda copy: copy.start())

    behind = jnp.where(k == 0, down, up)
    ahead = jnp.where(k == 0, up, down)
    relayed = remote(relay_z, out_ref.at[behind, mine], pass_send.at[3], z_recv.at[2], (r, ahead))
    far(0, 0).wait_recv()
    relayed.start()
    passed = []
    for i, source in enumerate((down, up, (z + 2) % 4)):
        got = out_ref.at[source, mine]
        remote(got, got, pass_send.at[i], z_recv.at[i], other).wait_recv()
        copy = remote(got, got, pass_send.at[i], pass_recv.at[i], other)
        copy.start()
        passed.append(copy)
    for copy in first:
        copy.wait_send()
    for copy, _ in final:
        copy.wait_send()

    for i, source in enumerate((down, up, (z + 2) % 4)):
        passed[i].wait_send()
        got = out_ref.at[source, theirs]
        remote(got, got, pass_send.at[i], pass_recv.at[i], other).wait_recv()
    relayed.wait_send()
    for h, half in pieces:
        send(h, half, lambda copy: copy.wait_send())

    @pl.when(k != holder)
    def _():
        for half in range(2):
            own(0, half).wait_recv()


def layer_kernel(len_ref, x_ref, gain_ref, wqkv_ref, wout_ref, gain2_ref, win_hbm, wdown_hbm, out_ref,
                 nrm, qs, ke, ko, vt, wvt, sc, att, hid, act, obuf, relay, win_ref, wdown_ref, sems,
                 send_sem, far_recv, recv_sem, pass_send):
    r, z, _, _, k = place()
    base = r - k
    up, down = (z + 1) % 4, (z + 3) % 4
    holder, slot = z // 2, z % 2
    peers = [(base + 1 - k, z)]
    for kk in range(2):
        for s in (1, 3):
            peers.append((base + kk, (z + s) % 4))
    barrier = pltpu.get_barrier_semaphore()
    for device in peers:
        pl.semaphore_signal(barrier, inc=1, device_id=device, device_id_type=MESH)
    get_in = pltpu.make_async_copy(win_hbm, win_ref, sems.at[0])
    get_down = pltpu.make_async_copy(wdown_hbm, wdown_ref, sems.at[1])
    get_in.start()
    get_down.start()
    length = len_ref[0, 126 + z % 2]

    def worker(q):
        return jnp.where((q == 0) | (q == 3), 0, 1)

    def quarter_of(step):
        early = jnp.where(z < 2, 1, 0)
        return jnp.where(step == early, k, 3 - k)

    def block(b):
        return pl.ds(256 * b, 256)

    def near(step, b, q):
        return remote(obuf.at[step, block(b)], out_ref.at[slot, block(b)], send_sem.at[step, b],
                      recv_sem.at[slot, b], (base + holder, q))

    def own(step, b):
        return remote(obuf.at[step, block(b)], out_ref.at[slot, block(b)], send_sem.at[step, b],
                      recv_sem.at[slot, b], (base + 1 - k, z))

    def far(b):
        return remote(obuf.at[0, block(b)], relay, send_sem.at[0, b], far_recv, (r, (up, down)[b]))

    def passing(b):
        source, target = ((down, up), (up, down))[b]
        return remote(relay, out_ref.at[source % 2, block(b)], pass_send, recv_sem.at[source % 2, b],
                      (base + source // 2, target))

    def send(step, b, act):
        q = quarter_of(step)
        dist = (q - z) % 4

        @pl.when((dist == 1) | (dist == 3))
        def _():
            act(near(step, b, q))

        @pl.when((dist == 0) & (holder != k))
        def _():
            act(own(step, b))

        if step == 0:
            @pl.when(dist == 2)
            def _():
                act(far(b))

    for c in range(4):
        wvt[128 * c : 128 * c + 128, :] = wqkv_ref[:, 2 * D + 128 * c : 2 * D + 128 * c + 128].astype(F32).T.astype(BF)

    def project(i, _):
        rows = pl.ds(pl.multiple_of(i * 512, 512), 512)
        parts = [x_ref[c, rows, :].astype(F32) for c in range(4)]
        square = parts[0] * parts[0]
        for part in parts[1:]:
            square = square + part * part
        scale = lax.rsqrt(jnp.sum(square, axis=1, keepdims=True) * (1.0 / D) + 1e-6)
        here = jnp.concatenate(
            [(parts[c] * scale * gain_ref[:, 128 * c : 128 * c + 128]).astype(BF) for c in range(4)], axis=1)
        nrm[rows, :] = here
        keys = dot(here, wqkv_ref[:, D : 2 * D])
        vals = dot_t(wvt[...], here)
        lane = lax.broadcasted_iota(jnp.int32, (512, 128), 1)
        pos = lax.broadcasted_iota(jnp.int32, (512, 128), 0) + i * 512
        bias = jnp.where(pos < length, 0.0, NEG)
        tail = jnp.where(lax.broadcasted_iota(jnp.int32, (16, 512), 0) == 0, 1.0, 0.0).astype(BF)
        for c in range(4):
            cols = slice(128 * c, 128 * c + 128)
            ke[rows, cols] = jnp.where(lane == 64, bias, keys[:, cols]).astype(BF)
            ko[rows, cols] = jnp.where(lane == 0, bias, keys[:, cols]).astype(BF)
        for h in range(8):
            vt[h, 0:64, rows] = vals[64 * h : 64 * h + 64, :].astype(BF)
            vt[h, 64:80, rows] = tail
        return 0

    lax.fori_loop(0, 4, project, 0)

    def attend(quarter):
        lane = lax.broadcasted_iota(jnp.int32, (256, 128), 1)
        tri = (lax.broadcasted_iota(jnp.int32, (256, 256), 0)
               <= lax.broadcasted_iota(jnp.int32, (256, 256), 1))
        order = [(0, 0), (0, 1), (1, 0), (1, 1)]

        def tiles(j):
            return 2 * quarter + j + 1

        def columns(hp):
            return pl.ds(pl.multiple_of(hp * 128, 128), 128)

        def query(hp, g):
            j, odd = order[g]
            q = qs[256 * j : 256 * j + 256, columns(hp)].astype(F32)
            if odd:
                return jnp.where(lane >= 64, q, jnp.where(lane == 0, 1.0, 0.0)).astype(BF)
            return jnp.where(lane < 64, q, jnp.where(lane == 64, 1.0, 0.0)).astype(BF)

        def score(hp, g, qa, c, top):
            j, odd = order[g]
            s = dot_t((ko if odd else ke)[256 * c : 256 * c + 256, columns(hp)], qa)
            if c == tiles(j) - 1:
                s = jnp.where(tri, s, NEG)
            sc[g % 2, c] = s
            m = jnp.max(s.reshape(4, 8, 8, 256), axis=1)
            return m if top is None else jnp.maximum(top, m)

        def finish(top):
            return jnp.max(jnp.max(top, axis=0), axis=0, keepdims=True)

        def first_scores(hp):
            qa, top = query(hp, 0), None
            for c in range(tiles(0)):
                top = score(hp, 0, qa, c, top)
            return finish(top)

        def heads(hp, top):
            outs = []
            after = jnp.minimum(hp + 1, 3)
            for g, (j, odd) in enumerate(order):
                ahead, hp_ahead = (g + 1) % 4, hp if g < 3 else after
                qa, top_ahead, acc = query(hp_ahead, ahead), None, None
                n, n_ahead = tiles(j), tiles(order[ahead][0])
                for c in range(max(n, n_ahead)):
                    if c < n_ahead:
                        top_ahead = score(hp_ahead, ahead, qa, c, top_ahead)
                    if c < n:
                        p = jnp.exp2(sc[g % 2, c] - top).astype(BF)
                        o = dot(vt[2 * hp + odd, :, 256 * c : 256 * c + 256], p)
                        acc = o if acc is None else acc + o
                outs.append(acc[0:64, :] / acc[64:65, :])
                if odd:
                    att[256 * j : 256 * j + 256, columns(hp)] = jnp.concatenate(outs, axis=0).T.astype(BF)
                    outs = []
                top = finish(top_ahead)
            return top

        lax.fori_loop(0, 4, heads, first_scores(0))

    def compute_attention(quarter):
        rows = pl.ds(pl.multiple_of(quarter * 512, 512), 512)
        qs[...] = (dot(nrm[rows, :], wqkv_ref[:, :D]) * (0.125 * LOG2E)).astype(BF)
        for q in range(4):
            @pl.when(quarter == q)
            def _():
                attend(q)

    def mlp(quarter):
        src = pl.ds(pl.multiple_of(quarter * 512, 512), 512)
        resid = jnp.concatenate([x_ref[c, src, :].astype(F32) for c in range(4)], axis=1)
        hidden = (resid + dot(att[...], wout_ref[...])).astype(BF)
        hid[...] = hidden
        hidden = hidden.astype(F32)
        scale = lax.rsqrt(jnp.mean(hidden * hidden, axis=1, keepdims=True) + 1e-6)
        att[...] = (hidden * scale * gain2_ref[...]).astype(BF)

        for f in range(0, FF, 256):
            gate = dot(att[...], win_ref[:, f : f + 256])
            high = dot(att[...], win_ref[:, FF + f : FF + f + 256])
            act[:, f : f + 256] = (gate / (1.0 + jnp.exp(-gate)) * high).astype(BF)

    def lower(step, b, quarter):
        rows = pl.ds(pl.multiple_of(256 * b, 256), 256)
        out = (hid[rows, :].astype(F32) + dot(act[rows, :], wdown_ref[...])).astype(BF)
        obuf[step, rows, :] = out

        @pl.when((quarter == z) & (holder == k))
        def _():
            out_ref[slot, rows, :] = out

    def run(step, _):
        quarter = quarter_of(step)
        compute_attention(quarter)

        @pl.when(step == 0)
        def _():
            get_in.wait()
            get_down.wait()
            pl.semaphore_wait(barrier, len(peers))

        @pl.when(step == 1)
        def _():
            for b in range(2):
                @pl.when(worker((up, down)[b]) == k)
                def _():
                    far(b).wait_recv()
                    passing(b).start()

        mlp(quarter)

        def each(b, _):
            lower(step, b, quarter)
            for ss in range(2):
                for bb in range(2):
                    @pl.when((step == ss) & (b == bb))
                    def _():
                        send(ss, bb, lambda copy: copy.start())
            return 0

        lax.fori_loop(0, 2, each, 0)
        return 0

    lax.fori_loop(0, 2, run, 0)

    for h in range(2):
        @pl.when((2 * k + h != z) | (worker(z) != k))
        def _():
            for b in range(2):
                remote(obuf.at[0, block(b)], out_ref.at[h, block(b)], send_sem.at[0, b], recv_sem.at[h, b],
                       (base + 1 - k, z)).wait_recv()
    for ss in range(2):
        for b in range(2):
            send(ss, b, lambda copy: copy.wait_send())
    for b in range(2):
        @pl.when(worker((up, down)[b]) == k)
        def _():
            passing(b).wait_send()


def local(token_ids, lengths, table, attn_gain, w_qkv, w_out, mlp_gain, w_in, w_down):
    dma = pltpu.SemaphoreType.DMA
    full, lens = pl.pallas_call(
        front_kernel,
        out_shape=[jax.ShapeDtypeStruct((4, 2048, 128), BF), jax.ShapeDtypeStruct((1, 128), jnp.int32)],
        in_specs=[SM, VM, ANY], out_specs=[VM, VM],
        scratch_shapes=[
            pltpu.VMEM((4, 2, 512), jnp.int32), pltpu.VMEM((32, 4, 128), jnp.int32), pltpu.VMEM((32, 4, 128), jnp.int32),
            pltpu.SMEM((32, 4, 128), jnp.int32), pltpu.VMEM((32, 128), jnp.int32), pltpu.SMEM((32, 128), jnp.int32),
            pltpu.VMEM((16384, 128), BF), pltpu.VMEM((16384, 128), F32), pltpu.VMEM((1024, 128), F32),
            pltpu.VMEM((31, CAP, 128), BF), pltpu.VMEM((14, CAP, 128), BF), pltpu.VMEM((32, CAP, 128), BF),
            pltpu.VMEM((2, 2048, 128), BF), pltpu.VMEM((1024, 128), BF),
            dma((3,)), dma((3,)), dma((31,)), dma((31,)), dma((3,)), dma((31,)), dma((31,)), dma((14,)), dma((14,)),
            dma((2, 2)), dma((2,)), dma, dma((3,)), dma((4,)), dma((3,)), dma((2,)), dma((2,))],
        compiler_params=params(1),
    )(lengths, token_ids, table)
    return pl.pallas_call(
        layer_kernel,
        out_shape=jax.ShapeDtypeStruct((2, 512, D), BF),
        in_specs=[SM, VM, VM, VM, VM, VM, ANY, ANY], out_specs=VM,
        scratch_shapes=[pltpu.VMEM((2048, D), BF), pltpu.VMEM((512, D), BF), pltpu.VMEM((2048, D), BF),
                        pltpu.VMEM((2048, D), BF), pltpu.VMEM((8, 80, 2048), BF), pltpu.VMEM((D, D), BF),
                        pltpu.VMEM((2, 8, 256, 256), F32), pltpu.VMEM((512, D), BF), pltpu.VMEM((512, D), BF),
                        pltpu.VMEM((512, FF), BF), pltpu.VMEM((2, 512, D), BF),
                        pltpu.VMEM((256, D), BF), pltpu.VMEM((D, 2 * FF), BF), pltpu.VMEM((FF, D), BF), dma((2,)),
                        dma((2, 2)), dma, dma((2, 2)), dma],
        compiler_params=params(2),
    )(lens, full, attn_gain.reshape(1, D), w_qkv, w_out, mlp_gain.reshape(1, D), w_in, w_down)


def solution(mesh):
    in_specs = (P("rows", "cols"), P("rows"), P("rows", "cols"), P(), P(), P(), P(), P(), P())
    return jax.shard_map(local, mesh=mesh, in_specs=in_specs, out_specs=P("rows", "cols", None), check_vma=False)
```

```python
import functools

import jax
import jax.numpy as jnp
from jax import lax
from jax.experimental import pallas as pl
from jax.experimental.pallas import tpu as pltpu
from jax.sharding import PartitionSpec as P

D = 512
FF = 2048
CAP = 344
BF = jnp.bfloat16
F32 = jnp.float32
MESH = pl.DeviceIdType.MESH
ANY = pl.BlockSpec(memory_space=pl.ANY)
VM = pl.BlockSpec(memory_space=pltpu.VMEM)
SM = pl.BlockSpec(memory_space=pltpu.SMEM)
LOG2E = 1.4426950408889634
NEG = -1e30


def dot(a, b):
    return jnp.dot(a, b, preferred_element_type=F32)


def dot_t(a, b):
    return lax.dot_general(a, b, (((1,), (1,)), ((), ())), preferred_element_type=F32)


def place():
    r, z = lax.axis_index("rows"), lax.axis_index("cols")
    return r, z, r // 8, (r // 2) % 4, r % 2


def greet(devices):
    barrier = pltpu.get_barrier_semaphore()
    for device in devices:
        pl.semaphore_signal(barrier, inc=1, device_id=device, device_id_type=MESH)
    pl.semaphore_wait(barrier, len(devices))


def remote(src, dst, send_sem, recv_sem, device):
    return pltpu.make_async_remote_copy(
        src_ref=src, dst_ref=dst, send_sem=send_sem, recv_sem=recv_sem,
        device_id=device, device_id_type=MESH)


def params(collective_id=None, vmem=60):
    kw = {}
    if collective_id is not None:
        kw = dict(collective_id=collective_id, has_side_effects=True)
    return pltpu.CompilerParams(vmem_limit_bytes=vmem * 2**20, **kw)


def routes():
    out = []
    for dy in range(4):
        for dx in range(4):
            for dk in range(2):
                if dx == dy == dk == 0:
                    continue
                side = 1 if dk == 0 else 3
                hop = None
                if dx == 2 or dy == 2:
                    hop = (side if dy == 2 else 0, side if dx == 2 else 0)
                out.append((dy, dx, dk, hop))
    key = lambda f: (f[3] is None, (f[0] * 5 + f[1] * 3 + f[2] * 7) % 11)
    return sorted(out, key=key)


def requests(ids, lens, msg_ref, slot_ref):
    before = (lax.broadcasted_iota(jnp.int32, (128, 128), 0)
              < lax.broadcasted_iota(jnp.int32, (128, 128), 1)).astype(F32)
    above = (lax.broadcasted_iota(jnp.int32, (32, 32), 1)
             < lax.broadcasted_iota(jnp.int32, (32, 32), 0)).astype(F32).astype(BF)
    both = jnp.concatenate([before, jnp.ones((128, 128), F32)], axis=0).astype(BF)
    owners = lax.broadcasted_iota(jnp.int32, (32, 128), 0)
    column = lax.broadcasted_iota(jnp.int32, (4 * 128, 128), 0)
    ks = jnp.where((column & 127) < CAP // 4, (column >> 7) * (CAP // 4) + (column & 127), -1)
    lane = lax.broadcasted_iota(jnp.int32, (32, 128), 1)
    owner = ids >> 14
    low, high = (ids & 127).astype(F32), ((ids >> 7) & 127).astype(F32)
    ones = [jnp.where(owner == o, 1.0, 0.0).astype(BF) for o in range(32)]
    rows_above = dot(above, jnp.concatenate(ones, axis=1)).astype(BF)
    prior = dot(
        jnp.concatenate(
            [jnp.concatenate(ones, axis=0),
             jnp.concatenate([rows_above[:, 128 * o : 128 * o + 128] for o in range(32)], axis=0)], axis=1),
        both)
    rank = jnp.zeros((32, 128), F32)
    for o in range(32):
        rank = rank + jnp.where(owner == o, prior[32 * o : 32 * o + 32], 0.0)
    rank_i = rank.astype(jnp.int32)
    slot_ref[...] = jnp.clip(owner * CAP + rank_i, 0, 32 * CAP - 1)
    acc = jnp.zeros((64, 4 * 128), F32)
    for a in range(0, 32, 2):
        lefts, rights = [], []
        for b in (a, a + 1):
            hit = owners == owner[b : b + 1, :]
            lefts.append(jnp.concatenate(
                [jnp.where(hit, low[b : b + 1, :], 0.0), jnp.where(hit, high[b : b + 1, :], 0.0)], axis=0).astype(BF))
            rights.append(jnp.where(ks == rank_i[b : b + 1, :], 1.0, 0.0).astype(BF))
        acc = acc + dot_t(jnp.concatenate(lefts, axis=1), jnp.concatenate(rights, axis=1))
    req = (acc[32:] * 128.0 + acc[:32]).astype(jnp.int32)
    req0 = jnp.where(lane == 126, lens[0], jnp.where(lane == 127, lens[1], req[:, :128]))
    msg_ref[:, 0, :] = req0
    for j in range(1, 4):
        msg_ref[:, j, :] = req[:, 128 * j : 128 * j + 128]


def front_kernel(len_ref, tok_ref, table_hbm, out_ref, lens_ref,
                 ids_ref, msg_ref, asked_v, asked_s, slot_v, slot_s, table_ref, wide, stage, block, relay, back, emb,
                 relay_z, ids_send, ids_recv, ask_send, ask_recv, copy_sem, send_sem, recv_sem, hop_send, hop_recv,
                 z_send, z_relay_send, z_relay_recv, z_recv, pass_send, pass_recv, own_send, own_recv):
    r, z, y, x, k = place()
    base = r - k
    other = (base + 1 - k, z)
    up, down = (z + 1) % 4, (z + 3) % 4
    holder = z // 2
    column = [(r, (z + s) % 4) for s in (1, 2, 3)]
    plane = [((r + s) % 32, z) for s in range(1, 32)]
    load = pltpu.make_async_copy(table_hbm, table_ref, copy_sem.at[0])
    load.start()
    greet(column + plane + [(base + 1 - k, up), (base + 1 - k, down)])

    copies = []
    for s, device in enumerate(column):
        copy = remote(tok_ref, ids_ref.at[z], ids_send.at[s], ids_recv.at[s], device)
        copy.start()
        copies.append(copy)
    ids_ref[z] = tok_ref[...]
    for copy in copies:
        copy.wait()
    ids = jnp.concatenate(
        [ids_ref[c, h : h + 1, 128 * j : 128 * j + 128] for c in range(4) for h in range(2) for j in range(4)], axis=0)
    requests(ids, (len_ref[0], len_ref[1]), msg_ref, slot_v)

    copies = []
    for s, device in enumerate(plane):
        copy = remote(msg_ref.at[device[0]], asked_v.at[r], ask_send.at[s], ask_recv.at[s], device)
        copy.start()
        copies.append(copy)
    asked_v[r] = msg_ref[r]
    to_slots = pltpu.make_async_copy(slot_v, slot_s, copy_sem.at[1])
    to_slots.start()
    load.wait()

    def widen(i, _):
        rows = pl.ds(pl.multiple_of(i * 256, 256), 256)
        wide[rows, :] = table_ref[rows, :].astype(F32)
        return 0

    lax.fori_loop(0, 64, widen, 0)
    for copy in copies:
        copy.wait()
    asked_v[...] = jnp.clip(asked_v[...], 0, 16383)
    to_asked = pltpu.make_async_copy(asked_v, asked_s, copy_sem.at[2])
    to_asked.start()
    to_asked.wait()
    to_slots.wait()
    lens_ref[...] = asked_v[base + holder, 0:1, :]

    def row(dy, dx, dk):
        return (((y + dy) % 4) * 4 + (x + dx) % 4) * 2 + (k + dk) % 2

    def fill(p, dst):
        def some(j, _):
            for i in range(CAP // 4):
                stage[pl.ds(j * (CAP // 4) + i, 1), :] = wide[pl.ds(asked_s[p, j, i], 1), :]
            return 0

        lax.fori_loop(0, 4, some, 0)
        dst[...] = stage[0:CAP, :].astype(BF)

    flows = routes()
    hops = [f for f in flows if f[3] is not None]
    direct = [f for f in flows if f[3] is None]
    first, final, waiting = [], [], None
    for n, (dy, dx, dk, hop) in enumerate(hops + direct):
        p = row(dy, dx, dk)
        fill(p, block.at[n])
        if hop is not None:
            copy = remote(block.at[n], relay.at[n], hop_send.at[n], hop_recv.at[n], (row(*hop, 0), z))
            first.append(copy)
        else:
            i = n - len(hops)
            copy = remote(block.at[n], back.at[r], send_sem.at[i], recv_sem.at[i], (p, z))
            final.append((copy, row(-dy, -dx, dk)))
        if waiting is not None:
            waiting.start()
        waiting = copy
    fill(r, back.at[r])
    waiting.start()
    for i, (dy, dx, dk, (hy, hx)) in enumerate(hops):
        first[i].wait_recv()
        n = len(direct) + i
        copy = remote(relay.at[i], back.at[row(-hy, -hx, 0)], send_sem.at[n], recv_sem.at[n],
                      (row(dy - hy, dx - hx, dk), z))
        copy.start()
        final.append((copy, row(-dy, -dx, dk)))

    def spread(source):
        wide[pl.ds(pl.multiple_of(source * CAP, 8), CAP), :] = back[source].astype(F32)

    spread(r)
    for copy, source in final:
        copy.wait_recv()
        spread(source)

    mine = pl.ds(pl.multiple_of(1024 * k, 1024), 1024)
    theirs = pl.ds(pl.multiple_of(1024 * (1 - k), 1024), 1024)

    def part(i):
        return pl.ds(1024 * i, 1024)

    def far(h, half):
        return remote(emb.at[h, part(half)], relay_z, z_relay_send.at[half], z_relay_recv,
                      (base + half, up if half == 0 else down))

    def near(h, half, step):
        return remote(emb.at[h, part(half)], out_ref.at[z, part(half)],
                      z_send.at[step // 2, half], z_recv.at[step // 2], (base + half, (z + step) % 4))

    def own(h, half):
        return remote(emb.at[h, part(half)], out_ref.at[z, part(half)], own_send.at[half], own_recv.at[half], other)

    def send(h, half, act):
        dist = (2 * k + h - z) % 4

        @pl.when(dist == 2)
        def _():
            act(far(h, half))

        for step in (1, 3):
            @pl.when(dist == step)
            def _():
                act(near(h, half, step))

        @pl.when(dist == 0)
        def _():
            act(own(h, half))

    lead = jnp.where((2 * k - z) % 4 < 2, 1, 0)
    pieces = [(h, half) for h in (lead, 1 - lead) for half in range(2)]
    waiting = None
    for h, half in pieces:
        def gather(j, _):
            a = (half * 2 + j // 4) * 8 + h * 4 + lax.rem(j, 4)
            for i in range(128):
                stage[pl.ds(j * 128 + i, 1), :] = wide[pl.ds(slot_s[a, i], 1), :]
            return 0

        lax.fori_loop(0, 8, gather, 0)
        emb[h, part(half), :] = stage[...].astype(BF)

        @pl.when((2 * k + h - z) % 4 == 0)
        def _():
            out_ref[z, part(half), :] = stage[...].astype(BF)

        if waiting is not None:
            send(*waiting, lambda copy: copy.start())
        waiting = (h, half)
    send(*waiting, lambda copy: copy.start())

    behind = jnp.where(k == 0, down, up)
    ahead = jnp.where(k == 0, up, down)
    relayed = remote(relay_z, out_ref.at[behind, mine], pass_send.at[3], z_recv.at[2], (r, ahead))
    far(0, 0).wait_recv()
    relayed.start()
    passed = []
    for i, source in enumerate((down, up, (z + 2) % 4)):
        got = out_ref.at[source, mine]
        remote(got, got, pass_send.at[i], z_recv.at[i], other).wait_recv()
        copy = remote(got, got, pass_send.at[i], pass_recv.at[i], other)
        copy.start()
        passed.append(copy)
    for copy in first:
        copy.wait_send()
    for copy, _ in final:
        copy.wait_send()

    for i, source in enumerate((down, up, (z + 2) % 4)):
        passed[i].wait_send()
        got = out_ref.at[source, theirs]
        remote(got, got, pass_send.at[i], pass_recv.at[i], other).wait_recv()
    relayed.wait_send()
    for h, half in pieces:
        send(h, half, lambda copy: copy.wait_send())

    @pl.when(k != holder)
    def _():
        for half in range(2):
            own(0, half).wait_recv()


def layer_kernel(len_ref, x_ref, gain_ref, wqkv_ref, wout_ref, gain2_ref, win_hbm, wdown_hbm, out_ref,
                 nrm, qs, ke, ko, vt, wvt, sc, att, hid, act, obuf, relay, win_ref, wdown_ref, sems,
                 send_sem, far_recv, recv_sem, pass_send):
    r, z, _, _, k = place()
    base = r - k
    up, down = (z + 1) % 4, (z + 3) % 4
    holder, slot = z // 2, z % 2
    peers = [(base + 1 - k, z)]
    for kk in range(2):
        for s in (1, 3):
            peers.append((base + kk, (z + s) % 4))
    barrier = pltpu.get_barrier_semaphore()
    for device in peers:
        pl.semaphore_signal(barrier, inc=1, device_id=device, device_id_type=MESH)
    get_in = pltpu.make_async_copy(win_hbm, win_ref, sems.at[0])
    get_down = pltpu.make_async_copy(wdown_hbm, wdown_ref, sems.at[1])
    get_in.start()
    get_down.start()
    length = len_ref[0, 126 + z % 2]
    ahead, behind = jnp.where(k == 0, up, down), jnp.where(k == 0, down, up)

    def quarter_of(step):
        return jnp.where(step == 0, (z + 2) % 4, jnp.where(step == 1, ahead, jnp.where(step == 2, behind, z)))

    def half_of(quarter):
        return (quarter + k) % 2

    def rows_of(half):
        return pl.ds(pl.multiple_of(256 * half, 256), 256)

    def block(step):
        return obuf.at[pl.ds(256 * step, 256)]

    def landing(step):
        return out_ref.at[slot, rows_of(half_of(quarter_of(step)))]

    def far():
        return remote(block(0), relay, send_sem.at[0], far_recv, (r, ahead))

    def near(step):
        q = quarter_of(step)
        return remote(block(step), landing(step), send_sem.at[step], recv_sem.at[slot, half_of(q)], (base + holder, q))

    def own():
        return remote(block(3), landing(3), send_sem.at[3], recv_sem.at[slot, half_of(z)], (base + 1 - k, z))

    def passing():
        half = half_of(ahead)
        return remote(relay, out_ref.at[behind % 2, rows_of(half)], pass_send, recv_sem.at[behind % 2, half],
                      (base + behind // 2, ahead))

    for c in range(4):
        wvt[128 * c : 128 * c + 128, :] = wqkv_ref[:, 2 * D + 128 * c : 2 * D + 128 * c + 128].astype(F32).T.astype(BF)

    def project(i, _):
        rows = pl.ds(pl.multiple_of(i * 512, 512), 512)
        parts = [x_ref[c, rows, :].astype(F32) for c in range(4)]
        square = parts[0] * parts[0]
        for part in parts[1:]:
            square = square + part * part
        scale = lax.rsqrt(jnp.sum(square, axis=1, keepdims=True) * (1.0 / D) + 1e-6)
        here = jnp.concatenate(
            [(parts[c] * scale * gain_ref[:, 128 * c : 128 * c + 128]).astype(BF) for c in range(4)], axis=1)
        nrm[rows, :] = here
        keys = dot(here, wqkv_ref[:, D : 2 * D])
        vals = dot_t(wvt[...], here)
        lane = lax.broadcasted_iota(jnp.int32, (512, 128), 1)
        pos = lax.broadcasted_iota(jnp.int32, (512, 128), 0) + i * 512
        bias = jnp.where(pos < length, 0.0, NEG)
        tail = jnp.where(lax.broadcasted_iota(jnp.int32, (16, 512), 0) == 0, 1.0, 0.0).astype(BF)
        for c in range(4):
            cols = slice(128 * c, 128 * c + 128)
            ke[rows, cols] = jnp.where(lane == 64, bias, keys[:, cols]).astype(BF)
            ko[rows, cols] = jnp.where(lane == 0, bias, keys[:, cols]).astype(BF)
        for h in range(8):
            vt[h, 0:64, rows] = vals[64 * h : 64 * h + 64, :].astype(BF)
            vt[h, 64:80, rows] = tail
        return 0

    lax.fori_loop(0, 4, project, 0)
    pl.semaphore_wait(barrier, len(peers))

    def attend(n, at):
        lane = lax.broadcasted_iota(jnp.int32, (256, 128), 1)
        tri = (lax.broadcasted_iota(jnp.int32, (256, 256), 0)
               <= lax.broadcasted_iota(jnp.int32, (256, 256), 1))

        def columns(hp):
            return pl.ds(pl.multiple_of(hp * 128, 128), 128)

        def query(hp, odd):
            q = qs[:, columns(hp)].astype(F32)
            if odd:
                return jnp.where(lane >= 64, q, jnp.where(lane == 0, 1.0, 0.0)).astype(BF)
            return jnp.where(lane < 64, q, jnp.where(lane == 64, 1.0, 0.0)).astype(BF)

        def score(hp, odd, qa, c, top):
            s = dot_t((ko if odd else ke)[256 * c : 256 * c + 256, columns(hp)], qa)
            if c == n - 1:
                s = jnp.where(tri, s, NEG)
            sc[odd, c] = s
            m = jnp.max(s.reshape(4, 8, 8, 256), axis=1)
            return m if top is None else jnp.maximum(top, m)

        def finish(top):
            return jnp.max(jnp.max(top, axis=0), axis=0, keepdims=True)

        qa, top = query(0, 0), None
        for c in range(n):
            top = score(0, 0, qa, c, top)

        def heads(hp, top):
            outs = []
            for odd in range(2):
                hp_next = hp if odd == 0 else jnp.minimum(hp + 1, 3)
                qa, top_next, acc = query(hp_next, 1 - odd), None, None
                for c in range(n):
                    top_next = score(hp_next, 1 - odd, qa, c, top_next)
                    p = jnp.exp2(sc[odd, c] - top).astype(BF)
                    o = dot(vt[2 * hp + odd, :, 256 * c : 256 * c + 256], p)
                    acc = o if acc is None else acc + o
                outs.append(acc[0:64, :] / acc[64:65, :])
                top = finish(top_next)
            att[at, columns(hp)] = jnp.concatenate(outs, axis=0).T.astype(BF)
            return top

        lax.fori_loop(0, 4, heads, finish(top))

    def mlp(steps):
        rows = slice(0, 256 * len(steps))
        resid = []
        for step in steps:
            quarter = quarter_of(step)
            src = pl.ds(pl.multiple_of(quarter * 512 + half_of(quarter) * 256, 256), 256)
            resid.append(jnp.concatenate([x_ref[c, src, :].astype(F32) for c in range(4)], axis=1))
        hidden = (jnp.concatenate(resid, axis=0) + dot(att[rows, :], wout_ref[...])).astype(BF)
        hid[rows, :] = hidden
        hidden = hidden.astype(F32)
        scale = lax.rsqrt(jnp.mean(hidden * hidden, axis=1, keepdims=True) + 1e-6)
        att[rows, :] = (hidden * scale * gain2_ref[...]).astype(BF)
        for f in range(0, FF, 256):
            gate = dot(att[rows, :], win_ref[:, f : f + 256])
            high = dot(att[rows, :], win_ref[:, FF + f : FF + f + 256])
            act[rows, f : f + 256] = (gate / (1.0 + jnp.exp(-gate)) * high).astype(BF)
        return (hid[rows, :].astype(F32) + dot(act[rows, :], wdown_ref[...])).astype(BF)

    def run(step, _):
        quarter = quarter_of(step)
        half = half_of(quarter)

        @pl.when(step == 3)
        def _():
            far().wait_recv()
            passing().start()

        src = pl.ds(pl.multiple_of(quarter * 512 + half * 256, 256), 256)
        qs[...] = (dot(nrm[src, :], wqkv_ref[:, :D]) * (0.125 * LOG2E)).astype(BF)
        at = rows_of(jnp.where(step == 1, 1, 0))
        for n in range(1, 9):
            @pl.when(2 * quarter + half + 1 == n)
            def _():
                attend(n, at)

        @pl.when(step == 1)
        def _():
            get_in.wait()
            get_down.wait()
            obuf[0:512, :] = mlp((0, 1))
            far().start()
            near(1).start()

        @pl.when(step >= 2)
        def _():
            out = mlp((step,))
            obuf[pl.ds(pl.multiple_of(256 * step, 256), 256), :] = out

            @pl.when(step == 2)
            def _():
                near(2).start()

            @pl.when((step == 3) & (holder == k))
            def _():
                out_ref[slot, rows_of(half), :] = out

            @pl.when((step == 3) & (holder != k))
            def _():
                own().start()

        return 0

    lax.fori_loop(0, 4, run, 0)

    for h in range(2):
        for b in range(2):
            @pl.when((2 * k + h != z) | ((z + k) % 2 != b))
            def _():
                remote(block(0), out_ref.at[h, pl.ds(256 * b, 256)], send_sem.at[0], recv_sem.at[h, b],
                       (base + 1 - k, z)).wait_recv()
    far().wait_send()
    near(1).wait_send()
    near(2).wait_send()

    @pl.when(holder != k)
    def _():
        own().wait_send()

    passing().wait_send()


def local(token_ids, lengths, table, attn_gain, w_qkv, w_out, mlp_gain, w_in, w_down):
    dma = pltpu.SemaphoreType.DMA
    full, lens = pl.pallas_call(
        front_kernel,
        out_shape=[jax.ShapeDtypeStruct((4, 2048, 128), BF), jax.ShapeDtypeStruct((1, 128), jnp.int32)],
        in_specs=[SM, VM, ANY], out_specs=[VM, VM],
        scratch_shapes=[
            pltpu.VMEM((4, 2, 512), jnp.int32), pltpu.VMEM((32, 4, 128), jnp.int32), pltpu.VMEM((32, 4, 128), jnp.int32),
            pltpu.SMEM((32, 4, 128), jnp.int32), pltpu.VMEM((32, 128), jnp.int32), pltpu.SMEM((32, 128), jnp.int32),
            pltpu.VMEM((16384, 128), BF), pltpu.VMEM((16384, 128), F32), pltpu.VMEM((1024, 128), F32),
            pltpu.VMEM((31, CAP, 128), BF), pltpu.VMEM((14, CAP, 128), BF), pltpu.VMEM((32, CAP, 128), BF),
            pltpu.VMEM((2, 2048, 128), BF), pltpu.VMEM((1024, 128), BF),
            dma((3,)), dma((3,)), dma((31,)), dma((31,)), dma((3,)), dma((31,)), dma((31,)), dma((14,)), dma((14,)),
            dma((2, 2)), dma((2,)), dma, dma((3,)), dma((4,)), dma((3,)), dma((2,)), dma((2,))],
        compiler_params=params(1),
    )(lengths, token_ids, table)
    return pl.pallas_call(
        layer_kernel,
        out_shape=jax.ShapeDtypeStruct((2, 512, D), BF),
        in_specs=[SM, VM, VM, VM, VM, VM, ANY, ANY], out_specs=VM,
        scratch_shapes=[pltpu.VMEM((2048, D), BF), pltpu.VMEM((256, D), BF), pltpu.VMEM((2048, D), BF),
                        pltpu.VMEM((2048, D), BF), pltpu.VMEM((8, 80, 2048), BF), pltpu.VMEM((D, D), BF),
                        pltpu.VMEM((2, 8, 256, 256), F32), pltpu.VMEM((512, D), BF), pltpu.VMEM((512, D), BF),
                        pltpu.VMEM((512, FF), BF), pltpu.VMEM((1024, D), BF), pltpu.VMEM((256, D), BF),
                        pltpu.VMEM((D, 2 * FF), BF), pltpu.VMEM((FF, D), BF), dma((2,)),
                        dma((4,)), dma, dma((2, 2)), dma],
        compiler_params=params(2),
    )(lens, full, attn_gain.reshape(1, D), w_qkv, w_out, mlp_gain.reshape(1, D), w_in, w_down)


def solution(mesh):
    in_specs = (P("rows", "cols"), P("rows"), P("rows", "cols"), P(), P(), P(), P(), P(), P())
    return jax.shard_map(local, mesh=mesh, in_specs=in_specs, out_specs=P("rows", "cols", None), check_vma=False)
```

```python
import functools

import jax
import jax.numpy as jnp
from jax import lax
from jax.experimental import pallas as pl
from jax.experimental.pallas import tpu as pltpu
from jax.sharding import PartitionSpec as P

D = 512
FF = 2048
CAP = 344
BF = jnp.bfloat16
F32 = jnp.float32
MESH = pl.DeviceIdType.MESH
ANY = pl.BlockSpec(memory_space=pl.ANY)
VM = pl.BlockSpec(memory_space=pltpu.VMEM)
SM = pl.BlockSpec(memory_space=pltpu.SMEM)
LOG2E = 1.4426950408889634
NEG = -1e30


def dot(a, b):
    return jnp.dot(a, b, preferred_element_type=F32)


def dot_t(a, b):
    return lax.dot_general(a, b, (((1,), (1,)), ((), ())), preferred_element_type=F32)


def place():
    r, z = lax.axis_index("rows"), lax.axis_index("cols")
    return r, z, r // 8, (r // 2) % 4, r % 2


def greet(devices):
    barrier = pltpu.get_barrier_semaphore()
    for device in devices:
        pl.semaphore_signal(barrier, inc=1, device_id=device, device_id_type=MESH)
    pl.semaphore_wait(barrier, len(devices))


def remote(src, dst, send_sem, recv_sem, device):
    return pltpu.make_async_remote_copy(
        src_ref=src, dst_ref=dst, send_sem=send_sem, recv_sem=recv_sem,
        device_id=device, device_id_type=MESH)


def params(collective_id=None, vmem=60):
    kw = {}
    if collective_id is not None:
        kw = dict(collective_id=collective_id, has_side_effects=True)
    return pltpu.CompilerParams(vmem_limit_bytes=vmem * 2**20, **kw)


def routes():
    out = []
    for dy in range(4):
        for dx in range(4):
            for dk in range(2):
                if dx == dy == dk == 0:
                    continue
                side = 1 if dk == 0 else 3
                hop = None
                if dx == 2 or dy == 2:
                    hop = (side if dy == 2 else 0, side if dx == 2 else 0)
                out.append((dy, dx, dk, hop))
    key = lambda f: (f[3] is None, (f[0] * 5 + f[1] * 3 + f[2] * 7) % 11)
    return sorted(out, key=key)


def requests(ids, lens, msg_ref, slot_ref):
    before = (lax.broadcasted_iota(jnp.int32, (128, 128), 0)
              < lax.broadcasted_iota(jnp.int32, (128, 128), 1)).astype(F32)
    above = (lax.broadcasted_iota(jnp.int32, (32, 32), 1)
             < lax.broadcasted_iota(jnp.int32, (32, 32), 0)).astype(F32).astype(BF)
    both = jnp.concatenate([before, jnp.ones((128, 128), F32)], axis=0).astype(BF)
    owners = lax.broadcasted_iota(jnp.int32, (32, 128), 0)
    column = lax.broadcasted_iota(jnp.int32, (4 * 128, 128), 0)
    ks = jnp.where((column & 127) < CAP // 4, (column >> 7) * (CAP // 4) + (column & 127), -1)
    lane = lax.broadcasted_iota(jnp.int32, (32, 128), 1)
    owner = ids >> 14
    low, high = (ids & 127).astype(F32), ((ids >> 7) & 127).astype(F32)
    ones = [jnp.where(owner == o, 1.0, 0.0).astype(BF) for o in range(32)]
    rows_above = dot(above, jnp.concatenate(ones, axis=1)).astype(BF)
    prior = dot(
        jnp.concatenate(
            [jnp.concatenate(ones, axis=0),
             jnp.concatenate([rows_above[:, 128 * o : 128 * o + 128] for o in range(32)], axis=0)], axis=1),
        both)
    rank = jnp.zeros((32, 128), F32)
    for o in range(32):
        rank = rank + jnp.where(owner == o, prior[32 * o : 32 * o + 32], 0.0)
    rank_i = rank.astype(jnp.int32)
    slot_ref[...] = jnp.clip(owner * CAP + rank_i, 0, 32 * CAP - 1)
    acc = jnp.zeros((64, 4 * 128), F32)
    for a in range(0, 32, 2):
        lefts, rights = [], []
        for b in (a, a + 1):
            hit = owners == owner[b : b + 1, :]
            lefts.append(jnp.concatenate(
                [jnp.where(hit, low[b : b + 1, :], 0.0), jnp.where(hit, high[b : b + 1, :], 0.0)], axis=0).astype(BF))
            rights.append(jnp.where(ks == rank_i[b : b + 1, :], 1.0, 0.0).astype(BF))
        acc = acc + dot_t(jnp.concatenate(lefts, axis=1), jnp.concatenate(rights, axis=1))
    req = (acc[32:] * 128.0 + acc[:32]).astype(jnp.int32)
    req0 = jnp.where(lane == 126, lens[0], jnp.where(lane == 127, lens[1], req[:, :128]))
    msg_ref[:, 0, :] = req0
    for j in range(1, 4):
        msg_ref[:, j, :] = req[:, 128 * j : 128 * j + 128]


def whole_kernel(len_ref, tok_ref, table_hbm, gain_ref, wqkv_hbm, wout_hbm, gain2_ref, win_hbm, wdown_hbm, out_ref, *rest):
    front, layer = rest[: -len(LAYER)], rest[-len(LAYER) :]
    start, prepare, project, late = layer_kernel(
        gain_ref, wqkv_hbm, wout_hbm, gain2_ref, win_hbm, wdown_hbm, out_ref, layer, front[0])
    front_kernel(len_ref, tok_ref, table_hbm, *front, start, prepare, project)
    late()


def front_kernel(len_ref, tok_ref, table_hbm, out_ref,
                 ids_ref, msg_ref, asked_v, asked_s, slot_v, slot_s, table_ref, wide, stage, block, relay, back, emb,
                 relay_z, ids_send, ids_recv, ask_send, ask_recv, copy_sem, send_sem, recv_sem, hop_send, hop_recv,
                 z_send, z_relay_send, z_relay_recv, z_recv, pass_send, pass_recv, own_send, own_recv, start, prepare, project):
    r, z, y, x, k = place()
    base = r - k
    other = (base + 1 - k, z)
    up, down = (z + 1) % 4, (z + 3) % 4
    holder = z // 2
    column = [(r, (z + s) % 4) for s in (1, 2, 3)]
    plane = [((r + s) % 32, z) for s in range(1, 32)]
    load = pltpu.make_async_copy(table_hbm, table_ref, copy_sem.at[0])
    load.start()
    start()
    greet(column + plane + [(base + 1 - k, up), (base + 1 - k, down)])

    copies = []
    for s, device in enumerate(column):
        copy = remote(tok_ref, ids_ref.at[z], ids_send.at[s], ids_recv.at[s], device)
        copy.start()
        copies.append(copy)
    ids_ref[z] = tok_ref[...]
    for copy in copies:
        copy.wait()
    ids = jnp.concatenate(
        [ids_ref[c, h : h + 1, 128 * j : 128 * j + 128] for c in range(4) for h in range(2) for j in range(4)], axis=0)
    requests(ids, (len_ref[0], len_ref[1]), msg_ref, slot_v)

    copies = []
    for s, device in enumerate(plane):
        copy = remote(msg_ref.at[device[0]], asked_v.at[r], ask_send.at[s], ask_recv.at[s], device)
        copy.start()
        copies.append(copy)
    asked_v[r] = msg_ref[r]
    to_slots = pltpu.make_async_copy(slot_v, slot_s, copy_sem.at[1])
    to_slots.start()
    load.wait()

    def widen(i, _):
        rows = pl.ds(pl.multiple_of(i * 256, 256), 256)
        wide[rows, :] = table_ref[rows, :].astype(F32)
        return 0

    lax.fori_loop(0, 64, widen, 0)
    for copy in copies:
        copy.wait()
    asked_v[...] = jnp.clip(asked_v[...], 0, 16383)
    to_asked = pltpu.make_async_copy(asked_v, asked_s, copy_sem.at[2])
    to_asked.start()
    to_asked.wait()
    to_slots.wait()
    length = asked_s[base + holder, 0, 126 + z % 2]

    def row(dy, dx, dk):
        return (((y + dy) % 4) * 4 + (x + dx) % 4) * 2 + (k + dk) % 2

    def fill(p, dst):
        def some(j, _):
            for i in range(CAP // 4):
                stage[pl.ds(j * (CAP // 4) + i, 1), :] = wide[pl.ds(asked_s[p, j, i], 1), :]
            return 0

        lax.fori_loop(0, 4, some, 0)
        dst[...] = stage[0:CAP, :].astype(BF)

    flows = routes()
    hops = [f for f in flows if f[3] is not None]
    direct = [f for f in flows if f[3] is None]
    first, final, waiting = [], [], None
    for n, (dy, dx, dk, hop) in enumerate(hops + direct):
        p = row(dy, dx, dk)
        fill(p, block.at[n])
        if hop is not None:
            copy = remote(block.at[n], relay.at[n], hop_send.at[n], hop_recv.at[n], (row(*hop, 0), z))
            first.append(copy)
        else:
            i = n - len(hops)
            copy = remote(block.at[n], back.at[r], send_sem.at[i], recv_sem.at[i], (p, z))
            final.append((copy, row(-dy, -dx, dk)))
        if waiting is not None:
            waiting.start()
        waiting = copy
    fill(r, back.at[r])
    waiting.start()
    for i, (dy, dx, dk, (hy, hx)) in enumerate(hops):
        first[i].wait_recv()
        n = len(direct) + i
        copy = remote(relay.at[i], back.at[row(-hy, -hx, 0)], send_sem.at[n], recv_sem.at[n],
                      (row(dy - hy, dx - hx, dk), z))
        copy.start()
        final.append((copy, row(-dy, -dx, dk)))

    prepare()

    def spread(source):
        wide[pl.ds(pl.multiple_of(source * CAP, 8), CAP), :] = back[source].astype(F32)

    spread(r)
    for copy, source in final:
        copy.wait_recv()
        spread(source)

    mine = pl.ds(pl.multiple_of(1024 * k, 1024), 1024)
    theirs = pl.ds(pl.multiple_of(1024 * (1 - k), 1024), 1024)

    def part(i):
        return pl.ds(1024 * i, 1024)

    def far(h, half):
        return remote(emb.at[h, part(half)], relay_z, z_relay_send.at[half], z_relay_recv,
                      (base + half, up if half == 0 else down))

    def near(h, half, step):
        return remote(emb.at[h, part(half)], out_ref.at[z, part(half)],
                      z_send.at[step // 2, half], z_recv.at[step // 2], (base + half, (z + step) % 4))

    def own(h, half):
        return remote(emb.at[h, part(half)], out_ref.at[z, part(half)], own_send.at[half], own_recv.at[half], other)

    def send(h, half, act):
        dist = (2 * k + h - z) % 4

        @pl.when(dist == 2)
        def _():
            act(far(h, half))

        for step in (1, 3):
            @pl.when(dist == step)
            def _():
                act(near(h, half, step))

        @pl.when(dist == 0)
        def _():
            act(own(h, half))

    lead = jnp.where((2 * k - z) % 4 < 2, 1, 0)
    pieces = [(h, half) for h in (lead, 1 - lead) for half in range(2)]
    waiting = None
    for h, half in pieces:
        def gather(j, _):
            a = (half * 2 + j // 4) * 8 + h * 4 + lax.rem(j, 4)
            for i in range(128):
                stage[pl.ds(j * 128 + i, 1), :] = wide[pl.ds(slot_s[a, i], 1), :]
            return 0

        lax.fori_loop(0, 8, gather, 0)
        emb[h, part(half), :] = stage[...].astype(BF)

        @pl.when((2 * k + h - z) % 4 == 0)
        def _():
            out_ref[z, part(half), :] = stage[...].astype(BF)

        if waiting is not None:
            send(*waiting, lambda copy: copy.start())
        waiting = (h, half)
    send(*waiting, lambda copy: copy.start())

    behind = jnp.where(k == 0, down, up)
    ahead = jnp.where(k == 0, up, down)
    relayed = remote(relay_z, out_ref.at[behind, mine], pass_send.at[3], z_recv.at[2], (r, ahead))
    far(0, 0).wait_recv()
    relayed.start()
    passed = []
    for i, source in enumerate((down, up, (z + 2) % 4)):
        got = out_ref.at[source, mine]
        remote(got, got, pass_send.at[i], z_recv.at[i], other).wait_recv()
        copy = remote(got, got, pass_send.at[i], pass_recv.at[i], other)
        copy.start()
        passed.append(copy)
    for copy in first:
        copy.wait_send()
    for copy, _ in final:
        copy.wait_send()

    @pl.when(k != holder)
    def _():
        for half in range(2):
            own(0, half).wait_recv()

    project(2 * k, 2 * k + 2, length)
    for i, source in enumerate((down, up, (z + 2) % 4)):
        passed[i].wait_send()
        got = out_ref.at[source, theirs]
        remote(got, got, pass_send.at[i], pass_recv.at[i], other).wait_recv()
    relayed.wait_send()
    for h, half in pieces:
        send(h, half, lambda copy: copy.wait_send())
    project(2 - 2 * k, 4 - 2 * k, length)


LAYER = [(2048, D, BF), (1024, D, BF), (2048, D, BF), (2048, D, BF), (8, 80, 2048, BF), (D, D, BF), (2, 8, 256, 256, F32),
         (8, 80, 256, F32), (512, D, BF), (512, D, BF), (512, FF, BF), (1024, D, BF), (256, D, BF), (D, 3 * D, BF), (D, D, BF),
         (D, 2 * FF, BF), (FF, D, BF), 4, (4,), (), (2, 2), ()]


def layer_kernel(gain_ref, wqkv_hbm, wout_hbm, gain2_ref, win_hbm, wdown_hbm, out_ref, scratch, x_ref):
    (nrm, qs, ke, ko, vt, wvt, sc, ot, att, hid, act, obuf, relay, wqkv_ref, wout_ref, win_ref, wdown_ref, sems,
     send_sem, far_recv, recv_sem, pass_send) = scratch
    r, z, _, _, k = place()
    base = r - k
    up, down = (z + 1) % 4, (z + 3) % 4
    holder, slot = z // 2, z % 2
    gets = [pltpu.make_async_copy(src, dst, sems.at[i]) for i, (src, dst) in enumerate(
        [(wqkv_hbm, wqkv_ref), (wout_hbm, wout_ref), (win_hbm, win_ref), (wdown_hbm, wdown_ref)])]
    ahead, behind = jnp.where(k == 0, up, down), jnp.where(k == 0, down, up)

    def quarter_of(step):
        return jnp.where(step == 0, (z + 2) % 4, jnp.where(step == 1, ahead, jnp.where(step == 2, behind, z)))

    def half_of(quarter):
        return (quarter + k) % 2

    def rows_of(half):
        return pl.ds(pl.multiple_of(256 * half, 256), 256)

    def block(step):
        return obuf.at[pl.ds(256 * step, 256)]

    def landing(step):
        return out_ref.at[slot, rows_of(half_of(quarter_of(step)))]

    def far():
        return remote(block(0), relay, send_sem.at[0], far_recv, (r, ahead))

    def near(step):
        q = quarter_of(step)
        return remote(block(step), landing(step), send_sem.at[step], recv_sem.at[slot, half_of(q)], (base + holder, q))

    def own():
        return remote(block(3), landing(3), send_sem.at[3], recv_sem.at[slot, half_of(z)], (base + 1 - k, z))

    def passing():
        half = half_of(ahead)
        return remote(relay, out_ref.at[behind % 2, rows_of(half)], pass_send, recv_sem.at[behind % 2, half],
                      (base + behind // 2, ahead))

    def start():
        for get in gets:
            get.start()

    def prepare():
        for get in gets:
            get.wait()
        for c in range(4):
            rows = slice(128 * c, 128 * c + 128)
            wvt[rows, :] = wqkv_ref[:, 2 * D + 128 * c : 2 * D + 128 * c + 128].astype(F32).T.astype(BF)

    def project_rows(low, high, length):
        lax.fori_loop(low, high, functools.partial(project, length), 0)

    def project(length, i, _):
        rows = pl.ds(pl.multiple_of(i * 512, 512), 512)
        parts = [x_ref[c, rows, :].astype(F32) for c in range(4)]
        square = parts[0] * parts[0]
        for part in parts[1:]:
            square = square + part * part
        scale = lax.rsqrt(jnp.sum(square, axis=1, keepdims=True) * (1.0 / D) + 1e-6)
        here = jnp.concatenate(
            [(parts[c] * scale * gain_ref[:, 128 * c : 128 * c + 128]).astype(BF) for c in range(4)], axis=1)
        nrm[rows, :] = here
        keys = dot(here, wqkv_ref[:, D : 2 * D])
        vals = dot_t(wvt[...], here)
        lane = lax.broadcasted_iota(jnp.int32, (512, 128), 1)
        pos = lax.broadcasted_iota(jnp.int32, (512, 128), 0) + i * 512
        bias = jnp.where(pos < length, 0.0, NEG)
        tail = jnp.where(lax.broadcasted_iota(jnp.int32, (16, 512), 0) == 0, 1.0, 0.0).astype(BF)
        for c in range(4):
            cols = slice(128 * c, 128 * c + 128)
            ke[rows, cols] = jnp.where(lane == 64, bias, keys[:, cols]).astype(BF)
            ko[rows, cols] = jnp.where(lane == 0, bias, keys[:, cols]).astype(BF)
        for h in range(8):
            vt[h, 0:64, rows] = vals[64 * h : 64 * h + 64, :].astype(BF)
            vt[h, 64:80, rows] = tail
        return 0


    def attend(n, step):
        lane = lax.broadcasted_iota(jnp.int32, (256, 128), 1)
        tri = (lax.broadcasted_iota(jnp.int32, (256, 256), 0)
               <= lax.broadcasted_iota(jnp.int32, (256, 256), 1))
        here = pl.ds(pl.multiple_of(256 * step, 256), 256)

        def columns(hp):
            return pl.ds(pl.multiple_of(hp * 128, 128), 128)

        def query(hp, odd):
            q = qs[here, columns(hp)].astype(F32)
            if odd:
                return jnp.where(lane >= 64, q, jnp.where(lane == 0, 1.0, 0.0)).astype(BF)
            return jnp.where(lane < 64, q, jnp.where(lane == 64, 1.0, 0.0)).astype(BF)

        def score(hp, odd, qa, c, top):
            s = dot_t((ko if odd else ke)[256 * c : 256 * c + 256, columns(hp)], qa)
            if c == n - 1:
                s = jnp.where(tri, s, NEG)
            sc[odd, c] = s
            m = jnp.max(s.reshape(4, 8, 8, 256), axis=1)
            return m if top is None else jnp.maximum(top, m)

        def finish(top):
            return jnp.max(jnp.max(top, axis=0), axis=0, keepdims=True)

        def pair(hp, tops, more):
            new = []
            for odd in range(2):
                qa, top, acc = query(hp + 1, odd) if more else None, None, None
                for c in range(n):
                    p = jnp.exp2(sc[odd, c] - tops[odd]).astype(BF)
                    o = dot(vt[2 * hp + odd, :, 256 * c : 256 * c + 256], p)
                    acc = o if acc is None else acc + o
                    if more:
                        top = score(hp + 1, odd, qa, c, top)
                ot[2 * hp + odd] = acc
                if more:
                    new.append(finish(top))
            return tuple(new)

        tops = []
        for odd in range(2):
            qa, top = query(0, odd), None
            for c in range(n):
                top = score(0, odd, qa, c, top)
            tops.append(finish(top))
        tops = lax.fori_loop(0, 3, lambda hp, tops: pair(hp, tops, True), tuple(tops))
        pair(3, tops, False)

    def normalise(at):
        for hp in range(4):
            outs = [ot[2 * hp + odd, 0:64, :] / ot[2 * hp + odd, 64:65, :] for odd in range(2)]
            att[at, 128 * hp : 128 * hp + 128] = jnp.concatenate(outs, axis=0).T.astype(BF)

    def mlp(steps):
        rows = slice(0, 256 * len(steps))
        resid = []
        for step in steps:
            quarter = quarter_of(step)
            src = pl.ds(pl.multiple_of(quarter * 512 + half_of(quarter) * 256, 256), 256)
            resid.append(jnp.concatenate([x_ref[c, src, :].astype(F32) for c in range(4)], axis=1))
        hidden = (jnp.concatenate(resid, axis=0) + dot(att[rows, :], wout_ref[...])).astype(BF)
        hid[rows, :] = hidden
        hidden = hidden.astype(F32)
        scale = lax.rsqrt(jnp.mean(hidden * hidden, axis=1, keepdims=True) + 1e-6)
        att[rows, :] = (hidden * scale * gain2_ref[...]).astype(BF)
        for f in range(0, FF, 256):
            gate = dot(att[rows, :], win_ref[:, f : f + 256])
            high = dot(att[rows, :], win_ref[:, FF + f : FF + f + 256])
            act[rows, f : f + 256] = (gate / (1.0 + jnp.exp(-gate)) * high).astype(BF)
        return (hid[rows, :].astype(F32) + dot(act[rows, :], wdown_ref[...])).astype(BF)

    def run(step, _):
        quarter = quarter_of(step)
        half = half_of(quarter)

        @pl.when(step == 3)
        def _():
            far().wait_recv()
            passing().start()

        for n in range(1, 9):
            @pl.when(2 * quarter + half + 1 == n)
            def _():
                attend(n, step)

        normalise(rows_of(jnp.where(step == 1, 1, 0)))

        @pl.when(step == 1)
        def _():
            obuf[0:512, :] = mlp((0, 1))
            far().start()
            near(1).start()

        @pl.when(step >= 2)
        def _():
            out = mlp((step,))
            obuf[pl.ds(pl.multiple_of(256 * step, 256), 256), :] = out

            @pl.when(step == 2)
            def _():
                near(2).start()

            @pl.when((step == 3) & (holder == k))
            def _():
                out_ref[slot, rows_of(half), :] = out

            @pl.when((step == 3) & (holder != k))
            def _():
                own().start()

        return 0

    def late():
        mine = []
        for step in range(4):
            quarter = quarter_of(step)
            src = pl.ds(pl.multiple_of(quarter * 512 + half_of(quarter) * 256, 256), 256)
            mine.append(nrm[src, :])
        qs[...] = (dot(jnp.concatenate(mine, axis=0), wqkv_ref[:, :D]) * (0.125 * LOG2E)).astype(BF)
        lax.fori_loop(0, 4, run, 0)

        for h in range(2):
            for b in range(2):
                @pl.when((2 * k + h != z) | ((z + k) % 2 != b))
                def _():
                    remote(block(0), out_ref.at[h, pl.ds(256 * b, 256)], send_sem.at[0], recv_sem.at[h, b],
                           (base + 1 - k, z)).wait_recv()
        far().wait_send()
        near(1).wait_send()
        near(2).wait_send()

        @pl.when(holder != k)
        def _():
            own().wait_send()

        passing().wait_send()

    return start, prepare, project_rows, late


def local(token_ids, lengths, table, attn_gain, w_qkv, w_out, mlp_gain, w_in, w_down):
    dma = pltpu.SemaphoreType.DMA
    layer = []
    for entry in LAYER:
        if isinstance(entry, tuple) and entry and not isinstance(entry[-1], int):
            layer.append(pltpu.VMEM(entry[:-1], entry[-1]))
        else:
            layer.append(dma if entry == () else dma((entry,) if isinstance(entry, int) else entry))
    return pl.pallas_call(
        whole_kernel,
        out_shape=jax.ShapeDtypeStruct((2, 512, D), BF),
        in_specs=[SM, VM, ANY, VM, ANY, ANY, VM, ANY, ANY], out_specs=VM,
        scratch_shapes=[
            pltpu.VMEM((4, 2048, 128), BF),
            pltpu.VMEM((4, 2, 512), jnp.int32), pltpu.VMEM((32, 4, 128), jnp.int32), pltpu.VMEM((32, 4, 128), jnp.int32),
            pltpu.SMEM((32, 4, 128), jnp.int32), pltpu.VMEM((32, 128), jnp.int32), pltpu.SMEM((32, 128), jnp.int32),
            pltpu.VMEM((16384, 128), BF), pltpu.VMEM((16384, 128), F32), pltpu.VMEM((1024, 128), F32),
            pltpu.VMEM((31, CAP, 128), BF), pltpu.VMEM((14, CAP, 128), BF), pltpu.VMEM((32, CAP, 128), BF),
            pltpu.VMEM((2, 2048, 128), BF), pltpu.VMEM((1024, 128), BF),
            dma((3,)), dma((3,)), dma((31,)), dma((31,)), dma((3,)), dma((31,)), dma((31,)), dma((14,)), dma((14,)),
            dma((2, 2)), dma((2,)), dma, dma((3,)), dma((4,)), dma((3,)), dma((2,)), dma((2,))] + layer,
        compiler_params=params(1, 63),
    )(lengths, token_ids, table, attn_gain.reshape(1, D), w_qkv, w_out, mlp_gain.reshape(1, D), w_in, w_down)


def solution(mesh):
    in_specs = (P("rows", "cols"), P("rows"), P("rows", "cols"), P(), P(), P(), P(), P(), P())
    return jax.shard_map(local, mesh=mesh, in_specs=in_specs, out_specs=P("rows", "cols", None), check_vma=False)
```

```python
import jax
import jax.numpy as jnp
from jax import lax
from jax.experimental import pallas as pl
from jax.experimental.pallas import tpu as pltpu
from jax.sharding import PartitionSpec as P

D = 512
FF = 2048
CAP = 344
BF = jnp.bfloat16
F32 = jnp.float32
MESH = pl.DeviceIdType.MESH
ANY = pl.BlockSpec(memory_space=pl.ANY)
VM = pl.BlockSpec(memory_space=pltpu.VMEM)
SM = pl.BlockSpec(memory_space=pltpu.SMEM)
LOG2E = 1.4426950408889634
NEG = -1e30


def dot(a, b):
    return jnp.dot(a, b, preferred_element_type=F32)


def dot_t(a, b):
    return lax.dot_general(a, b, (((1,), (1,)), ((), ())), preferred_element_type=F32)


def place():
    r, z = lax.axis_index("rows"), lax.axis_index("cols")
    return r, z, r // 8, (r // 2) % 4, r % 2


def greet(devices):
    barrier = pltpu.get_barrier_semaphore()
    for device in devices:
        pl.semaphore_signal(barrier, inc=1, device_id=device, device_id_type=MESH)
    pl.semaphore_wait(barrier, len(devices))


def remote(src, dst, send_sem, recv_sem, device):
    return pltpu.make_async_remote_copy(
        src_ref=src, dst_ref=dst, send_sem=send_sem, recv_sem=recv_sem,
        device_id=device, device_id_type=MESH)


def params(collective_id=None, vmem=60):
    kw = {}
    if collective_id is not None:
        kw = dict(collective_id=collective_id, has_side_effects=True)
    return pltpu.CompilerParams(vmem_limit_bytes=vmem * 2**20, **kw)


def routes():
    out = []
    for dy in range(4):
        for dx in range(4):
            for dk in range(2):
                if dx == dy == dk == 0:
                    continue
                side = 1 if dk == 0 else 3
                hop = None
                if dx == 2 or dy == 2:
                    hop = (side if dy == 2 else 0, side if dx == 2 else 0)
                out.append((dy, dx, dk, hop))
    key = lambda f: (f[3] is None, (f[0] * 5 + f[1] * 3 + f[2] * 7) % 11)
    return sorted(out, key=key)


def requests(ids, lens, msg_ref, slot_ref):
    before = (lax.broadcasted_iota(jnp.int32, (128, 128), 0)
              < lax.broadcasted_iota(jnp.int32, (128, 128), 1)).astype(F32)
    above = (lax.broadcasted_iota(jnp.int32, (32, 32), 1)
             < lax.broadcasted_iota(jnp.int32, (32, 32), 0)).astype(F32).astype(BF)
    both = jnp.concatenate([before, jnp.ones((128, 128), F32)], axis=0).astype(BF)
    owners = lax.broadcasted_iota(jnp.int32, (32, 128), 0)
    column = lax.broadcasted_iota(jnp.int32, (4 * 128, 128), 0)
    ks = jnp.where((column & 127) < CAP // 4, (column >> 7) * (CAP // 4) + (column & 127), -1)
    lane = lax.broadcasted_iota(jnp.int32, (32, 128), 1)
    owner = ids >> 14
    low, high = (ids & 127).astype(F32), ((ids >> 7) & 127).astype(F32)
    ones = [jnp.where(owner == o, 1.0, 0.0).astype(BF) for o in range(32)]
    rows_above = dot(above, jnp.concatenate(ones, axis=1)).astype(BF)
    prior = dot(
        jnp.concatenate(
            [jnp.concatenate(ones, axis=0),
             jnp.concatenate([rows_above[:, 128 * o : 128 * o + 128] for o in range(32)], axis=0)], axis=1),
        both)
    rank = jnp.zeros((32, 128), F32)
    for o in range(32):
        rank = rank + jnp.where(owner == o, prior[32 * o : 32 * o + 32], 0.0)
    rank_i = rank.astype(jnp.int32)
    slot_ref[...] = jnp.clip(owner * CAP + rank_i, 0, 32 * CAP - 1)
    acc = jnp.zeros((64, 4 * 128), F32)
    for a in range(0, 32, 2):
        lefts, rights = [], []
        for b in (a, a + 1):
            hit = owners == owner[b : b + 1, :]
            lefts.append(jnp.concatenate(
                [jnp.where(hit, low[b : b + 1, :], 0.0), jnp.where(hit, high[b : b + 1, :], 0.0)], axis=0).astype(BF))
            rights.append(jnp.where(ks == rank_i[b : b + 1, :], 1.0, 0.0).astype(BF))
        acc = acc + dot_t(jnp.concatenate(lefts, axis=1), jnp.concatenate(rights, axis=1))
    req = (acc[32:] * 128.0 + acc[:32]).astype(jnp.int32)
    req0 = jnp.where(lane == 126, lens[0], jnp.where(lane == 127, lens[1], req[:, :128]))
    msg_ref[:, 0, :] = req0
    for j in range(1, 4):
        msg_ref[:, j, :] = req[:, 128 * j : 128 * j + 128]


def whole_kernel(len_ref, tok_ref, table_hbm, gain_ref, wqkv_hbm, wout_hbm, gain2_ref, win_hbm, wdown_hbm, out_ref, *rest):
    front, layer = rest[: -len(LAYER)], rest[-len(LAYER) :]
    start, prepare, project, late = layer_kernel(
        gain_ref, wqkv_hbm, wout_hbm, gain2_ref, win_hbm, wdown_hbm, out_ref, layer, front[0])
    front_kernel(len_ref, tok_ref, table_hbm, *front, start, prepare, project)
    late()


def front_kernel(len_ref, tok_ref, table_hbm, out_ref,
                 ids_ref, msg_ref, asked_v, asked_s, slot_v, slot_s, table_ref, wide, stage, block, relay, back, emb,
                 relay_z, ids_send, ids_recv, ask_send, ask_recv, copy_sem, send_sem, recv_sem, hop_send, hop_recv,
                 z_send, z_relay_send, z_relay_recv, z_recv, relay_pass, pass_send, pass_recv, own_send, own_recv, start, prepare, project):
    r, z, y, x, k = place()
    base = r - k
    other = (base + 1 - k, z)
    up, down = (z + 1) % 4, (z + 3) % 4
    holder = z // 2
    column = [(r, (z + s) % 4) for s in (1, 2, 3)]
    plane = [((r + s) % 32, z) for s in range(1, 32)]
    load = pltpu.make_async_copy(table_hbm, table_ref, copy_sem.at[0])
    load.start()
    start()
    greet(column + plane + [(base + 1 - k, up), (base + 1 - k, down)])

    copies = []
    for s, device in enumerate(column):
        copy = remote(tok_ref, ids_ref.at[z], ids_send.at[s], ids_recv.at[s], device)
        copy.start()
        copies.append(copy)
    ids_ref[z] = tok_ref[...]
    for copy in copies:
        copy.wait()
    ids = jnp.concatenate(
        [ids_ref[c, h : h + 1, 128 * j : 128 * j + 128] for c in range(4) for h in range(2) for j in range(4)], axis=0)
    requests(ids, (len_ref[0], len_ref[1]), msg_ref, slot_v)

    copies = []
    for s, device in enumerate(plane):
        copy = remote(msg_ref.at[device[0]], asked_v.at[r], ask_send.at[s], ask_recv.at[s], device)
        copy.start()
        copies.append(copy)
    asked_v[r] = msg_ref[r]
    to_slots = pltpu.make_async_copy(slot_v, slot_s, copy_sem.at[1])
    to_slots.start()
    load.wait()

    def widen(i, _):
        rows = pl.ds(pl.multiple_of(i * 256, 256), 256)
        wide[rows, :] = table_ref[rows, :].astype(F32)
        return 0

    lax.fori_loop(0, 64, widen, 0)
    for copy in copies:
        copy.wait()
    asked_v[...] = jnp.clip(asked_v[...], 0, 16383)
    to_asked = pltpu.make_async_copy(asked_v, asked_s, copy_sem.at[2])
    to_asked.start()
    to_asked.wait()
    to_slots.wait()
    length = asked_s[base + holder, 0, 126 + z % 2]

    def row(dy, dx, dk):
        return (((y + dy) % 4) * 4 + (x + dx) % 4) * 2 + (k + dk) % 2

    def fill(p, dst):
        def some(j, _):
            for i in range(CAP // 4):
                stage[pl.ds(j * (CAP // 4) + i, 1), :] = wide[pl.ds(asked_s[p, j, i], 1), :]
            return 0

        lax.fori_loop(0, 4, some, 0)
        dst[...] = stage[0:CAP, :].astype(BF)

    flows = routes()
    hops = [f for f in flows if f[3] is not None]
    direct = [f for f in flows if f[3] is None]
    first, final, waiting = [], [], None
    for n, (dy, dx, dk, hop) in enumerate(hops + direct):
        p = row(dy, dx, dk)
        fill(p, block.at[n])
        if hop is not None:
            copy = remote(block.at[n], relay.at[n], hop_send.at[n], hop_recv.at[n], (row(*hop, 0), z))
            first.append(copy)
        else:
            i = n - len(hops)
            copy = remote(block.at[n], back.at[r], send_sem.at[i], recv_sem.at[i], (p, z))
            final.append((copy, row(-dy, -dx, dk)))
        if waiting is not None:
            waiting.start()
        waiting = copy
    fill(r, back.at[r])
    waiting.start()
    for i, (dy, dx, dk, (hy, hx)) in enumerate(hops):
        first[i].wait_recv()
        n = len(direct) + i
        copy = remote(relay.at[i], back.at[row(-hy, -hx, 0)], send_sem.at[n], recv_sem.at[n],
                      (row(dy - hy, dx - hx, dk), z))
        copy.start()
        final.append((copy, row(-dy, -dx, dk)))

    prepare()

    def spread(source):
        wide[pl.ds(pl.multiple_of(source * CAP, 8), CAP), :] = back[source].astype(F32)

    spread(r)
    for copy, source in final:
        copy.wait_recv()
        spread(source)

    def rows(c):
        return pl.ds(pl.multiple_of(512 * c, 512), 512)

    def far(h, c):
        return remote(emb.at[h, rows(c)], relay_z.at[rows(c % 2)], z_relay_send.at[c], z_relay_recv.at[c % 2],
                      (base + c // 2, (up, down)[c // 2]))

    def near(h, c, step):
        return remote(emb.at[h, rows(c)], out_ref.at[z, rows(c)],
                      z_send.at[step // 2, c], z_recv.at[step // 2, c % 2], (base + c // 2, (z + step) % 4))

    def own(h, c):
        return remote(emb.at[h, rows(c)], out_ref.at[z, rows(c)], own_send.at[c], own_recv.at[c], other)

    def send(h, c, act):
        dist = (2 * k + h - z) % 4

        @pl.when(dist == 2)
        def _():
            act(far(h, c))

        for step in (1, 3):
            @pl.when(dist == step)
            def _():
                act(near(h, c, step))

        @pl.when(dist == 0)
        def _():
            act(own(h, c))

    lead = jnp.where((2 * k - z) % 4 < 2, 1, 0)
    pieces = [(h, c) for h in (lead, 1 - lead) for c in (0, 2, 1, 3)]
    waiting = None
    for h, c in pieces:
        def gather(j, _):
            a = c * 8 + h * 4 + j
            for i in range(128):
                stage[pl.ds(j * 128 + i, 1), :] = wide[pl.ds(slot_s[a, i], 1), :]
            return 0

        lax.fori_loop(0, 4, gather, 0)
        emb[h, rows(c), :] = stage[0:512, :].astype(BF)

        @pl.when((2 * k + h - z) % 4 == 0)
        def _():
            out_ref[z, rows(c), :] = stage[0:512, :].astype(BF)

        if waiting is not None:
            send(*waiting, lambda copy: copy.start())
        waiting = (h, c)
    send(*waiting, lambda copy: copy.start())

    behind = jnp.where(k == 0, down, up)
    ahead = jnp.where(k == 0, up, down)
    sources = (down, up, (z + 2) % 4)
    relayed = []
    for j in range(2):
        copy = remote(relay_z.at[rows(j)], out_ref.at[behind, rows(2 * k + j)], relay_pass.at[j], z_recv.at[2, j], (r, ahead))
        far(0, j).wait_recv()
        copy.start()
        relayed.append(copy)
    passed = []
    for j in range(2):
        for i, source in enumerate(sources):
            got = out_ref.at[source, rows(2 * k + j)]
            remote(got, got, pass_send.at[i, j], z_recv.at[i, j], other).wait_recv()
            copy = remote(got, got, pass_send.at[i, j], pass_recv.at[i, j], other)
            copy.start()
            passed.append(copy)

        if j == 0:
            @pl.when(k != holder)
            def _():
                for c in range(4):
                    own(0, c).wait_recv()

        project(2 * k + j, length)
    for j in range(2):
        for i, source in enumerate(sources):
            got = out_ref.at[source, rows(2 * (1 - k) + j)]
            remote(got, got, pass_send.at[i, j], pass_recv.at[i, j], other).wait_recv()
        project(2 * (1 - k) + j, length)
    for copy in first:
        copy.wait_send()
    for copy, _ in final:
        copy.wait_send()
    for copy in passed + relayed:
        copy.wait_send()
    for h, c in pieces:
        send(h, c, lambda copy: copy.wait_send())


LAYER = [(2048, D, BF), (1024, D, BF), (2048, D, BF), (2048, D, BF), (8, 80, 2048, BF), (D, D, BF), (2, 8, 256, 256, F32),
         (8, 80, 256, F32), (512, D, BF), (512, D, BF), (512, FF, BF), (1024, D, BF), (256, D, BF), (D, 3 * D, BF), (D, D, BF),
         (D, 2 * FF, BF), (FF, D, BF), 4, (4,), (), (2, 2), ()]


def layer_kernel(gain_ref, wqkv_hbm, wout_hbm, gain2_ref, win_hbm, wdown_hbm, out_ref, scratch, x_ref):
    (nrm, qs, ke, ko, vt, wvt, sc, ot, att, hid, act, obuf, relay, wqkv_ref, wout_ref, win_ref, wdown_ref, sems,
     send_sem, far_recv, recv_sem, pass_send) = scratch
    r, z, _, _, k = place()
    base = r - k
    up, down = (z + 1) % 4, (z + 3) % 4
    holder, slot = z // 2, z % 2
    gets = [pltpu.make_async_copy(src, dst, sems.at[i]) for i, (src, dst) in enumerate(
        [(wqkv_hbm, wqkv_ref), (wout_hbm, wout_ref), (win_hbm, win_ref), (wdown_hbm, wdown_ref)])]
    ahead, behind = jnp.where(k == 0, up, down), jnp.where(k == 0, down, up)

    def quarter_of(step):
        return jnp.where(step == 0, (z + 2) % 4, jnp.where(step == 1, ahead, jnp.where(step == 2, behind, z)))

    def half_of(quarter):
        return (quarter + k) % 2

    def rows_of(half):
        return pl.ds(pl.multiple_of(256 * half, 256), 256)

    def block(step):
        return obuf.at[pl.ds(256 * step, 256)]

    def landing(step):
        return out_ref.at[slot, rows_of(half_of(quarter_of(step)))]

    def far():
        return remote(block(0), relay, send_sem.at[0], far_recv, (r, ahead))

    def near(step):
        q = quarter_of(step)
        return remote(block(step), landing(step), send_sem.at[step], recv_sem.at[slot, half_of(q)], (base + holder, q))

    def own():
        return remote(block(3), landing(3), send_sem.at[3], recv_sem.at[slot, half_of(z)], (base + 1 - k, z))

    def passing():
        half = half_of(ahead)
        return remote(relay, out_ref.at[behind % 2, rows_of(half)], pass_send, recv_sem.at[behind % 2, half],
                      (base + behind // 2, ahead))

    def start():
        for get in gets:
            get.start()

    def prepare():
        for get in gets:
            get.wait()
        for c in range(4):
            rows = slice(128 * c, 128 * c + 128)
            wvt[rows, :] = wqkv_ref[:, 2 * D + 128 * c : 2 * D + 128 * c + 128].astype(F32).T.astype(BF)

    def project(i, length):
        rows = pl.ds(pl.multiple_of(i * 512, 512), 512)
        parts = [x_ref[c, rows, :].astype(F32) for c in range(4)]
        square = parts[0] * parts[0]
        for part in parts[1:]:
            square = square + part * part
        scale = lax.rsqrt(jnp.sum(square, axis=1, keepdims=True) * (1.0 / D) + 1e-6)
        here = jnp.concatenate(
            [(parts[c] * scale * gain_ref[:, 128 * c : 128 * c + 128]).astype(BF) for c in range(4)], axis=1)
        nrm[rows, :] = here
        keys = dot(here, wqkv_ref[:, D : 2 * D])
        vals = dot_t(wvt[...], here)
        lane = lax.broadcasted_iota(jnp.int32, (512, 128), 1)
        pos = lax.broadcasted_iota(jnp.int32, (512, 128), 0) + i * 512
        bias = jnp.where(pos < length, 0.0, NEG)
        tail = jnp.where(lax.broadcasted_iota(jnp.int32, (16, 512), 0) == 0, 1.0, 0.0).astype(BF)
        for c in range(4):
            cols = slice(128 * c, 128 * c + 128)
            ke[rows, cols] = jnp.where(lane == 64, bias, keys[:, cols]).astype(BF)
            ko[rows, cols] = jnp.where(lane == 0, bias, keys[:, cols]).astype(BF)
        for h in range(8):
            vt[h, 0:64, rows] = vals[64 * h : 64 * h + 64, :].astype(BF)
            vt[h, 64:80, rows] = tail


    def attend(n, step):
        lane = lax.broadcasted_iota(jnp.int32, (256, 128), 1)
        tri = (lax.broadcasted_iota(jnp.int32, (256, 256), 0)
               <= lax.broadcasted_iota(jnp.int32, (256, 256), 1))
        here = pl.ds(pl.multiple_of(256 * step, 256), 256)

        def columns(hp):
            return pl.ds(pl.multiple_of(hp * 128, 128), 128)

        def query(hp, odd):
            q = qs[here, columns(hp)].astype(F32)
            if odd:
                return jnp.where(lane >= 64, q, jnp.where(lane == 0, 1.0, 0.0)).astype(BF)
            return jnp.where(lane < 64, q, jnp.where(lane == 64, 1.0, 0.0)).astype(BF)

        def score(hp, odd, qa, c, top):
            s = dot_t((ko if odd else ke)[256 * c : 256 * c + 256, columns(hp)], qa)
            if c == n - 1:
                s = jnp.where(tri, s, NEG)
            sc[odd, c] = s
            m = jnp.max(s.reshape(4, 8, 8, 256), axis=1)
            return m if top is None else jnp.maximum(top, m)

        def finish(top):
            return jnp.max(jnp.max(top, axis=0), axis=0, keepdims=True)

        def pair(hp, tops, more):
            new = []
            for odd in range(2):
                qa, top, acc = query(hp + 1, odd) if more else None, None, None
                for c in range(n):
                    p = jnp.exp2(sc[odd, c] - tops[odd]).astype(BF)
                    o = dot(vt[2 * hp + odd, :, 256 * c : 256 * c + 256], p)
                    acc = o if acc is None else acc + o
                    if more:
                        top = score(hp + 1, odd, qa, c, top)
                ot[2 * hp + odd] = acc
                if more:
                    new.append(finish(top))
            return tuple(new)

        tops = []
        for odd in range(2):
            qa, top = query(0, odd), None
            for c in range(n):
                top = score(0, odd, qa, c, top)
            tops.append(finish(top))
        tops = lax.fori_loop(0, 3, lambda hp, tops: pair(hp, tops, True), tuple(tops))
        pair(3, tops, False)

    def normalise(at):
        for hp in range(4):
            outs = [ot[2 * hp + odd, 0:64, :] / ot[2 * hp + odd, 64:65, :] for odd in range(2)]
            att[at, 128 * hp : 128 * hp + 128] = jnp.concatenate(outs, axis=0).T.astype(BF)

    def mlp(steps):
        rows = slice(0, 256 * len(steps))
        resid = []
        for step in steps:
            quarter = quarter_of(step)
            src = pl.ds(pl.multiple_of(quarter * 512 + half_of(quarter) * 256, 256), 256)
            resid.append(jnp.concatenate([x_ref[c, src, :].astype(F32) for c in range(4)], axis=1))
        hidden = (jnp.concatenate(resid, axis=0) + dot(att[rows, :], wout_ref[...])).astype(BF)
        hid[rows, :] = hidden
        hidden = hidden.astype(F32)
        scale = lax.rsqrt(jnp.mean(hidden * hidden, axis=1, keepdims=True) + 1e-6)
        att[rows, :] = (hidden * scale * gain2_ref[...]).astype(BF)
        for f in range(0, FF, 256):
            gate = dot(att[rows, :], win_ref[:, f : f + 256])
            high = dot(att[rows, :], win_ref[:, FF + f : FF + f + 256])
            act[rows, f : f + 256] = (gate / (1.0 + jnp.exp(-gate)) * high).astype(BF)
        return (hid[rows, :].astype(F32) + dot(act[rows, :], wdown_ref[...])).astype(BF)

    def run(step, _):
        quarter = quarter_of(step)
        half = half_of(quarter)

        @pl.when(step == 3)
        def _():
            far().wait_recv()
            passing().start()

        for n in range(1, 9):
            @pl.when(2 * quarter + half + 1 == n)
            def _():
                attend(n, step)

        normalise(rows_of(jnp.where(step == 1, 1, 0)))

        @pl.when(step == 1)
        def _():
            obuf[0:512, :] = mlp((0, 1))
            far().start()
            near(1).start()

        @pl.when(step >= 2)
        def _():
            out = mlp((step,))
            obuf[pl.ds(pl.multiple_of(256 * step, 256), 256), :] = out

            @pl.when(step == 2)
            def _():
                near(2).start()

            @pl.when((step == 3) & (holder == k))
            def _():
                out_ref[slot, rows_of(half), :] = out

            @pl.when((step == 3) & (holder != k))
            def _():
                own().start()

        return 0

    def late():
        mine = []
        for step in range(4):
            quarter = quarter_of(step)
            src = pl.ds(pl.multiple_of(quarter * 512 + half_of(quarter) * 256, 256), 256)
            mine.append(nrm[src, :])
        qs[...] = (dot(jnp.concatenate(mine, axis=0), wqkv_ref[:, :D]) * (0.125 * LOG2E)).astype(BF)
        lax.fori_loop(0, 4, run, 0)

        for h in range(2):
            for b in range(2):
                @pl.when((2 * k + h != z) | ((z + k) % 2 != b))
                def _():
                    remote(block(0), out_ref.at[h, pl.ds(256 * b, 256)], send_sem.at[0], recv_sem.at[h, b],
                           (base + 1 - k, z)).wait_recv()
        far().wait_send()
        near(1).wait_send()
        near(2).wait_send()

        @pl.when(holder != k)
        def _():
            own().wait_send()

        passing().wait_send()

    return start, prepare, project, late


def local(token_ids, lengths, table, attn_gain, w_qkv, w_out, mlp_gain, w_in, w_down):
    dma = pltpu.SemaphoreType.DMA
    layer = []
    for entry in LAYER:
        if isinstance(entry, tuple) and entry and not isinstance(entry[-1], int):
            layer.append(pltpu.VMEM(entry[:-1], entry[-1]))
        else:
            layer.append(dma if entry == () else dma((entry,) if isinstance(entry, int) else entry))
    return pl.pallas_call(
        whole_kernel,
        out_shape=pltpu.VMEM((2, 512, D), BF),
        in_specs=[SM, VM, ANY, VM, ANY, ANY, VM, ANY, ANY], out_specs=VM,
        scratch_shapes=[
            pltpu.VMEM((4, 2048, 128), BF),
            pltpu.VMEM((4, 2, 512), jnp.int32), pltpu.VMEM((32, 4, 128), jnp.int32), pltpu.VMEM((32, 4, 128), jnp.int32),
            pltpu.SMEM((32, 4, 128), jnp.int32), pltpu.VMEM((32, 128), jnp.int32), pltpu.SMEM((32, 128), jnp.int32),
            pltpu.VMEM((16384, 128), BF), pltpu.VMEM((16384, 128), F32), pltpu.VMEM((1024, 128), F32),
            pltpu.VMEM((31, CAP, 128), BF), pltpu.VMEM((14, CAP, 128), BF), pltpu.VMEM((32, CAP, 128), BF),
            pltpu.VMEM((2, 2048, 128), BF), pltpu.VMEM((1024, 128), BF),
            dma((3,)), dma((3,)), dma((31,)), dma((31,)), dma((3,)), dma((31,)), dma((31,)), dma((14,)), dma((14,)),
            dma((2, 4)), dma((4,)), dma((2,)), dma((3, 2)), dma((2,)), dma((3, 2)), dma((3, 2)), dma((4,)), dma((4,))] + layer,
        compiler_params=params(1, 61),
    )(lengths, token_ids, table, attn_gain.reshape(1, D), w_qkv, w_out, mlp_gain.reshape(1, D), w_in, w_down)


def solution(mesh):
    in_specs = (P("rows", "cols"), P("rows"), P("rows", "cols"), P(), P(), P(), P(), P(), P())
    return jax.shard_map(local, mesh=mesh, in_specs=in_specs, out_specs=P("rows", "cols", None), check_vma=False)
```

```python
import jax
import jax.numpy as jnp
from jax import lax
from jax.experimental import pallas as pl
from jax.experimental.pallas import tpu as pltpu
from jax.sharding import PartitionSpec as P

D = 512
FF = 2048
CAP = 344
BF = jnp.bfloat16
F32 = jnp.float32
MESH = pl.DeviceIdType.MESH
ANY = pl.BlockSpec(memory_space=pl.ANY)
VM = pl.BlockSpec(memory_space=pltpu.VMEM)
SM = pl.BlockSpec(memory_space=pltpu.SMEM)
LOG2E = 1.4426950408889634
NEG = -1e30


def dot(a, b):
    return jnp.dot(a, b, preferred_element_type=F32)


def dot_t(a, b):
    return lax.dot_general(a, b, (((1,), (1,)), ((), ())), preferred_element_type=F32)


def place():
    r, z = lax.axis_index("rows"), lax.axis_index("cols")
    return r, z, r // 8, (r // 2) % 4, r % 2


def greet(devices):
    barrier = pltpu.get_barrier_semaphore()
    for device in devices:
        pl.semaphore_signal(barrier, inc=1, device_id=device, device_id_type=MESH)
    pl.semaphore_wait(barrier, len(devices))


def remote(src, dst, send_sem, recv_sem, device):
    return pltpu.make_async_remote_copy(
        src_ref=src, dst_ref=dst, send_sem=send_sem, recv_sem=recv_sem,
        device_id=device, device_id_type=MESH)


def params(collective_id=None, vmem=60):
    kw = {}
    if collective_id is not None:
        kw = dict(collective_id=collective_id, has_side_effects=True)
    return pltpu.CompilerParams(vmem_limit_bytes=vmem * 2**20, **kw)


def routes():
    out = []
    for dy in range(4):
        for dx in range(4):
            for dk in range(2):
                if dx == dy == dk == 0:
                    continue
                side = 1 if dk == 0 else 3
                hop = None
                if dx == 2 or dy == 2:
                    hop = (side if dy == 2 else 0, side if dx == 2 else 0)
                out.append((dy, dx, dk, hop))
    def key(f):
        near = f[3] is None and (f[0] == 0 or f[1] == 0)
        return (0 if near else 1 if f[3] else 2, f[2] == 0 if f[0] or f[1] else False, (f[0] * 5 + f[1] * 3 + f[2] * 7) % 11)

    return sorted(out, key=key)


def requests(ids, lens, msg_ref, slot_ref):
    before = (lax.broadcasted_iota(jnp.int32, (128, 128), 0)
              < lax.broadcasted_iota(jnp.int32, (128, 128), 1)).astype(F32)
    above = (lax.broadcasted_iota(jnp.int32, (32, 32), 1)
             < lax.broadcasted_iota(jnp.int32, (32, 32), 0)).astype(F32).astype(BF)
    both = jnp.concatenate([before, jnp.ones((128, 128), F32)], axis=0).astype(BF)
    owners = lax.broadcasted_iota(jnp.int32, (32, 128), 0)
    ks = lax.broadcasted_iota(jnp.int32, (384, 128), 0)
    lane = lax.broadcasted_iota(jnp.int32, (32, 128), 1)
    owner = ids >> 14
    low, high = (ids & 127).astype(F32), ((ids >> 7) & 127).astype(F32)
    ones = [jnp.where(owner == o, 1.0, 0.0).astype(BF) for o in range(32)]
    rows_above = dot(above, jnp.concatenate(ones, axis=1)).astype(BF)
    prior = dot(
        jnp.concatenate(
            [jnp.concatenate(ones, axis=0),
             jnp.concatenate([rows_above[:, 128 * o : 128 * o + 128] for o in range(32)], axis=0)], axis=1),
        both)
    rank = jnp.zeros((32, 128), F32)
    for o in range(32):
        rank = rank + jnp.where(owner == o, prior[32 * o : 32 * o + 32], 0.0)
    rank_i = rank.astype(jnp.int32)
    slot_ref[...] = jnp.clip(owner * CAP + rank_i, 0, 32 * CAP - 1)
    acc = jnp.zeros((64, 384), F32)
    for a in range(0, 32, 2):
        lefts, rights = [], []
        for b in (a, a + 1):
            hit = owners == owner[b : b + 1, :]
            lefts.append(jnp.concatenate(
                [jnp.where(hit, low[b : b + 1, :], 0.0), jnp.where(hit, high[b : b + 1, :], 0.0)], axis=0).astype(BF))
            rights.append(jnp.where(ks == rank_i[b : b + 1, :], 1.0, 0.0).astype(BF))
        acc = acc + dot_t(jnp.concatenate(lefts, axis=1), jnp.concatenate(rights, axis=1))
    req = (acc[32:] * 128.0 + acc[:32]).astype(jnp.int32)
    msg_ref[...] = jnp.zeros_like(msg_ref)
    msg_ref[:, 0, :] = jnp.where(lane == 126, lens[0], jnp.where(lane == 127, lens[1], 0))
    for j in range(4):
        msg_ref[:, j, 0 : CAP // 4] = req[:, CAP // 4 * j : CAP // 4 * (j + 1)]


def whole_kernel(len_ref, tok_ref, table_hbm, gain_ref, wqkv_hbm, wout_hbm, gain2_ref, win_hbm, wdown_hbm, out_ref, *rest):
    front, layer = rest[: -len(LAYER)], rest[-len(LAYER) :]
    start, prepare, project, late = layer_kernel(
        gain_ref, wqkv_hbm, wout_hbm, gain2_ref, win_hbm, wdown_hbm, out_ref, layer, front[0])
    front_kernel(len_ref, tok_ref, table_hbm, *front, start, prepare, project)
    late()


def front_kernel(len_ref, tok_ref, table_hbm, out_ref,
                 ids_ref, msg_ref, asked_v, asked_s, slot_v, slot_s, table_ref, wide, stage, block, relay, back, emb,
                 relay_z, ids_send, ids_recv, ask_send, ask_recv, copy_sem, list_sem, send_sem, recv_sem, hop_send, hop_recv,
                 z_send, z_relay_send, z_relay_recv, z_recv, relay_pass, pass_send, pass_recv, own_send, own_recv, start, prepare, project):
    r, z, y, x, k = place()
    base = r - k
    other = (base + 1 - k, z)
    up, down = (z + 1) % 4, (z + 3) % 4
    holder = z // 2
    column = [(r, (z + s) % 4) for s in (1, 2, 3)]
    plane = [((r + s) % 32, z) for s in range(1, 32)]
    load = pltpu.make_async_copy(table_hbm, table_ref, copy_sem.at[0])
    load.start()
    start()
    greet(column + plane + [(base + 1 - k, up), (base + 1 - k, down)])

    copies = []
    for s, device in enumerate(column):
        copy = remote(tok_ref, ids_ref.at[z], ids_send.at[s], ids_recv.at[s], device)
        copy.start()
        copies.append(copy)
    ids_ref[z] = tok_ref[...]
    for copy in copies:
        copy.wait()
    ids = jnp.concatenate(
        [ids_ref[c, h : h + 1, 128 * j : 128 * j + 128] for c in range(4) for h in range(2) for j in range(4)], axis=0)
    requests(ids, (len_ref[0], len_ref[1]), msg_ref, slot_v)

    copies = []
    for s, device in enumerate(plane):
        copy = remote(msg_ref.at[device[0]], asked_v.at[r], ask_send.at[s], ask_recv.at[s], device)
        copy.start()
        copies.append(copy)
    asked_v[r] = msg_ref[r]
    to_slots = pltpu.make_async_copy(slot_v, slot_s, copy_sem.at[1])
    to_slots.start()
    load.wait()

    def widen(i, _):
        rows = pl.ds(pl.multiple_of(i * 256, 256), 256)
        wide[rows, :] = table_ref[rows, :].astype(F32)
        return 0

    lax.fori_loop(0, 64, widen, 0)
    to_slots.wait()

    def row(dy, dx, dk):
        return (((y + dy) % 4) * 4 + (x + dx) % 4) * 2 + (k + dk) % 2

    def fill(p, dst):
        def some(j, _):
            for i in range(CAP // 4):
                stage[pl.ds(j * (CAP // 4) + i, 1), :] = wide[pl.ds(asked_s[p, j, i], 1), :]
            return 0

        lax.fori_loop(0, 4, some, 0)
        dst[...] = stage[0:CAP, :].astype(BF)

    def take(p, n, arrived=True):
        if arrived:
            remote(msg_ref.at[0], asked_v.at[p], ask_send.at[0], ask_recv.at[(r - p) % 32 - 1], other).wait_recv()
        asked_v[p] = jnp.clip(asked_v[p], 0, 16383)
        copy = pltpu.make_async_copy(asked_v.at[p], asked_s.at[p], list_sem.at[n])
        copy.start()
        return copy

    flows = routes()
    hops = [f for f in flows if f[3] is not None]
    direct = [f for f in flows if f[3] is None]
    first, final, waiting = [], [], None
    lists = [take(row(*flows[0][:3]), 0)]
    for n, flow in enumerate(flows):
        dy, dx, dk, hop = flow
        p = row(dy, dx, dk)
        lists.append(take(row(*flows[n + 1][:3]), n + 1) if n + 1 < len(flows) else take(r, 31, False))
        lists[n].wait()
        fill(p, block.at[n])
        if hop is not None:
            i = hops.index(flow)
            copy = remote(block.at[n], relay.at[i], hop_send.at[i], hop_recv.at[i], (row(*hop, 0), z))
            first.append(copy)
        else:
            i = direct.index(flow)
            copy = remote(block.at[n], back.at[r], send_sem.at[i], recv_sem.at[i], (p, z))
            final.append((copy, row(-dy, -dx, dk)))
        if waiting is not None:
            waiting.start()
        waiting = copy
    lists[31].wait()
    length = asked_s[base + holder, 0, 126 + z % 2]
    for copy in copies:
        copy.wait_send()
    fill(r, back.at[r])
    waiting.start()
    for i, (dy, dx, dk, (hy, hx)) in enumerate(hops):
        first[i].wait_recv()
        n = len(direct) + i
        copy = remote(relay.at[i], back.at[row(-hy, -hx, 0)], send_sem.at[n], recv_sem.at[n],
                      (row(dy - hy, dx - hx, dk), z))
        copy.start()
        final.append((copy, row(-dy, -dx, dk)))

    prepare()

    def spread(source):
        wide[pl.ds(pl.multiple_of(source * CAP, 8), CAP), :] = back[source].astype(F32)

    spread(r)
    for copy, source in final:
        copy.wait_recv()
        spread(source)

    def rows(c):
        return pl.ds(pl.multiple_of(512 * c, 512), 512)

    def far(h, c):
        return remote(emb.at[h, rows(c)], relay_z.at[rows(c % 2)], z_relay_send.at[c], z_relay_recv.at[c % 2],
                      (base + c // 2, (up, down)[c // 2]))

    def near(h, c, step):
        return remote(emb.at[h, rows(c)], out_ref.at[z, rows(c)],
                      z_send.at[step // 2, c], z_recv.at[step // 2, c % 2], (base + c // 2, (z + step) % 4))

    def own(h, c):
        return remote(emb.at[h, rows(c)], out_ref.at[z, rows(c)], own_send.at[c], own_recv.at[c], other)

    def send(h, c, act):
        dist = (2 * k + h - z) % 4

        @pl.when(dist == 2)
        def _():
            act(far(h, c))

        for step in (1, 3):
            @pl.when(dist == step)
            def _():
                act(near(h, c, step))

        @pl.when(dist == 0)
        def _():
            act(own(h, c))

    lead = jnp.where((2 * k - z) % 4 < 2, 1, 0)
    pieces = [(h, c) for h in (lead, 1 - lead) for c in (0, 2, 1, 3)]
    waiting = None
    for h, c in pieces:
        def gather(j, _):
            a = c * 8 + h * 4 + j
            for i in range(128):
                stage[pl.ds(j * 128 + i, 1), :] = wide[pl.ds(slot_s[a, i], 1), :]
            return 0

        lax.fori_loop(0, 4, gather, 0)
        emb[h, rows(c), :] = stage[0:512, :].astype(BF)

        @pl.when((2 * k + h - z) % 4 == 0)
        def _():
            out_ref[z, rows(c), :] = stage[0:512, :].astype(BF)

        if waiting is not None:
            send(*waiting, lambda copy: copy.start())
        waiting = (h, c)
    send(*waiting, lambda copy: copy.start())

    behind = jnp.where(k == 0, down, up)
    ahead = jnp.where(k == 0, up, down)
    sources = (down, up, (z + 2) % 4)
    relayed = []
    for j in range(2):
        copy = remote(relay_z.at[rows(j)], out_ref.at[behind, rows(2 * k + j)], relay_pass.at[j], z_recv.at[2, j], (r, ahead))
        far(0, j).wait_recv()
        copy.start()
        relayed.append(copy)
    passed = []
    for j in range(2):
        for i, source in enumerate(sources):
            got = out_ref.at[source, rows(2 * k + j)]
            remote(got, got, pass_send.at[i, j], z_recv.at[i, j], other).wait_recv()
            copy = remote(got, got, pass_send.at[i, j], pass_recv.at[i, j], other)
            copy.start()
            passed.append(copy)

        if j == 0:
            @pl.when(k != holder)
            def _():
                for c in range(4):
                    own(0, c).wait_recv()

        project(2 * k + j, length)
    for j in range(2):
        for i, source in enumerate(sources):
            got = out_ref.at[source, rows(2 * (1 - k) + j)]
            remote(got, got, pass_send.at[i, j], pass_recv.at[i, j], other).wait_recv()
        project(2 * (1 - k) + j, length)
    for copy in first:
        copy.wait_send()
    for copy, _ in final:
        copy.wait_send()
    for copy in passed + relayed:
        copy.wait_send()
    for h, c in pieces:
        send(h, c, lambda copy: copy.wait_send())


LAYER = [(2048, D, BF), (1024, D, BF), (2048, D, BF), (2048, D, BF), (8, 80, 2048, BF), (D, D, BF), (2, 8, 256, 256, F32),
         (8, 80, 256, F32), (512, D, BF), (512, D, BF), (512, FF, BF), (1024, D, BF), (256, D, BF), (D, 3 * D, BF), (D, D, BF),
         (D, 2 * FF, BF), (FF, D, BF), 4, (4,), (), (2, 2), ()]


def layer_kernel(gain_ref, wqkv_hbm, wout_hbm, gain2_ref, win_hbm, wdown_hbm, out_ref, scratch, x_ref):
    (nrm, qs, ke, ko, vt, wvt, sc, ot, att, hid, act, obuf, relay, wqkv_ref, wout_ref, win_ref, wdown_ref, sems,
     send_sem, far_recv, recv_sem, pass_send) = scratch
    r, z, _, _, k = place()
    base = r - k
    up, down = (z + 1) % 4, (z + 3) % 4
    holder, slot = z // 2, z % 2
    gets = [pltpu.make_async_copy(src, dst, sems.at[i]) for i, (src, dst) in enumerate(
        [(wqkv_hbm, wqkv_ref), (wout_hbm, wout_ref), (win_hbm, win_ref), (wdown_hbm, wdown_ref)])]
    ahead, behind = jnp.where(k == 0, up, down), jnp.where(k == 0, down, up)

    def quarter_of(step):
        return jnp.where(step == 0, (z + 2) % 4, jnp.where(step == 1, ahead, jnp.where(step == 2, behind, z)))

    def half_of(quarter):
        return (quarter + k) % 2

    def rows_of(half):
        return pl.ds(pl.multiple_of(256 * half, 256), 256)

    def block(step):
        return obuf.at[pl.ds(256 * step, 256)]

    def landing(step):
        return out_ref.at[slot, rows_of(half_of(quarter_of(step)))]

    def far():
        return remote(block(0), relay, send_sem.at[0], far_recv, (r, ahead))

    def near(step):
        q = quarter_of(step)
        return remote(block(step), landing(step), send_sem.at[step], recv_sem.at[slot, half_of(q)], (base + holder, q))

    def own():
        return remote(block(3), landing(3), send_sem.at[3], recv_sem.at[slot, half_of(z)], (base + 1 - k, z))

    def passing():
        half = half_of(ahead)
        return remote(relay, out_ref.at[behind % 2, rows_of(half)], pass_send, recv_sem.at[behind % 2, half],
                      (base + behind // 2, ahead))

    def start():
        for get in gets:
            get.start()

    def prepare():
        for get in gets:
            get.wait()
        for c in range(4):
            rows = slice(128 * c, 128 * c + 128)
            wvt[rows, :] = wqkv_ref[:, 2 * D + 128 * c : 2 * D + 128 * c + 128].astype(F32).T.astype(BF)

    def project(i, length):
        rows = pl.ds(pl.multiple_of(i * 512, 512), 512)
        parts = [x_ref[c, rows, :].astype(F32) for c in range(4)]
        square = parts[0] * parts[0]
        for part in parts[1:]:
            square = square + part * part
        scale = lax.rsqrt(jnp.sum(square, axis=1, keepdims=True) * (1.0 / D) + 1e-6)
        here = jnp.concatenate(
            [(parts[c] * scale * gain_ref[:, 128 * c : 128 * c + 128]).astype(BF) for c in range(4)], axis=1)
        nrm[rows, :] = here
        keys = dot(here, wqkv_ref[:, D : 2 * D])
        vals = dot_t(wvt[...], here)
        lane = lax.broadcasted_iota(jnp.int32, (512, 128), 1)
        pos = lax.broadcasted_iota(jnp.int32, (512, 128), 0) + i * 512
        bias = jnp.where(pos < length, 0.0, NEG)
        tail = jnp.where(lax.broadcasted_iota(jnp.int32, (16, 512), 0) == 0, 1.0, 0.0).astype(BF)
        for c in range(4):
            cols = slice(128 * c, 128 * c + 128)
            ke[rows, cols] = jnp.where(lane == 64, bias, keys[:, cols]).astype(BF)
            ko[rows, cols] = jnp.where(lane == 0, bias, keys[:, cols]).astype(BF)
        for h in range(8):
            vt[h, 0:64, rows] = vals[64 * h : 64 * h + 64, :].astype(BF)
            vt[h, 64:80, rows] = tail


    def attend(n, step):
        lane = lax.broadcasted_iota(jnp.int32, (256, 128), 1)
        tri = (lax.broadcasted_iota(jnp.int32, (256, 256), 0)
               <= lax.broadcasted_iota(jnp.int32, (256, 256), 1))
        here = pl.ds(pl.multiple_of(256 * step, 256), 256)

        def columns(hp):
            return pl.ds(pl.multiple_of(hp * 128, 128), 128)

        def query(hp, odd):
            q = qs[here, columns(hp)].astype(F32)
            if odd:
                return jnp.where(lane >= 64, q, jnp.where(lane == 0, 1.0, 0.0)).astype(BF)
            return jnp.where(lane < 64, q, jnp.where(lane == 64, 1.0, 0.0)).astype(BF)

        def score(hp, odd, qa, c, top):
            s = dot_t((ko if odd else ke)[256 * c : 256 * c + 256, columns(hp)], qa)
            if c == n - 1:
                s = jnp.where(tri, s, NEG)
            sc[odd, c] = s
            m = jnp.max(s.reshape(4, 8, 8, 256), axis=1)
            return m if top is None else jnp.maximum(top, m)

        def finish(top):
            return jnp.max(jnp.max(top, axis=0), axis=0, keepdims=True)

        def pair(hp, tops, more):
            new = []
            for odd in range(2):
                qa, top, acc = query(hp + 1, odd) if more else None, None, None
                for c in range(n):
                    p = jnp.exp2(sc[odd, c] - tops[odd]).astype(BF)
                    o = dot(vt[2 * hp + odd, :, 256 * c : 256 * c + 256], p)
                    acc = o if acc is None else acc + o
                    if more:
                        top = score(hp + 1, odd, qa, c, top)
                ot[2 * hp + odd] = acc
                if more:
                    new.append(finish(top))
            return tuple(new)

        tops = []
        for odd in range(2):
            qa, top = query(0, odd), None
            for c in range(n):
                top = score(0, odd, qa, c, top)
            tops.append(finish(top))
        tops = lax.fori_loop(0, 3, lambda hp, tops: pair(hp, tops, True), tuple(tops))
        pair(3, tops, False)

    def normalise(at):
        for hp in range(4):
            outs = [ot[2 * hp + odd, 0:64, :] / ot[2 * hp + odd, 64:65, :] for odd in range(2)]
            att[at, 128 * hp : 128 * hp + 128] = jnp.concatenate(outs, axis=0).T.astype(BF)

    def mlp(steps):
        rows = slice(0, 256 * len(steps))
        resid = []
        for step in steps:
            quarter = quarter_of(step)
            src = pl.ds(pl.multiple_of(quarter * 512 + half_of(quarter) * 256, 256), 256)
            resid.append(jnp.concatenate([x_ref[c, src, :].astype(F32) for c in range(4)], axis=1))
        hidden = (jnp.concatenate(resid, axis=0) + dot(att[rows, :], wout_ref[...])).astype(BF)
        hid[rows, :] = hidden
        hidden = hidden.astype(F32)
        scale = lax.rsqrt(jnp.mean(hidden * hidden, axis=1, keepdims=True) + 1e-6)
        att[rows, :] = (hidden * scale * gain2_ref[...]).astype(BF)
        for f in range(0, FF, 256):
            gate = dot(att[rows, :], win_ref[:, f : f + 256])
            high = dot(att[rows, :], win_ref[:, FF + f : FF + f + 256])
            act[rows, f : f + 256] = (gate / (1.0 + jnp.exp(-gate)) * high).astype(BF)
        return (hid[rows, :].astype(F32) + dot(act[rows, :], wdown_ref[...])).astype(BF)

    def run(step, _):
        quarter = quarter_of(step)
        half = half_of(quarter)

        @pl.when(step == 3)
        def _():
            far().wait_recv()
            passing().start()

        for n in range(1, 9):
            @pl.when(2 * quarter + half + 1 == n)
            def _():
                attend(n, step)

        normalise(rows_of(jnp.where(step == 1, 1, 0)))

        @pl.when(step == 1)
        def _():
            obuf[0:512, :] = mlp((0, 1))
            far().start()
            near(1).start()

        @pl.when(step >= 2)
        def _():
            out = mlp((step,))
            obuf[pl.ds(pl.multiple_of(256 * step, 256), 256), :] = out

            @pl.when(step == 2)
            def _():
                near(2).start()

            @pl.when((step == 3) & (holder == k))
            def _():
                out_ref[slot, rows_of(half), :] = out

            @pl.when((step == 3) & (holder != k))
            def _():
                own().start()

        return 0

    def late():
        mine = []
        for step in range(4):
            quarter = quarter_of(step)
            src = pl.ds(pl.multiple_of(quarter * 512 + half_of(quarter) * 256, 256), 256)
            mine.append(nrm[src, :])
        qs[...] = (dot(jnp.concatenate(mine, axis=0), wqkv_ref[:, :D]) * (0.125 * LOG2E)).astype(BF)
        lax.fori_loop(0, 4, run, 0)

        for h in range(2):
            for b in range(2):
                @pl.when((2 * k + h != z) | ((z + k) % 2 != b))
                def _():
                    remote(block(0), out_ref.at[h, pl.ds(256 * b, 256)], send_sem.at[0], recv_sem.at[h, b],
                           (base + 1 - k, z)).wait_recv()
        far().wait_send()
        near(1).wait_send()
        near(2).wait_send()

        @pl.when(holder != k)
        def _():
            own().wait_send()

        passing().wait_send()

    return start, prepare, project, late


def local(token_ids, lengths, table, attn_gain, w_qkv, w_out, mlp_gain, w_in, w_down):
    dma = pltpu.SemaphoreType.DMA
    layer = []
    for entry in LAYER:
        if isinstance(entry, tuple) and entry and not isinstance(entry[-1], int):
            layer.append(pltpu.VMEM(entry[:-1], entry[-1]))
        else:
            layer.append(dma if entry == () else dma((entry,) if isinstance(entry, int) else entry))
    return pl.pallas_call(
        whole_kernel,
        out_shape=pltpu.VMEM((2, 512, D), BF),
        in_specs=[SM, VM, ANY, VM, ANY, ANY, VM, ANY, ANY], out_specs=VM,
        scratch_shapes=[
            pltpu.VMEM((4, 2048, 128), BF),
            pltpu.VMEM((4, 2, 512), jnp.int32), pltpu.VMEM((32, 4, 128), jnp.int32), pltpu.VMEM((32, 4, 128), jnp.int32),
            pltpu.SMEM((32, 4, 128), jnp.int32), pltpu.VMEM((32, 128), jnp.int32), pltpu.SMEM((32, 128), jnp.int32),
            pltpu.VMEM((16384, 128), BF), pltpu.VMEM((16384, 128), F32), pltpu.VMEM((1024, 128), F32),
            pltpu.VMEM((31, CAP, 128), BF), pltpu.VMEM((14, CAP, 128), BF), pltpu.VMEM((32, CAP, 128), BF),
            pltpu.VMEM((2, 2048, 128), BF), pltpu.VMEM((1024, 128), BF),
            dma((3,)), dma((3,)), dma((31,)), dma((31,)), dma((2,)), dma((32,)), dma((31,)), dma((31,)), dma((14,)), dma((14,)),
            dma((2, 4)), dma((4,)), dma((2,)), dma((3, 2)), dma((2,)), dma((3, 2)), dma((3, 2)), dma((4,)), dma((4,))] + layer,
        compiler_params=params(1, 61),
    )(lengths, token_ids, table, attn_gain.reshape(1, D), w_qkv, w_out, mlp_gain.reshape(1, D), w_in, w_down)


def solution(mesh):
    in_specs = (P("rows", "cols"), P("rows"), P("rows", "cols"), P(), P(), P(), P(), P(), P())
    return jax.shard_map(local, mesh=mesh, in_specs=in_specs, out_specs=P("rows", "cols", None), check_vma=False)
```

```python
import jax
import jax.numpy as jnp
from jax import lax
from jax.experimental import pallas as pl
from jax.experimental.pallas import tpu as pltpu
from jax.sharding import PartitionSpec as P

D = 512
FF = 2048
CAP = 344
BF = jnp.bfloat16
F32 = jnp.float32
MESH = pl.DeviceIdType.MESH
ANY = pl.BlockSpec(memory_space=pl.ANY)
VM = pl.BlockSpec(memory_space=pltpu.VMEM)
SM = pl.BlockSpec(memory_space=pltpu.SMEM)
LOG2E = 1.4426950408889634
NEG = -1e30


def dot(a, b):
    return jnp.dot(a, b, preferred_element_type=F32)


def dot_t(a, b):
    return lax.dot_general(a, b, (((1,), (1,)), ((), ())), preferred_element_type=F32)


def place():
    r, z = lax.axis_index("rows"), lax.axis_index("cols")
    return r, z, r // 8, (r // 2) % 4, r % 2


def greet(devices):
    barrier = pltpu.get_barrier_semaphore()
    for device in devices:
        pl.semaphore_signal(barrier, inc=1, device_id=device, device_id_type=MESH)
    pl.semaphore_wait(barrier, len(devices))


def remote(src, dst, send_sem, recv_sem, device):
    return pltpu.make_async_remote_copy(
        src_ref=src, dst_ref=dst, send_sem=send_sem, recv_sem=recv_sem,
        device_id=device, device_id_type=MESH)


def params(collective_id=None, vmem=60):
    kw = {}
    if collective_id is not None:
        kw = dict(collective_id=collective_id, has_side_effects=True)
    return pltpu.CompilerParams(vmem_limit_bytes=vmem * 2**20, **kw)


def routes():
    out = []
    for dy in range(4):
        for dx in range(4):
            for dk in range(2):
                if dx == dy == dk == 0:
                    continue
                side = 1 if dk == 0 else 3
                hop = None
                if dx == 2 or dy == 2:
                    hop = (side if dy == 2 else 0, side if dx == 2 else 0)
                out.append((dy, dx, dk, hop))
    def key(f):
        near = f[3] is None and (f[0] == 0 or f[1] == 0)
        return (0 if near else 1 if f[3] else 2, f[2] == 0 if f[0] or f[1] else False, (f[0] * 5 + f[1] * 3 + f[2] * 7) % 11)

    return sorted(out, key=key)


def requests(ids, lens, msg_ref, slot_ref):
    before = (lax.broadcasted_iota(jnp.int32, (128, 128), 0)
              < lax.broadcasted_iota(jnp.int32, (128, 128), 1)).astype(F32)
    above = (lax.broadcasted_iota(jnp.int32, (32, 32), 1)
             < lax.broadcasted_iota(jnp.int32, (32, 32), 0)).astype(F32).astype(BF)
    both = jnp.concatenate([before, jnp.ones((128, 128), F32)], axis=0).astype(BF)
    owners = lax.broadcasted_iota(jnp.int32, (32, 128), 0)
    ks = lax.broadcasted_iota(jnp.int32, (176, 128), 0)
    lane = lax.broadcasted_iota(jnp.int32, (32, 128), 1)
    owner = ids >> 14
    low, high = (ids & 127).astype(F32), ((ids >> 7) & 127).astype(F32)
    ones = [jnp.where(owner == o, 1.0, 0.0).astype(BF) for o in range(32)]
    rows_above = dot(above, jnp.concatenate(ones, axis=1)).astype(BF)
    prior = dot(
        jnp.concatenate(
            [jnp.concatenate(ones, axis=0),
             jnp.concatenate([rows_above[:, 128 * o : 128 * o + 128] for o in range(32)], axis=0)], axis=1),
        both)
    rank = jnp.zeros((32, 128), F32)
    for o in range(32):
        rank = rank + jnp.where(owner == o, prior[32 * o : 32 * o + 32], 0.0)
    rank_i = rank.astype(jnp.int32)
    slot_ref[...] = jnp.clip(owner * CAP + rank_i, 0, 32 * CAP - 1)
    upper = jnp.where(rank_i >= CAP // 2, 1, 0)
    within = rank_i - upper * (CAP // 2)
    acc = jnp.zeros((128, 176), F32)
    for a in range(0, 32, 2):
        lefts, rights = [], []
        for b in (a, a + 1):
            part = slice(b, b + 1)
            left = []
            for half in range(2):
                hit = owners == jnp.where(upper[part] == half, owner[part], -1)
                left += [jnp.where(hit, low[part], 0.0), jnp.where(hit, high[part], 0.0)]
            lefts.append(jnp.concatenate(left, axis=0).astype(BF))
            rights.append(jnp.where(ks == jnp.where(within[part] < CAP // 2, within[part], -1), 1.0, 0.0).astype(BF))
        acc = acc + dot_t(jnp.concatenate(lefts, axis=1), jnp.concatenate(rights, axis=1))
    req = [(acc[64 * half + 32 : 64 * half + 64] * 128.0 + acc[64 * half : 64 * half + 32]).astype(jnp.int32)
           for half in range(2)]
    msg_ref[...] = jnp.zeros_like(msg_ref)
    msg_ref[:, 0, :] = jnp.where(lane == 126, lens[0], jnp.where(lane == 127, lens[1], 0))
    for j in range(4):
        at = CAP // 4 * (j % 2)
        msg_ref[:, j, 0 : CAP // 4] = req[j // 2][:, at : at + CAP // 4]


def whole_kernel(len_ref, tok_ref, table_hbm, gain_ref, wqkv_hbm, wout_hbm, gain2_ref, win_hbm, wdown_hbm, out_ref, *rest):
    front, layer = rest[: -len(LAYER)], rest[-len(LAYER) :]
    start, prepare, project, late = layer_kernel(
        gain_ref, wqkv_hbm, wout_hbm, gain2_ref, win_hbm, wdown_hbm, out_ref, layer, front[0])
    front_kernel(len_ref, tok_ref, table_hbm, *front, start, prepare, project)
    late()


def front_kernel(len_ref, tok_ref, table_hbm, out_ref,
                 ids_ref, msg_ref, asked_v, asked_s, slot_v, slot_s, table_ref, wide, stage, block, relay, back, emb,
                 relay_z, ids_send, ids_recv, ask_send, ask_recv, copy_sem, list_sem, send_sem, recv_sem, hop_send, hop_recv,
                 z_send, z_relay_send, z_relay_recv, z_recv, relay_pass, pass_send, pass_recv, own_send, own_recv, start, prepare, project):
    r, z, y, x, k = place()
    base = r - k
    other = (base + 1 - k, z)
    up, down = (z + 1) % 4, (z + 3) % 4
    holder = z // 2
    column = [(r, (z + s) % 4) for s in (1, 2, 3)]
    plane = [((r + s) % 32, z) for s in range(1, 32)]
    load = pltpu.make_async_copy(table_hbm, table_ref, copy_sem.at[0])
    load.start()
    start()
    greet(column + plane + [(base + 1 - k, up), (base + 1 - k, down)])

    copies = []
    for s, device in enumerate(column):
        copy = remote(tok_ref, ids_ref.at[z], ids_send.at[s], ids_recv.at[s], device)
        copy.start()
        copies.append(copy)
    ids_ref[z] = tok_ref[...]
    for copy in copies:
        copy.wait()
    ids = jnp.concatenate(
        [ids_ref[c, h : h + 1, 128 * j : 128 * j + 128] for c in range(4) for h in range(2) for j in range(4)], axis=0)
    requests(ids, (len_ref[0], len_ref[1]), msg_ref, slot_v)

    copies = []
    for s, device in enumerate(plane):
        copy = remote(msg_ref.at[device[0]], asked_v.at[r], ask_send.at[s], ask_recv.at[s], device)
        copy.start()
        copies.append(copy)
    asked_v[r] = msg_ref[r]
    to_slots = pltpu.make_async_copy(slot_v, slot_s, copy_sem.at[1])
    to_slots.start()
    load.wait()

    def widen(i, _):
        rows = pl.ds(pl.multiple_of(i * 256, 256), 256)
        wide[rows, :] = table_ref[rows, :].astype(F32)
        return 0

    lax.fori_loop(0, 64, widen, 0)
    to_slots.wait()

    def row(dy, dx, dk):
        return (((y + dy) % 4) * 4 + (x + dx) % 4) * 2 + (k + dk) % 2

    def fill(p, dst):
        def some(j, _):
            for i in range(CAP // 4):
                stage[pl.ds(j * (CAP // 4) + i, 1), :] = wide[pl.ds(asked_s[p, j, i], 1), :]
            return 0

        lax.fori_loop(0, 4, some, 0)
        dst[...] = stage[0:CAP, :].astype(BF)

    def take(p, n, arrived=True):
        if arrived:
            remote(msg_ref.at[0], asked_v.at[p], ask_send.at[0], ask_recv.at[(r - p) % 32 - 1], other).wait_recv()
        asked_v[p] = jnp.clip(asked_v[p], 0, 16383)
        copy = pltpu.make_async_copy(asked_v.at[p], asked_s.at[p], list_sem.at[n])
        copy.start()
        return copy

    flows = routes()
    hops = [f for f in flows if f[3] is not None]
    direct = [f for f in flows if f[3] is None]
    first, final, waiting = [], [], None
    lists = [take(row(*flows[0][:3]), 0)]
    for n, flow in enumerate(flows):
        dy, dx, dk, hop = flow
        p = row(dy, dx, dk)
        lists.append(take(row(*flows[n + 1][:3]), n + 1) if n + 1 < len(flows) else take(r, 31, False))
        lists[n].wait()
        fill(p, block.at[n])
        if hop is not None:
            i = hops.index(flow)
            copy = remote(block.at[n], relay.at[i], hop_send.at[i], hop_recv.at[i], (row(*hop, 0), z))
            first.append(copy)
        else:
            i = direct.index(flow)
            copy = remote(block.at[n], back.at[r], send_sem.at[i], recv_sem.at[i], (p, z))
            final.append((copy, row(-dy, -dx, dk)))
        if waiting is not None:
            waiting.start()
        waiting = copy
    lists[31].wait()
    length = asked_s[base + holder, 0, 126 + z % 2]
    for copy in copies:
        copy.wait_send()
    fill(r, back.at[r])
    waiting.start()
    for i, (dy, dx, dk, (hy, hx)) in enumerate(hops):
        first[i].wait_recv()
        n = len(direct) + i
        copy = remote(relay.at[i], back.at[row(-hy, -hx, 0)], send_sem.at[n], recv_sem.at[n],
                      (row(dy - hy, dx - hx, dk), z))
        copy.start()
        final.append((copy, row(-dy, -dx, dk)))

    prepare()

    def spread(source):
        wide[pl.ds(pl.multiple_of(source * CAP, 8), CAP), :] = back[source].astype(F32)

    spread(r)
    for copy, source in final:
        copy.wait_recv()
        spread(source)

    def rows(c):
        return pl.ds(pl.multiple_of(512 * c, 512), 512)

    def far(h, c):
        return remote(emb.at[h, rows(c)], relay_z.at[rows(c % 2)], z_relay_send.at[c], z_relay_recv.at[c % 2],
                      (base + c // 2, (up, down)[c // 2]))

    def near(h, c, step):
        return remote(emb.at[h, rows(c)], out_ref.at[z, rows(c)],
                      z_send.at[step // 2, c], z_recv.at[step // 2, c % 2], (base + c // 2, (z + step) % 4))

    def own(h, c):
        return remote(emb.at[h, rows(c)], out_ref.at[z, rows(c)], own_send.at[c], own_recv.at[c], other)

    def send(h, c, act):
        dist = (2 * k + h - z) % 4

        @pl.when(dist == 2)
        def _():
            act(far(h, c))

        for step in (1, 3):
            @pl.when(dist == step)
            def _():
                act(near(h, c, step))

        @pl.when(dist == 0)
        def _():
            act(own(h, c))

    lead = jnp.where((2 * k - z) % 4 < 2, 1, 0)
    pieces = [(h, c) for h in (lead, 1 - lead) for c in (0, 2, 1, 3)]
    waiting = None
    for h, c in pieces:
        def gather(j, _):
            a = c * 8 + h * 4 + j
            for i in range(128):
                stage[pl.ds(j * 128 + i, 1), :] = wide[pl.ds(slot_s[a, i], 1), :]
            return 0

        lax.fori_loop(0, 4, gather, 0)
        emb[h, rows(c), :] = stage[0:512, :].astype(BF)

        @pl.when((2 * k + h - z) % 4 == 0)
        def _():
            out_ref[z, rows(c), :] = stage[0:512, :].astype(BF)

        if waiting is not None:
            send(*waiting, lambda copy: copy.start())
        waiting = (h, c)
    send(*waiting, lambda copy: copy.start())

    behind = jnp.where(k == 0, down, up)
    ahead = jnp.where(k == 0, up, down)
    sources = (down, up, (z + 2) % 4)
    relayed = []
    for j in range(2):
        copy = remote(relay_z.at[rows(j)], out_ref.at[behind, rows(2 * k + j)], relay_pass.at[j], z_recv.at[2, j], (r, ahead))
        far(0, j).wait_recv()
        copy.start()
        relayed.append(copy)
    passed = []
    for j in range(2):
        for i, source in enumerate(sources):
            got = out_ref.at[source, rows(2 * k + j)]
            remote(got, got, pass_send.at[i, j], z_recv.at[i, j], other).wait_recv()
            copy = remote(got, got, pass_send.at[i, j], pass_recv.at[i, j], other)
            copy.start()
            passed.append(copy)

        if j == 0:
            @pl.when(k != holder)
            def _():
                for c in range(4):
                    own(0, c).wait_recv()

        project(2 * k + j, length)
    for j in range(2):
        for i, source in enumerate(sources):
            got = out_ref.at[source, rows(2 * (1 - k) + j)]
            remote(got, got, pass_send.at[i, j], pass_recv.at[i, j], other).wait_recv()
        project(2 * (1 - k) + j, length)
    for copy in first:
        copy.wait_send()
    for copy, _ in final:
        copy.wait_send()
    for copy in passed + relayed:
        copy.wait_send()
    for h, c in pieces:
        send(h, c, lambda copy: copy.wait_send())


LAYER = [(2048, D, BF), (1024, D, BF), (2048, D, BF), (2048, D, BF), (8, 80, 2048, BF), (D, D, BF), (2, 8, 256, 256, F32),
         (8, 80, 256, F32), (512, D, BF), (512, D, BF), (512, FF, BF), (1024, D, BF), (256, D, BF), (D, 3 * D, BF), (D, D, BF),
         (D, 2 * FF, BF), (FF, D, BF), 4, (4,), (), (2, 2), ()]


def layer_kernel(gain_ref, wqkv_hbm, wout_hbm, gain2_ref, win_hbm, wdown_hbm, out_ref, scratch, x_ref):
    (nrm, qs, ke, ko, vt, wvt, sc, ot, att, hid, act, obuf, relay, wqkv_ref, wout_ref, win_ref, wdown_ref, sems,
     send_sem, far_recv, recv_sem, pass_send) = scratch
    r, z, _, _, k = place()
    base = r - k
    up, down = (z + 1) % 4, (z + 3) % 4
    holder, slot = z // 2, z % 2
    gets = [pltpu.make_async_copy(src, dst, sems.at[i]) for i, (src, dst) in enumerate(
        [(wqkv_hbm, wqkv_ref), (wout_hbm, wout_ref), (win_hbm, win_ref), (wdown_hbm, wdown_ref)])]
    ahead, behind = jnp.where(k == 0, up, down), jnp.where(k == 0, down, up)

    def quarter_of(step):
        return jnp.where(step == 0, (z + 2) % 4, jnp.where(step == 1, ahead, jnp.where(step == 2, behind, z)))

    def half_of(quarter):
        return (quarter + k) % 2

    def rows_of(half):
        return pl.ds(pl.multiple_of(256 * half, 256), 256)

    def block(step):
        return obuf.at[pl.ds(256 * step, 256)]

    def landing(step):
        return out_ref.at[slot, rows_of(half_of(quarter_of(step)))]

    def far():
        return remote(block(0), relay, send_sem.at[0], far_recv, (r, ahead))

    def near(step):
        q = quarter_of(step)
        return remote(block(step), landing(step), send_sem.at[step], recv_sem.at[slot, half_of(q)], (base + holder, q))

    def own():
        return remote(block(3), landing(3), send_sem.at[3], recv_sem.at[slot, half_of(z)], (base + 1 - k, z))

    def passing():
        half = half_of(ahead)
        return remote(relay, out_ref.at[behind % 2, rows_of(half)], pass_send, recv_sem.at[behind % 2, half],
                      (base + behind // 2, ahead))

    def start():
        for get in gets:
            get.start()

    def prepare():
        for get in gets:
            get.wait()
        for c in range(4):
            rows = slice(128 * c, 128 * c + 128)
            wvt[rows, :] = wqkv_ref[:, 2 * D + 128 * c : 2 * D + 128 * c + 128].astype(F32).T.astype(BF)

    def project(i, length):
        rows = pl.ds(pl.multiple_of(i * 512, 512), 512)
        parts = [x_ref[c, rows, :].astype(F32) for c in range(4)]
        square = parts[0] * parts[0]
        for part in parts[1:]:
            square = square + part * part
        scale = lax.rsqrt(jnp.sum(square, axis=1, keepdims=True) * (1.0 / D) + 1e-6)
        here = jnp.concatenate(
            [(parts[c] * scale * gain_ref[:, 128 * c : 128 * c + 128]).astype(BF) for c in range(4)], axis=1)
        nrm[rows, :] = here
        keys = dot(here, wqkv_ref[:, D : 2 * D])
        vals = dot_t(wvt[...], here)
        lane = lax.broadcasted_iota(jnp.int32, (512, 128), 1)
        pos = lax.broadcasted_iota(jnp.int32, (512, 128), 0) + i * 512
        bias = jnp.where(pos < length, 0.0, NEG)
        tail = jnp.where(lax.broadcasted_iota(jnp.int32, (16, 512), 0) == 0, 1.0, 0.0).astype(BF)
        for c in range(4):
            cols = slice(128 * c, 128 * c + 128)
            ke[rows, cols] = jnp.where(lane == 64, bias, keys[:, cols]).astype(BF)
            ko[rows, cols] = jnp.where(lane == 0, bias, keys[:, cols]).astype(BF)
        for h in range(8):
            vt[h, 0:64, rows] = vals[64 * h : 64 * h + 64, :].astype(BF)
            vt[h, 64:80, rows] = tail


    def attend(n, step):
        lane = lax.broadcasted_iota(jnp.int32, (256, 128), 1)
        tri = (lax.broadcasted_iota(jnp.int32, (256, 256), 0)
               <= lax.broadcasted_iota(jnp.int32, (256, 256), 1))
        here = pl.ds(pl.multiple_of(256 * step, 256), 256)

        def columns(hp):
            return pl.ds(pl.multiple_of(hp * 128, 128), 128)

        def query(hp, odd):
            q = qs[here, columns(hp)].astype(F32)
            if odd:
                return jnp.where(lane >= 64, q, jnp.where(lane == 0, 1.0, 0.0)).astype(BF)
            return jnp.where(lane < 64, q, jnp.where(lane == 64, 1.0, 0.0)).astype(BF)

        def score(hp, odd, qa, c, top):
            s = dot_t((ko if odd else ke)[256 * c : 256 * c + 256, columns(hp)], qa)
            if c == n - 1:
                s = jnp.where(tri, s, NEG)
            sc[odd, c] = s
            m = jnp.max(s.reshape(4, 8, 8, 256), axis=1)
            return m if top is None else jnp.maximum(top, m)

        def finish(top):
            return jnp.max(jnp.max(top, axis=0), axis=0, keepdims=True)

        def pair(hp, tops, more):
            new = []
            for odd in range(2):
                qa, top, acc = query(hp + 1, odd) if more else None, None, None
                for c in range(n):
                    p = jnp.exp2(sc[odd, c] - tops[odd]).astype(BF)
                    o = dot(vt[2 * hp + odd, :, 256 * c : 256 * c + 256], p)
                    acc = o if acc is None else acc + o
                    if more:
                        top = score(hp + 1, odd, qa, c, top)
                ot[2 * hp + odd] = acc
                if more:
                    new.append(finish(top))
            return tuple(new)

        tops = []
        for odd in range(2):
            qa, top = query(0, odd), None
            for c in range(n):
                top = score(0, odd, qa, c, top)
            tops.append(finish(top))
        tops = lax.fori_loop(0, 3, lambda hp, tops: pair(hp, tops, True), tuple(tops))
        pair(3, tops, False)

    def normalise(at):
        for hp in range(4):
            outs = [ot[2 * hp + odd, 0:64, :] * (1.0 / ot[2 * hp + odd, 64:65, :]) for odd in range(2)]
            att[at, 128 * hp : 128 * hp + 128] = jnp.concatenate(outs, axis=0).T.astype(BF)

    def mlp(steps):
        rows = slice(0, 256 * len(steps))
        resid = []
        for step in steps:
            quarter = quarter_of(step)
            src = pl.ds(pl.multiple_of(quarter * 512 + half_of(quarter) * 256, 256), 256)
            resid.append(jnp.concatenate([x_ref[c, src, :].astype(F32) for c in range(4)], axis=1))
        hidden = (jnp.concatenate(resid, axis=0) + dot(att[rows, :], wout_ref[...])).astype(BF)
        hid[rows, :] = hidden
        hidden = hidden.astype(F32)
        scale = lax.rsqrt(jnp.mean(hidden * hidden, axis=1, keepdims=True) + 1e-6)
        att[rows, :] = (hidden * scale * gain2_ref[...]).astype(BF)
        for f in range(0, FF, 256):
            gate = dot(att[rows, :], win_ref[:, f : f + 256])
            high = dot(att[rows, :], win_ref[:, FF + f : FF + f + 256])
            act[rows, f : f + 256] = (gate / (1.0 + jnp.exp(-gate)) * high).astype(BF)
        return (hid[rows, :].astype(F32) + dot(act[rows, :], wdown_ref[...])).astype(BF)

    def run(step, _):
        quarter = quarter_of(step)
        half = half_of(quarter)

        @pl.when(step == 3)
        def _():
            far().wait_recv()
            passing().start()

        for n in range(1, 9):
            @pl.when(2 * quarter + half + 1 == n)
            def _():
                attend(n, step)

        normalise(rows_of(jnp.where(step == 1, 1, 0)))

        @pl.when(step == 1)
        def _():
            obuf[0:512, :] = mlp((0, 1))
            far().start()
            near(1).start()

        @pl.when(step >= 2)
        def _():
            out = mlp((step,))
            obuf[pl.ds(pl.multiple_of(256 * step, 256), 256), :] = out

            @pl.when(step == 2)
            def _():
                near(2).start()

            @pl.when((step == 3) & (holder == k))
            def _():
                out_ref[slot, rows_of(half), :] = out

            @pl.when((step == 3) & (holder != k))
            def _():
                own().start()

        return 0

    def late():
        mine = []
        for step in range(4):
            quarter = quarter_of(step)
            src = pl.ds(pl.multiple_of(quarter * 512 + half_of(quarter) * 256, 256), 256)
            mine.append(nrm[src, :])
        qs[...] = (dot(jnp.concatenate(mine, axis=0), wqkv_ref[:, :D]) * (0.125 * LOG2E)).astype(BF)
        lax.fori_loop(0, 4, run, 0)

        for h in range(2):
            for b in range(2):
                @pl.when((2 * k + h != z) | ((z + k) % 2 != b))
                def _():
                    remote(block(0), out_ref.at[h, pl.ds(256 * b, 256)], send_sem.at[0], recv_sem.at[h, b],
                           (base + 1 - k, z)).wait_recv()
        far().wait_send()
        near(1).wait_send()
        near(2).wait_send()

        @pl.when(holder != k)
        def _():
            own().wait_send()

        passing().wait_send()

    return start, prepare, project, late


def local(token_ids, lengths, table, attn_gain, w_qkv, w_out, mlp_gain, w_in, w_down):
    dma = pltpu.SemaphoreType.DMA
    layer = []
    for entry in LAYER:
        if isinstance(entry, tuple) and entry and not isinstance(entry[-1], int):
            layer.append(pltpu.VMEM(entry[:-1], entry[-1]))
        else:
            layer.append(dma if entry == () else dma((entry,) if isinstance(entry, int) else entry))
    return pl.pallas_call(
        whole_kernel,
        out_shape=pltpu.VMEM((2, 512, D), BF),
        in_specs=[SM, VM, ANY, VM, ANY, ANY, VM, ANY, ANY], out_specs=VM,
        scratch_shapes=[
            pltpu.VMEM((4, 2048, 128), BF),
            pltpu.VMEM((4, 2, 512), jnp.int32), pltpu.VMEM((32, 4, 128), jnp.int32), pltpu.VMEM((32, 4, 128), jnp.int32),
            pltpu.SMEM((32, 4, 128), jnp.int32), pltpu.VMEM((32, 128), jnp.int32), pltpu.SMEM((32, 128), jnp.int32),
            pltpu.VMEM((16384, 128), BF), pltpu.VMEM((16384, 128), F32), pltpu.VMEM((1024, 128), F32),
            pltpu.VMEM((31, CAP, 128), BF), pltpu.VMEM((14, CAP, 128), BF), pltpu.VMEM((32, CAP, 128), BF),
            pltpu.VMEM((2, 2048, 128), BF), pltpu.VMEM((1024, 128), BF),
            dma((3,)), dma((3,)), dma((31,)), dma((31,)), dma((2,)), dma((32,)), dma((31,)), dma((31,)), dma((14,)), dma((14,)),
            dma((2, 4)), dma((4,)), dma((2,)), dma((3, 2)), dma((2,)), dma((3, 2)), dma((3, 2)), dma((4,)), dma((4,))] + layer,
        compiler_params=params(1, 61),
    )(lengths, token_ids, table, attn_gain.reshape(1, D), w_qkv, w_out, mlp_gain.reshape(1, D), w_in, w_down)


def solution(mesh):
    in_specs = (P("rows", "cols"), P("rows"), P("rows", "cols"), P(), P(), P(), P(), P(), P())
    return jax.shard_map(local, mesh=mesh, in_specs=in_specs, out_specs=P("rows", "cols", None), check_vma=False)
```

```python
import jax
import jax.numpy as jnp
from jax import lax
from jax.experimental import pallas as pl
from jax.experimental.pallas import tpu as pltpu
from jax.sharding import PartitionSpec as P

D = 512
FF = 2048
CAP = 344
BF = jnp.bfloat16
F32 = jnp.float32
MESH = pl.DeviceIdType.MESH
ANY = pl.BlockSpec(memory_space=pl.ANY)
VM = pl.BlockSpec(memory_space=pltpu.VMEM)
SM = pl.BlockSpec(memory_space=pltpu.SMEM)
LOG2E = 1.4426950408889634
NEG = -1e30


def dot(a, b):
    return jnp.dot(a, b, preferred_element_type=F32)


def dot_t(a, b):
    return lax.dot_general(a, b, (((1,), (1,)), ((), ())), preferred_element_type=F32)


def place():
    r, z = lax.axis_index("rows"), lax.axis_index("cols")
    return r, z, r // 8, (r // 2) % 4, r % 2


def greet(devices):
    barrier = pltpu.get_barrier_semaphore()
    for device in devices:
        pl.semaphore_signal(barrier, inc=1, device_id=device, device_id_type=MESH)
    pl.semaphore_wait(barrier, len(devices))


def remote(src, dst, send_sem, recv_sem, device):
    return pltpu.make_async_remote_copy(
        src_ref=src, dst_ref=dst, send_sem=send_sem, recv_sem=recv_sem,
        device_id=device, device_id_type=MESH)


def params(collective_id=None, vmem=60):
    kw = {}
    if collective_id is not None:
        kw = dict(collective_id=collective_id, has_side_effects=True)
    return pltpu.CompilerParams(vmem_limit_bytes=vmem * 2**20, **kw)


def routes():
    out = []
    for dy in range(4):
        for dx in range(4):
            for dk in range(2):
                if dx == dy == dk == 0:
                    continue
                side = 1 if dk == 0 else 3
                hop = None
                if dx == 2 or dy == 2:
                    hop = (side if dy == 2 else 0, side if dx == 2 else 0)
                out.append((dy, dx, dk, hop))
    def key(f):
        near = f[3] is None and (f[0] == 0 or f[1] == 0)
        late = near and f[2] == 1 and (f[0] or f[1])
        return (3 if late else 0 if near else 1 if f[3] else 2, f[2] == 0 if f[0] or f[1] else False, (f[0] * 5 + f[1] * 3 + f[2] * 7) % 11)

    return sorted(out, key=key)


def requests(ids, lens, msg_ref, slot_ref):
    before = (lax.broadcasted_iota(jnp.int32, (128, 128), 0)
              < lax.broadcasted_iota(jnp.int32, (128, 128), 1)).astype(F32)
    above = (lax.broadcasted_iota(jnp.int32, (32, 32), 1)
             < lax.broadcasted_iota(jnp.int32, (32, 32), 0)).astype(F32).astype(BF)
    both = jnp.concatenate([before, jnp.ones((128, 128), F32)], axis=0).astype(BF)
    owners = lax.broadcasted_iota(jnp.int32, (32, 128), 0)
    ks = lax.broadcasted_iota(jnp.int32, (176, 128), 0)
    lane = lax.broadcasted_iota(jnp.int32, (32, 128), 1)
    owner = ids >> 14
    low, high = (ids & 127).astype(F32), ((ids >> 7) & 127).astype(F32)
    ones = [jnp.where(owner == o, 1.0, 0.0).astype(BF) for o in range(32)]
    rows_above = dot(above, jnp.concatenate(ones, axis=1)).astype(BF)
    prior = dot(
        jnp.concatenate(
            [jnp.concatenate(ones, axis=0),
             jnp.concatenate([rows_above[:, 128 * o : 128 * o + 128] for o in range(32)], axis=0)], axis=1),
        both)
    rank = jnp.zeros((32, 128), F32)
    for o in range(32):
        rank = rank + jnp.where(owner == o, prior[32 * o : 32 * o + 32], 0.0)
    rank_i = rank.astype(jnp.int32)
    slot_ref[...] = jnp.clip(owner * CAP + rank_i, 0, 32 * CAP - 1)
    upper = jnp.where(rank_i >= CAP // 2, 1, 0)
    within = rank_i - upper * (CAP // 2)
    acc = jnp.zeros((128, 176), F32)
    for a in range(0, 32, 2):
        lefts, rights = [], []
        for b in (a, a + 1):
            part = slice(b, b + 1)
            left = []
            for half in range(2):
                hit = owners == jnp.where(upper[part] == half, owner[part], -1)
                left += [jnp.where(hit, low[part], 0.0), jnp.where(hit, high[part], 0.0)]
            lefts.append(jnp.concatenate(left, axis=0).astype(BF))
            rights.append(jnp.where(ks == jnp.where(within[part] < CAP // 2, within[part], -1), 1.0, 0.0).astype(BF))
        acc = acc + dot_t(jnp.concatenate(lefts, axis=1), jnp.concatenate(rights, axis=1))
    req = [(acc[64 * half + 32 : 64 * half + 64] * 128.0 + acc[64 * half : 64 * half + 32]).astype(jnp.int32)
           for half in range(2)]
    msg_ref[...] = jnp.zeros_like(msg_ref)
    msg_ref[:, 0, :] = jnp.where(lane == 126, lens[0], jnp.where(lane == 127, lens[1], 0))
    for j in range(4):
        at = CAP // 4 * (j % 2)
        msg_ref[:, j, 0 : CAP // 4] = req[j // 2][:, at : at + CAP // 4]


def whole_kernel(len_ref, tok_ref, table_hbm, gain_ref, wqkv_hbm, wout_hbm, gain2_ref, win_hbm, wdown_hbm, out_ref, *rest):
    front, layer = rest[: -len(LAYER)], rest[-len(LAYER) :]
    start, prepare, project, late = layer_kernel(
        gain_ref, wqkv_hbm, wout_hbm, gain2_ref, win_hbm, wdown_hbm, out_ref, layer, front[0])
    front_kernel(len_ref, tok_ref, table_hbm, *front, start, prepare, project)
    late()


def front_kernel(len_ref, tok_ref, table_hbm, out_ref,
                 ids_ref, msg_ref, asked_v, asked_s, slot_v, slot_s, table_ref, wide, stage, block, relay, back, emb,
                 relay_z, ids_send, ids_recv, ask_send, ask_recv, copy_sem, list_sem, send_sem, recv_sem, hop_send, hop_recv,
                 z_send, z_relay_send, z_relay_recv, z_recv, relay_pass, pass_send, pass_recv, own_send, own_recv, start, prepare, project):
    r, z, y, x, k = place()
    base = r - k
    other = (base + 1 - k, z)
    up, down = (z + 1) % 4, (z + 3) % 4
    holder = z // 2
    column = [(r, (z + s) % 4) for s in (1, 2, 3)]
    plane = [((r + s) % 32, z) for s in range(1, 32)]
    load = pltpu.make_async_copy(table_hbm, table_ref, copy_sem.at[0])
    load.start()
    start()
    greet(column + plane + [(base + 1 - k, up), (base + 1 - k, down)])

    copies = []
    for s, device in enumerate(column):
        copy = remote(tok_ref, ids_ref.at[z], ids_send.at[s], ids_recv.at[s], device)
        copy.start()
        copies.append(copy)
    ids_ref[z] = tok_ref[...]
    for copy in copies:
        copy.wait()
    ids = jnp.concatenate(
        [ids_ref[c, h : h + 1, 128 * j : 128 * j + 128] for c in range(4) for h in range(2) for j in range(4)], axis=0)
    requests(ids, (len_ref[0], len_ref[1]), msg_ref, slot_v)

    copies = []
    for s, device in enumerate(plane):
        copy = remote(msg_ref.at[device[0]], asked_v.at[r], ask_send.at[s], ask_recv.at[s], device)
        copy.start()
        copies.append(copy)
    asked_v[r] = msg_ref[r]
    to_slots = pltpu.make_async_copy(slot_v, slot_s, copy_sem.at[1])
    to_slots.start()
    load.wait()

    def widen(i, _):
        rows = pl.ds(pl.multiple_of(i * 256, 256), 256)
        wide[rows, :] = table_ref[rows, :].astype(F32)
        return 0

    lax.fori_loop(0, 64, widen, 0)
    to_slots.wait()

    def row(dy, dx, dk):
        return (((y + dy) % 4) * 4 + (x + dx) % 4) * 2 + (k + dk) % 2

    def fill(p, dst):
        def some(j, _):
            for i in range(CAP // 4):
                stage[pl.ds(j * (CAP // 4) + i, 1), :] = wide[pl.ds(asked_s[p, j, i], 1), :]
            return 0

        lax.fori_loop(0, 4, some, 0)
        dst[...] = stage[0:CAP, :].astype(BF)

    def take(p, n, arrived=True):
        if arrived:
            remote(msg_ref.at[0], asked_v.at[p], ask_send.at[0], ask_recv.at[(r - p) % 32 - 1], other).wait_recv()
        asked_v[p] = jnp.clip(asked_v[p], 0, 16383)
        copy = pltpu.make_async_copy(asked_v.at[p], asked_s.at[p], list_sem.at[n])
        copy.start()
        return copy

    flows = routes()
    hops = [f for f in flows if f[3] is not None]
    direct = [f for f in flows if f[3] is None]
    first, final, waiting = [], [], None
    lists = [take(row(*flows[0][:3]), 0)]
    for n, flow in enumerate(flows):
        dy, dx, dk, hop = flow
        p = row(dy, dx, dk)
        lists.append(take(row(*flows[n + 1][:3]), n + 1) if n + 1 < len(flows) else take(r, 31, False))
        lists[n].wait()
        fill(p, block.at[n])
        if hop is not None:
            i = hops.index(flow)
            copy = remote(block.at[n], relay.at[i], hop_send.at[i], hop_recv.at[i], (row(*hop, 0), z))
            first.append(copy)
        else:
            i = direct.index(flow)
            copy = remote(block.at[n], back.at[r], send_sem.at[i], recv_sem.at[i], (p, z))
            final.append((copy, row(-dy, -dx, dk)))
        if waiting is not None:
            waiting.start()
        waiting = copy
    lists[31].wait()
    length = asked_s[base + holder, 0, 126 + z % 2]
    for copy in copies:
        copy.wait_send()
    fill(r, back.at[r])
    waiting.start()
    for i, (dy, dx, dk, (hy, hx)) in enumerate(hops):
        first[i].wait_recv()
        n = len(direct) + i
        copy = remote(relay.at[i], back.at[row(-hy, -hx, 0)], send_sem.at[n], recv_sem.at[n],
                      (row(dy - hy, dx - hx, dk), z))
        copy.start()
        final.append((copy, row(-dy, -dx, dk)))

    prepare()

    def spread(source):
        wide[pl.ds(pl.multiple_of(source * CAP, 8), CAP), :] = back[source].astype(F32)

    spread(r)
    for copy, source in final:
        copy.wait_recv()
        spread(source)

    def rows(c):
        return pl.ds(pl.multiple_of(512 * c, 512), 512)

    def far(h, c):
        return remote(emb.at[h, rows(c)], relay_z.at[rows(c % 2)], z_relay_send.at[c], z_relay_recv.at[c % 2],
                      (base + c // 2, (up, down)[c // 2]))

    def near(h, c, step):
        return remote(emb.at[h, rows(c)], out_ref.at[z, rows(c)],
                      z_send.at[step // 2, c], z_recv.at[step // 2, c % 2], (base + c // 2, (z + step) % 4))

    def own(h, c):
        return remote(emb.at[h, rows(c)], out_ref.at[z, rows(c)], own_send.at[c], own_recv.at[c], other)

    def send(h, c, act):
        dist = (2 * k + h - z) % 4

        @pl.when(dist == 2)
        def _():
            act(far(h, c))

        for step in (1, 3):
            @pl.when(dist == step)
            def _():
                act(near(h, c, step))

        @pl.when(dist == 0)
        def _():
            act(own(h, c))

    lead = jnp.where((2 * k - z) % 4 < 2, 1, 0)
    pieces = [(h, c) for h in (lead, 1 - lead) for c in (0, 2, 1, 3)]
    waiting = None
    for h, c in pieces:
        def gather(j, _):
            a = c * 8 + h * 4 + j
            for i in range(128):
                stage[pl.ds(j * 128 + i, 1), :] = wide[pl.ds(slot_s[a, i], 1), :]
            return 0

        lax.fori_loop(0, 4, gather, 0)
        emb[h, rows(c), :] = stage[0:512, :].astype(BF)

        @pl.when((2 * k + h - z) % 4 == 0)
        def _():
            out_ref[z, rows(c), :] = stage[0:512, :].astype(BF)

        if waiting is not None:
            send(*waiting, lambda copy: copy.start())
        waiting = (h, c)
    send(*waiting, lambda copy: copy.start())

    behind = jnp.where(k == 0, down, up)
    ahead = jnp.where(k == 0, up, down)
    sources = (down, up, (z + 2) % 4)
    relayed = []
    for j in range(2):
        copy = remote(relay_z.at[rows(j)], out_ref.at[behind, rows(2 * k + j)], relay_pass.at[j], z_recv.at[2, j], (r, ahead))
        far(0, j).wait_recv()
        copy.start()
        relayed.append(copy)
    passed = []
    for j in range(2):
        for i, source in enumerate(sources):
            got = out_ref.at[source, rows(2 * k + j)]
            remote(got, got, pass_send.at[i, j], z_recv.at[i, j], other).wait_recv()
            copy = remote(got, got, pass_send.at[i, j], pass_recv.at[i, j], other)
            copy.start()
            passed.append(copy)

        if j == 0:
            @pl.when(k != holder)
            def _():
                for c in range(4):
                    own(0, c).wait_recv()

        project(2 * k + j, length)
    for j in range(2):
        for i, source in enumerate(sources):
            got = out_ref.at[source, rows(2 * (1 - k) + j)]
            remote(got, got, pass_send.at[i, j], pass_recv.at[i, j], other).wait_recv()
        project(2 * (1 - k) + j, length)
    for copy in first:
        copy.wait_send()
    for copy, _ in final:
        copy.wait_send()
    for copy in passed + relayed:
        copy.wait_send()
    for h, c in pieces:
        send(h, c, lambda copy: copy.wait_send())


LAYER = [(2048, D, BF), (1024, D, BF), (2048, D, BF), (2048, D, BF), (8, 80, 2048, BF), (D, D, BF), (2, 8, 256, 256, F32),
         (8, 80, 256, F32), (512, D, BF), (512, D, BF), (512, FF, BF), (1024, D, BF), (256, D, BF), (D, 3 * D, BF), (D, D, BF),
         (D, 2 * FF, BF), (FF, D, BF), 4, (4,), (), (2, 2), ()]


def layer_kernel(gain_ref, wqkv_hbm, wout_hbm, gain2_ref, win_hbm, wdown_hbm, out_ref, scratch, x_ref):
    (nrm, qs, ke, ko, vt, wvt, sc, ot, att, hid, act, obuf, relay, wqkv_ref, wout_ref, win_ref, wdown_ref, sems,
     send_sem, far_recv, recv_sem, pass_send) = scratch
    r, z, _, _, k = place()
    base = r - k
    up, down = (z + 1) % 4, (z + 3) % 4
    holder, slot = z // 2, z % 2
    gets = [pltpu.make_async_copy(src, dst, sems.at[i]) for i, (src, dst) in enumerate(
        [(wqkv_hbm, wqkv_ref), (wout_hbm, wout_ref), (win_hbm, win_ref), (wdown_hbm, wdown_ref)])]
    ahead, behind = jnp.where(k == 0, up, down), jnp.where(k == 0, down, up)

    def quarter_of(step):
        return jnp.where(step == 0, (z + 2) % 4, jnp.where(step == 1, ahead, jnp.where(step == 2, behind, z)))

    def half_of(quarter):
        return (quarter + k) % 2

    def rows_of(half):
        return pl.ds(pl.multiple_of(256 * half, 256), 256)

    def block(step):
        return obuf.at[pl.ds(256 * step, 256)]

    def landing(step):
        return out_ref.at[slot, rows_of(half_of(quarter_of(step)))]

    def far():
        return remote(block(0), relay, send_sem.at[0], far_recv, (r, ahead))

    def near(step):
        q = quarter_of(step)
        return remote(block(step), landing(step), send_sem.at[step], recv_sem.at[slot, half_of(q)], (base + holder, q))

    def own():
        return remote(block(3), landing(3), send_sem.at[3], recv_sem.at[slot, half_of(z)], (base + 1 - k, z))

    def passing():
        half = half_of(ahead)
        return remote(relay, out_ref.at[behind % 2, rows_of(half)], pass_send, recv_sem.at[behind % 2, half],
                      (base + behind // 2, ahead))

    def start():
        for get in gets:
            get.start()

    def prepare():
        for get in gets:
            get.wait()
        for c in range(4):
            rows = slice(128 * c, 128 * c + 128)
            wvt[rows, :] = wqkv_ref[:, 2 * D + 128 * c : 2 * D + 128 * c + 128].astype(F32).T.astype(BF)

    def project(i, length):
        rows = pl.ds(pl.multiple_of(i * 512, 512), 512)
        parts = [x_ref[c, rows, :].astype(F32) for c in range(4)]
        square = parts[0] * parts[0]
        for part in parts[1:]:
            square = square + part * part
        scale = lax.rsqrt(jnp.sum(square, axis=1, keepdims=True) * (1.0 / D) + 1e-6)
        here = jnp.concatenate(
            [(parts[c] * scale * gain_ref[:, 128 * c : 128 * c + 128]).astype(BF) for c in range(4)], axis=1)
        nrm[rows, :] = here
        keys = dot(here, wqkv_ref[:, D : 2 * D])
        vals = dot_t(wvt[...], here)
        lane = lax.broadcasted_iota(jnp.int32, (512, 128), 1)
        pos = lax.broadcasted_iota(jnp.int32, (512, 128), 0) + i * 512
        bias = jnp.where(pos < length, 0.0, NEG)
        tail = jnp.where(lax.broadcasted_iota(jnp.int32, (16, 512), 0) == 0, 1.0, 0.0).astype(BF)
        for c in range(4):
            cols = slice(128 * c, 128 * c + 128)
            ke[rows, cols] = jnp.where(lane == 64, bias, keys[:, cols]).astype(BF)
            ko[rows, cols] = jnp.where(lane == 0, bias, keys[:, cols]).astype(BF)
        for h in range(8):
            vt[h, 0:64, rows] = vals[64 * h : 64 * h + 64, :].astype(BF)
            vt[h, 64:80, rows] = tail


    def attend(n, step):
        lane = lax.broadcasted_iota(jnp.int32, (256, 128), 1)
        tri = (lax.broadcasted_iota(jnp.int32, (256, 256), 0)
               <= lax.broadcasted_iota(jnp.int32, (256, 256), 1))
        here = pl.ds(pl.multiple_of(256 * step, 256), 256)

        def columns(hp):
            return pl.ds(pl.multiple_of(hp * 128, 128), 128)

        def query(hp, odd):
            q = qs[here, columns(hp)].astype(F32)
            if odd:
                return jnp.where(lane >= 64, q, jnp.where(lane == 0, 1.0, 0.0)).astype(BF)
            return jnp.where(lane < 64, q, jnp.where(lane == 64, 1.0, 0.0)).astype(BF)

        def score(hp, odd, qa, c, top):
            s = dot_t((ko if odd else ke)[256 * c : 256 * c + 256, columns(hp)], qa)
            if c == n - 1:
                s = jnp.where(tri, s, NEG)
            sc[odd, c] = s
            m = jnp.max(s.reshape(4, 8, 8, 256), axis=1)
            return m if top is None else jnp.maximum(top, m)

        def finish(top):
            return jnp.max(jnp.max(top, axis=0), axis=0, keepdims=True)

        def pair(hp, tops, more):
            new = []
            for odd in range(2):
                qa, top, acc = query(hp + 1, odd) if more else None, None, None
                for c in range(n):
                    p = jnp.exp2(sc[odd, c] - tops[odd]).astype(BF)
                    o = dot(vt[2 * hp + odd, :, 256 * c : 256 * c + 256], p)
                    acc = o if acc is None else acc + o
                    if more:
                        top = score(hp + 1, odd, qa, c, top)
                ot[2 * hp + odd] = acc
                if more:
                    new.append(finish(top))
            return tuple(new)

        tops = []
        for odd in range(2):
            qa, top = query(0, odd), None
            for c in range(n):
                top = score(0, odd, qa, c, top)
            tops.append(finish(top))
        tops = lax.fori_loop(0, 3, lambda hp, tops: pair(hp, tops, True), tuple(tops))
        pair(3, tops, False)

    def normalise(at):
        for hp in range(4):
            outs = [ot[2 * hp + odd, 0:64, :] * (1.0 / ot[2 * hp + odd, 64:65, :]) for odd in range(2)]
            att[at, 128 * hp : 128 * hp + 128] = jnp.concatenate(outs, axis=0).T.astype(BF)

    def mlp(steps):
        rows = slice(0, 256 * len(steps))
        resid = []
        for step in steps:
            quarter = quarter_of(step)
            src = pl.ds(pl.multiple_of(quarter * 512 + half_of(quarter) * 256, 256), 256)
            resid.append(jnp.concatenate([x_ref[c, src, :].astype(F32) for c in range(4)], axis=1))
        hidden = (jnp.concatenate(resid, axis=0) + dot(att[rows, :], wout_ref[...])).astype(BF)
        hid[rows, :] = hidden
        hidden = hidden.astype(F32)
        scale = lax.rsqrt(jnp.mean(hidden * hidden, axis=1, keepdims=True) + 1e-6)
        att[rows, :] = (hidden * scale * gain2_ref[...]).astype(BF)
        for f in range(0, FF, 256):
            gate = dot(att[rows, :], win_ref[:, f : f + 256])
            high = dot(att[rows, :], win_ref[:, FF + f : FF + f + 256])
            act[rows, f : f + 256] = (gate / (1.0 + jnp.exp(-gate)) * high).astype(BF)
        return (hid[rows, :].astype(F32) + dot(act[rows, :], wdown_ref[...])).astype(BF)

    def run(step, _):
        quarter = quarter_of(step)
        half = half_of(quarter)

        @pl.when(step == 3)
        def _():
            far().wait_recv()
            passing().start()

        for n in range(1, 9):
            @pl.when(2 * quarter + half + 1 == n)
            def _():
                attend(n, step)

        normalise(rows_of(jnp.where(step == 1, 1, 0)))

        @pl.when(step == 1)
        def _():
            obuf[0:512, :] = mlp((0, 1))
            far().start()
            near(1).start()

        @pl.when(step >= 2)
        def _():
            out = mlp((step,))
            obuf[pl.ds(pl.multiple_of(256 * step, 256), 256), :] = out

            @pl.when(step == 2)
            def _():
                near(2).start()

            @pl.when((step == 3) & (holder == k))
            def _():
                out_ref[slot, rows_of(half), :] = out

            @pl.when((step == 3) & (holder != k))
            def _():
                own().start()

        return 0

    def late():
        mine = []
        for step in range(4):
            quarter = quarter_of(step)
            src = pl.ds(pl.multiple_of(quarter * 512 + half_of(quarter) * 256, 256), 256)
            mine.append(nrm[src, :])
        qs[...] = (dot(jnp.concatenate(mine, axis=0), wqkv_ref[:, :D]) * (0.125 * LOG2E)).astype(BF)
        lax.fori_loop(0, 4, run, 0)

        for h in range(2):
            for b in range(2):
                @pl.when((2 * k + h != z) | ((z + k) % 2 != b))
                def _():
                    remote(block(0), out_ref.at[h, pl.ds(256 * b, 256)], send_sem.at[0], recv_sem.at[h, b],
                           (base + 1 - k, z)).wait_recv()
        far().wait_send()
        near(1).wait_send()
        near(2).wait_send()

        @pl.when(holder != k)
        def _():
            own().wait_send()

        passing().wait_send()

    return start, prepare, project, late


def local(token_ids, lengths, table, attn_gain, w_qkv, w_out, mlp_gain, w_in, w_down):
    dma = pltpu.SemaphoreType.DMA
    layer = []
    for entry in LAYER:
        if isinstance(entry, tuple) and entry and not isinstance(entry[-1], int):
            layer.append(pltpu.VMEM(entry[:-1], entry[-1]))
        else:
            layer.append(dma if entry == () else dma((entry,) if isinstance(entry, int) else entry))
    return pl.pallas_call(
        whole_kernel,
        out_shape=pltpu.VMEM((2, 512, D), BF),
        in_specs=[SM, VM, ANY, VM, ANY, ANY, VM, ANY, ANY], out_specs=VM,
        scratch_shapes=[
            pltpu.VMEM((4, 2048, 128), BF),
            pltpu.VMEM((4, 2, 512), jnp.int32), pltpu.VMEM((32, 4, 128), jnp.int32), pltpu.VMEM((32, 4, 128), jnp.int32),
            pltpu.SMEM((32, 4, 128), jnp.int32), pltpu.VMEM((32, 128), jnp.int32), pltpu.SMEM((32, 128), jnp.int32),
            pltpu.VMEM((16384, 128), BF), pltpu.VMEM((16384, 128), F32), pltpu.VMEM((1024, 128), F32),
            pltpu.VMEM((31, CAP, 128), BF), pltpu.VMEM((14, CAP, 128), BF), pltpu.VMEM((32, CAP, 128), BF),
            pltpu.VMEM((2, 2048, 128), BF), pltpu.VMEM((1024, 128), BF),
            dma((3,)), dma((3,)), dma((31,)), dma((31,)), dma((2,)), dma((32,)), dma((31,)), dma((31,)), dma((14,)), dma((14,)),
            dma((2, 4)), dma((4,)), dma((2,)), dma((3, 2)), dma((2,)), dma((3, 2)), dma((3, 2)), dma((4,)), dma((4,))] + layer,
        compiler_params=params(1, 61),
    )(lengths, token_ids, table, attn_gain.reshape(1, D), w_qkv, w_out, mlp_gain.reshape(1, D), w_in, w_down)


def solution(mesh):
    in_specs = (P("rows", "cols"), P("rows"), P("rows", "cols"), P(), P(), P(), P(), P(), P())
    return jax.shard_map(local, mesh=mesh, in_specs=in_specs, out_specs=P("rows", "cols", None), check_vma=False)
```
